32 devices in a mesh: dp: 8 (over y, x, core), tensor: 4 (over z).
Axes of the slice: x: 2, y: 2, z: 4, core: 2. Of those that a mesh axis runs over, the one named last changes fastest.
Arguments:
- tokens: bfloat16 [8192, 2048], P(('dp', 'tensor')), may hold values from -6 to 6
- out_grad: bfloat16 [8192, 2048], P(('dp', 'tensor')), may hold values from -6 to 6
- segment_ids: int32 [8192], P('dp'), may hold values from 0 to 64, as said below
- positions: int32 [8192], P('dp'), may hold values from 0 to 1999, as said below
- norm1_gain: float32 [2048], replicated, may hold values from 0.1 to 1.9
- norm1_bias: float32 [2048], replicated, may hold values from -3 to 3
- norm2_gain: float32 [2048], replicated, may hold values from 0.1 to 1.9
- norm2_bias: float32 [2048], replicated, may hold values from -3 to 3
- qkv_weight: bfloat16 [2048, 8, 3, 256], P(None, 'tensor'), may hold values from -0.125 to 0.125
- qkv_bias: bfloat16 [8, 3, 256], P('tensor'), may hold values from -4 to 4
- out_weight: bfloat16 [8, 256, 2048], P('tensor'), may hold values from -0.75 to 0.75
- out_bias: bfloat16 [2048], replicated, may hold values from -3 to 3
- fc1_weight: bfloat16 [2048, 8192], P(None, 'tensor'), may hold values from -0.125 to 0.125
- fc1_bias: bfloat16 [8192], P('tensor'), may hold values from -3 to 3
- fc2_weight: bfloat16 [8192, 2048], P('tensor'), may hold values from -0.0625 to 0.0625
- fc2_bias: bfloat16 [2048], replicated, may hold values from -3 to 3
Outputs:
- block_out: bfloat16 [8192, 2048], P(('dp', 'tensor'))
- tokens_grad: bfloat16 [8192, 2048], P(('dp', 'tensor'))
- norm1_gain_grad: float32 [2048], replicated
- norm1_bias_grad: float32 [2048], replicated
- norm2_gain_grad: float32 [2048], replicated
- norm2_bias_grad: float32 [2048], replicated
- qkv_weight_grad: float32 [2048, 8, 3, 256], P(None, 'tensor')
- qkv_bias_grad: float32 [8, 3, 256], P('tensor')
- out_weight_grad: float32 [8, 256, 2048], P('tensor')
- out_bias_grad: float32 [2048], replicated
- fc1_weight_grad: float32 [2048, 8192], P(None, 'tensor')
- fc1_bias_grad: float32 [8192], P('tensor')
- fc2_weight_grad: float32 [8192, 2048], P('tensor')
- fc2_bias_grad: float32 [2048], replicated
The draws below stay inside these ranges and needn't reach their ends.
Inputs may be any that keep to these rules, and one draw needn't show every extreme that they name: `segment_ids`: never falling along the tokens; the tokens of one document share one number. A document has 1 to 2000 tokens; one document of exactly 2000 tokens ends on token 4096. The last document carries the largest number. `positions`: the token's index within its document, 0 at the document's first token.
All inputs are finite; a program needn't handle non-finite values.
Results may differ from the reference program's by a relative error of at most 0.0065.
The reference program's roundings to bfloat16 on the way count: a program that leaves them out, or rounds other values in their place, can miss the bound.
Values may be sent and summed in bfloat16 or wider, within the bound.
A program may use at most 256 MiB of HBM per device.

```python
import math
import jax
import jax.numpy as jnp
from jax import lax

D = 2048
HEADS = 8
HD = 256
ROT = 64
FF = 8192
MOST = 2000
MIN_DOC = 200
TOKENS = 8192
SEQ = 8192


def documents(key):
    folded = jax.random.fold_in(key, 11)
    anchor = TOKENS // 2 - MOST + 1
    before_slots = TOKENS // (2 * MIN_DOC) + 1
    after_slots = TOKENS // MIN_DOC + 1
    last_label = before_slots + after_slots + 2
    first_lengths = jax.random.randint(jax.random.fold_in(folded, 1), (before_slots,), MIN_DOC, MOST + 1).astype(jnp.int32)
    second_lengths = jax.random.randint(jax.random.fold_in(folded, 2), (after_slots,), MIN_DOC, MOST + 1).astype(jnp.int32)
    first_ends = jnp.cumsum(first_lengths).astype(jnp.int32)
    first_ends = jnp.where(first_ends < anchor, first_ends, TOKENS).astype(jnp.int32)
    second_ends = (anchor + MOST + jnp.cumsum(second_lengths)).astype(jnp.int32)
    second_ends = jnp.where(second_ends < TOKENS, second_ends, TOKENS).astype(jnp.int32)
    fixed_ends = jnp.array([anchor, anchor + MOST], dtype=jnp.int32)
    bounds = jnp.concatenate([first_ends, fixed_ends, second_ends], 0).astype(jnp.int32)
    token_index = jnp.arange(TOKENS, dtype=jnp.int32)
    passed = token_index[:, None] >= bounds[None, :]
    doc_index = jnp.sum(passed.astype(jnp.int32), axis=1).astype(jnp.int32)
    doc_begin = jnp.max(jnp.where(passed, bounds[None, :], 0), axis=1).astype(jnp.int32)
    position = (token_index - doc_begin).astype(jnp.int32)
    last_index = doc_index[TOKENS - 1]
    segment = jnp.where(doc_index == last_index, last_label, doc_index).astype(jnp.int32)
    return (segment, position)


def draw_segment_ids(key, part):
    return documents(key)[0]


def draw_positions(key, part):
    return documents(key)[1]


def draw_qkv_bias(key, part):
    base = jnp.clip(0.5 * jax.random.normal(jax.random.fold_in(key, 21), (HEADS, 3, HD), jnp.float32), -3.0, 3.0)
    return base.astype(jnp.bfloat16)


def block_scale(key, shape, shards, smallest, largest):
    def one(dim, blocks):
        steps = jax.random.uniform(jax.random.fold_in(jax.random.fold_in(key, 6), dim), (blocks,), jnp.float32, smallest / len(shards), largest / len(shards))
        return jnp.repeat(jnp.exp(steps), shape[dim] // blocks).reshape((-1,) + (1,) * (len(shape) - dim - 1))

    loudness = one(*shards[0])
    for cut in shards[1:]:
        loudness = loudness * one(*cut)
    return loudness


def bell_draw(own_key, extent, deviation, reach, cuts=(), held_as=jnp.bfloat16):
    loudness = block_scale(own_key, extent, cuts, -0.22, 0.18) if cuts else 1.0
    values = jax.random.normal(own_key, extent, jnp.float32) * deviation * loudness
    return jnp.minimum(jnp.maximum(values, -reach), reach).astype(held_as)


def setup_inputs(seed: int = 0) -> dict:
    seeds = jax.random.split(jax.random.key(seed), 17)
    return {
        "tokens": bell_draw(seeds[0], (TOKENS, D), 1.0, 6.0, ((0, 32),)),
        "out_grad": bell_draw(seeds[1], (TOKENS, D), 1.0, 6.0, ((0, 32),)),
        "segment_ids": draw_segment_ids(jax.random.fold_in(seeds[16], 71), 0),
        "positions": draw_positions(jax.random.fold_in(seeds[16], 71), 0),
        "norm1_gain": jnp.clip(1.0 + 0.18 * jax.random.normal(seeds[4], (D,), jnp.float32), 0.1, 1.9),
        "norm1_bias": bell_draw(seeds[5], (D,), 0.5, 3.0, (), jnp.float32),
        "norm2_gain": jnp.clip(1.0 + 0.18 * jax.random.normal(seeds[6], (D,), jnp.float32), 0.1, 1.9),
        "norm2_bias": bell_draw(seeds[7], (D,), 0.5, 3.0, (), jnp.float32),
        "qkv_weight": bell_draw(seeds[8], (D, HEADS, 3, HD), D ** -0.5, 0.125, ((1, 4),)),
        "qkv_bias": draw_qkv_bias(jax.random.fold_in(seeds[16], 71), 0),
        "out_weight": bell_draw(seeds[10], (HEADS, HD, D), (HEADS * HD // 32) ** -0.5, 0.75, ((0, 4),)),
        "out_bias": bell_draw(seeds[11], (D,), 0.5, 3.0),
        "fc1_weight": bell_draw(seeds[12], (D, FF), D ** -0.5, 0.125, ((1, 4),)),
        "fc1_bias": bell_draw(seeds[13], (FF,), 0.5, 3.0, ((0, 4),)),
        "fc2_weight": bell_draw(seeds[14], (FF, D), FF ** -0.5, 0.0625, ((0, 4),)),
        "fc2_bias": bell_draw(seeds[15], (D,), 0.5, 3.0),
    }


@jax.custom_vjp
def low(v):
    return lax.optimization_barrier(v.astype(jnp.bfloat16)).astype(jnp.float32)

@jax.custom_vjp
def low_back(v):
    return v

def low_keep(v):
    return (low(v), None)

def low_pass(kept, grad):
    return (grad,)

def back_keep(v):
    return (v, None)

def back_low(kept, grad):
    return (low(grad),)
low.defvjp(low_keep, low_pass)
low_back.defvjp(back_keep, back_low)
epsilon = 1e-05
precise = lax.Precision.HIGHEST

def layer_norm(values_in, gain, shift):
    average = lax.optimization_barrier(jnp.mean(values_in, -1, keepdims=True))
    centered = values_in - average
    variance = lax.optimization_barrier(jnp.mean(centered * centered, -1, keepdims=True))
    return centered * lax.rsqrt(variance + epsilon) * gain + shift

def rope_tables(position, rot_dims):
    half_rot = rot_dims // 2
    frequency = jnp.power(jnp.float32(10000.0), -jnp.arange(half_rot, dtype=jnp.float32) / jnp.float32(half_rot))
    angles = position.astype(jnp.float32)[:, None] * frequency[None, :]
    return (jnp.cos(angles), jnp.sin(angles))

def rotate(tensor_in, cos_table, sin_table, rot_dims):
    half_rot = rot_dims // 2
    first_half = tensor_in[..., :half_rot]
    second_half = tensor_in[..., half_rot:rot_dims]
    cos_part = cos_table[:, None, :]
    sin_part = sin_table[:, None, :]
    return jnp.concatenate([first_half * cos_part - second_half * sin_part, second_half * cos_part + first_half * sin_part, tensor_in[..., rot_dims:]], -1)

def attention(queries, all_keys, values, segment):
    seq_len = queries.shape[0]
    head_count = queries.shape[1]
    head_dim = queries.shape[2]
    block_rows = min(512, seq_len)
    block_count = seq_len // block_rows
    score_scale = 1.0 / math.sqrt(head_dim)
    token_index = jnp.arange(seq_len, dtype=jnp.int32)

    def one_block(inputs):
        query_block, segment_block, index_block = inputs
        scores = jnp.einsum('qhd,khd->hqk', query_block, all_keys, precision=precise) * score_scale
        scores = low_back(scores)
        allowed = (segment_block[:, None] == segment[None, :]) & (index_block[:, None] >= token_index[None, :])
        scores = jnp.where(allowed[None], scores, -1e+30)
        row_max = lax.optimization_barrier(jnp.max(scores, -1, keepdims=True))
        exp_scores = jnp.exp(scores - row_max)
        softmax_out = exp_scores / lax.optimization_barrier(jnp.sum(exp_scores, -1, keepdims=True))
        return jnp.einsum('hqk,khd->qhd', low(softmax_out), values, precision=precise)
    outcome = lax.map(jax.checkpoint(one_block), (queries.reshape(block_count, block_rows, head_count, head_dim), segment.reshape(block_count, block_rows), token_index.reshape(block_count, block_rows)))
    return outcome.reshape(seq_len, head_count, head_dim)

def forward(block_in, params, segment, position):
    gain_one, shift_one, gain_two, shift_two, w_qkv, b_qkv, w_out, b_out, w_fc1, b_fc1, w_fc2, b_fc2 = params
    seq_len = block_in.shape[0]
    model_width = block_in.shape[1]
    head_count = w_qkv.shape[1]
    head_dim = w_qkv.shape[3]
    normed_one = low(layer_norm(block_in, gain_one, shift_one))
    normed_two = low(layer_norm(block_in, gain_two, shift_two))
    projected = jnp.dot(normed_one, w_qkv.reshape(model_width, head_count * 3 * head_dim), precision=precise) + b_qkv.reshape(-1)
    projected = low_back(projected).reshape(seq_len, head_count, 3, head_dim)
    cos_table, sin_table = rope_tables(position, ROT)
    queries = low(rotate(projected[:, :, 0], cos_table, sin_table, ROT))
    all_keys = low(rotate(projected[:, :, 1], cos_table, sin_table, ROT))
    values = low(projected[:, :, 2])
    attended = low(low_back(attention(queries, all_keys, values, segment)))
    branch = jnp.dot(attended.reshape(seq_len, head_count * head_dim), w_out.reshape(head_count * head_dim, model_width), precision=precise)
    hidden = low_back(jnp.dot(normed_two, w_fc1, precision=precise) + b_fc1)
    activated = low(jax.nn.gelu(hidden, approximate=False))
    branch = branch + jnp.dot(activated, w_fc2, precision=precise)
    return block_in + branch + b_out + b_fc2

def reference(tokens, out_grad, segment_ids, positions, norm1_gain, norm1_bias, norm2_gain, norm2_bias, qkv_weight, qkv_bias, out_weight, out_bias, fc1_weight, fc1_bias, fc2_weight, fc2_bias):
    params = tuple((item.astype(jnp.float32) for item in (norm1_gain, norm1_bias, norm2_gain, norm2_bias, qkv_weight, qkv_bias, out_weight, out_bias, fc1_weight, fc1_bias, fc2_weight, fc2_bias)))
    seq_count = tokens.shape[0] // SEQ
    model_width = tokens.shape[1]
    inputs_all = tokens.astype(jnp.float32).reshape(seq_count, SEQ, model_width)
    cotangents = out_grad.astype(jnp.float32).reshape(seq_count, SEQ, model_width)
    segments_all = segment_ids.reshape(seq_count, SEQ)
    positions_all = positions.reshape(seq_count, SEQ)

    def one_sequence(grad_total, inputs):
        block_in, cotangent, segment, position = inputs

        def apply_layer(layer_in, layer_params):
            return forward(layer_in, layer_params, segment, position)
        result, pullback = jax.vjp(apply_layer, block_in, params)
        input_grad, param_grads = pullback(cotangent)
        new_total = tuple((left_item + right_item for left_item, right_item in zip(grad_total, param_grads)))
        return (new_total, (result.astype(jnp.bfloat16), input_grad.astype(jnp.bfloat16)))
    zero_grads = tuple((jnp.zeros_like(item) for item in params))
    grad_total, (results, input_grads) = lax.scan(one_sequence, zero_grads, (inputs_all, cotangents, segments_all, positions_all))
    return (results.reshape(tokens.shape), input_grads.reshape(tokens.shape), grad_total[0], grad_total[1], grad_total[2], grad_total[3], grad_total[4], grad_total[5], grad_total[6], grad_total[7], grad_total[8], grad_total[9], grad_total[10], grad_total[11])
```

```python
import math

import jax
import jax.numpy as jnp
from jax import lax
from jax.experimental import pallas as pl
from jax.experimental.pallas import tpu as pltpu
from jax.sharding import PartitionSpec as P

ROT = 64
MOST = 2000
EPSILON = 1e-05
BF16 = jnp.bfloat16
F32 = jnp.float32
MESH = pl.DeviceIdType.MESH


def shifted(x, axis, by):
    length = lax.axis_size(axis)
    pairs = [(i, i + by) for i in range(length) if 0 <= i + by < length]
    return lax.ppermute(x, axis, pairs)


def swapped(x, axis, bit):
    length = lax.axis_size(axis)
    return lax.ppermute(x, axis, [(i, i ^ (1 << bit)) for i in range(length)])


def dot_rows(first, second):
    return lax.dot_general(first, second, (((0,), (0,)), ((), ())), preferred_element_type=F32)


def dot_cols(first, second):
    return lax.dot_general(first, second, (((1,), (1,)), ((), ())), preferred_element_type=F32)


def dot(first, second):
    return jnp.dot(first, second, preferred_element_type=F32)


def cost(flops, bytes_accessed):
    return pl.CostEstimate(flops=int(flops), bytes_accessed=int(bytes_accessed), transcendentals=0)


def params(*semantics):
    return pltpu.CompilerParams(dimension_semantics=semantics, vmem_limit_bytes=60 << 20)


def moments(values):
    average = jnp.mean(values, -1, keepdims=True)
    centered = values - average
    variance = jnp.mean(centered * centered, -1, keepdims=True)
    return average, lax.rsqrt(variance + EPSILON)


def rope_tables(position, lanes):
    half = ROT // 2
    frequency = jnp.power(F32(10000.0), -jnp.arange(half, dtype=F32) / F32(half))
    angles = position.astype(F32)[:, None] * frequency[None, :]
    cosine, sine = jnp.cos(angles), jnp.sin(angles)
    rows = position.shape[0]
    ones = jnp.ones((rows, lanes - ROT), F32)
    return (
        jnp.concatenate([cosine, cosine, ones], 1),
        jnp.concatenate([-sine, sine, 0 * ones], 1),
    )


def turn(values, cos_block, sin_block):
    lane = lax.broadcasted_iota(jnp.int32, values.shape, 1)
    half = ROT // 2
    up = pltpu.roll(values, values.shape[1] - half, 1)
    down = pltpu.roll(values, half, 1)
    return values * cos_block + jnp.where(lane < half, up, down) * sin_block


def project_kernel(
    heads, head_dim, x_ref, g1_ref, b1_ref, g2_ref, b2_ref, w_ref, bias_ref, cos_ref, sin_ref,
    n1_ref, n2_ref, q_ref, kv_ref, mean_ref, inverse_ref,
):
    x = x_ref[...].astype(F32)
    average, inverse = moments(x)
    mean_ref[...] = average
    inverse_ref[...] = inverse
    standard = (x - average) * inverse
    n1 = (standard * g1_ref[...] + b1_ref[...]).astype(BF16)
    n1_ref[...] = n1
    n2_ref[...] = (standard * g2_ref[...] + b2_ref[...]).astype(BF16)
    cos_block, sin_block = cos_ref[...], sin_ref[...]
    width = heads * head_dim
    lanes = cos_block.shape[1]
    for part in range(3):
        low = part * width
        projected = dot(n1, w_ref[:, low : low + width]) + bias_ref[:, low : low + width]
        if part == 2:
            kv_ref[:, width:] = projected.astype(BF16)
            continue
        for head in range(heads):
            at = head * head_dim
            turned = turn(projected[:, at : at + lanes], cos_block, sin_block)
            rest = projected[:, at + lanes : at + head_dim]
            if part == 0:
                scale = 1.0 / math.sqrt(head_dim)
                q_ref[:, at : at + lanes] = (turned * scale).astype(BF16)
                q_ref[:, at + lanes : at + head_dim] = (rest * scale).astype(BF16)
            else:
                kv_ref[:, at : at + lanes] = turned.astype(BF16)
                kv_ref[:, at + lanes : at + head_dim] = rest.astype(BF16)


def project(x, gain1, bias1, gain2, bias2, weight, bias, cos_table, sin_table, heads, head_dim):
    rows, depth = x.shape
    block = min(256, rows)
    width = heads * head_dim
    whole = lambda i: (0, 0)
    by_row = lambda i: (i, 0)
    return pl.pallas_call(
        lambda *refs: project_kernel(heads, head_dim, *refs),
        name="project",
        grid=(rows // block,),
        in_specs=[
            pl.BlockSpec((block, depth), by_row),
            *[pl.BlockSpec((1, depth), whole)] * 4,
            pl.BlockSpec((depth, 3 * width), whole, pipeline_mode=pl.Buffered(1)),
            pl.BlockSpec((1, 3 * width), whole),
            pl.BlockSpec((block, cos_table.shape[1]), by_row),
            pl.BlockSpec((block, cos_table.shape[1]), by_row),
        ],
        out_specs=[
            pl.BlockSpec((block, depth), by_row),
            pl.BlockSpec((block, depth), by_row),
            pl.BlockSpec((block, width), by_row),
            pl.BlockSpec((block, 2 * width), by_row),
            pl.BlockSpec((block, 1), by_row),
            pl.BlockSpec((block, 1), by_row),
        ],
        out_shape=[
            jax.ShapeDtypeStruct((rows, depth), BF16),
            jax.ShapeDtypeStruct((rows, depth), BF16),
            jax.ShapeDtypeStruct((rows, width), BF16),
            jax.ShapeDtypeStruct((rows, 2 * width), BF16),
            jax.ShapeDtypeStruct((rows, 1), F32),
            jax.ShapeDtypeStruct((rows, 1), F32),
        ],
        compiler_params=params("arbitrary"),
        cost_estimate=cost(2 * rows * depth * 3 * width, 2 * (3 * rows * depth + 3 * depth * width)),
    )(x, gain1, bias1, gain2, bias2, weight, bias, cos_table, sin_table)


def up_kernel(x_ref, w_ref, b_ref, act_ref, slope_ref):
    hidden = dot(x_ref[...], w_ref[...]) + b_ref[...]
    phi = (1.0 + lax.erf(hidden * F32(math.sqrt(0.5)))) * 0.5
    act_ref[...] = (hidden * phi).astype(BF16)
    density = jnp.exp(hidden * hidden * -0.5) * F32(1.0 / math.sqrt(2.0 * math.pi))
    slope_ref[...] = phi + hidden * density


def up(x, weight, bias):
    rows, depth = x.shape
    width = weight.shape[1]
    bm, bn = min(256, rows), min(512, width)
    return pl.pallas_call(
        up_kernel,
        name="up",
        grid=(width // bn, rows // bm),
        in_specs=[
            pl.BlockSpec((bm, depth), lambda j, i: (i, 0)),
            pl.BlockSpec((depth, bn), lambda j, i: (0, j)),
            pl.BlockSpec((1, bn), lambda j, i: (0, j)),
        ],
        out_specs=[pl.BlockSpec((bm, bn), lambda j, i: (i, j))] * 2,
        out_shape=[
            jax.ShapeDtypeStruct((rows, width), BF16),
            jax.ShapeDtypeStruct((rows, width), F32),
        ],
        compiler_params=params("arbitrary", "arbitrary"),
        cost_estimate=cost(2 * rows * depth * width, 2 * depth * width + 6 * rows * width),
    )(x, weight, bias)


def hidden_kernel(g_ref, w_ref, slope_ref, out_ref, sum_ref):
    grad = dot_cols(g_ref[...], w_ref[...])
    low = (grad * slope_ref[...]).astype(BF16)
    out_ref[...] = low
    total = jnp.sum(low.astype(F32), 0, keepdims=True)

    @pl.when(pl.program_id(1) == 0)
    def _():
        sum_ref[...] = total

    @pl.when(pl.program_id(1) > 0)
    def _():
        sum_ref[...] += total


def hidden_grads(grad, weight, slope):
    rows, depth = grad.shape
    width = weight.shape[0]
    bm, bn = min(256, rows), min(512, width)
    return pl.pallas_call(
        hidden_kernel,
        name="hidden_grads",
        grid=(width // bn, rows // bm),
        in_specs=[
            pl.BlockSpec((bm, depth), lambda j, i: (i, 0)),
            pl.BlockSpec((bn, depth), lambda j, i: (j, 0)),
            pl.BlockSpec((bm, bn), lambda j, i: (i, j)),
        ],
        out_specs=[
            pl.BlockSpec((bm, bn), lambda j, i: (i, j)),
            pl.BlockSpec((1, bn), lambda j, i: (0, j)),
        ],
        out_shape=[
            jax.ShapeDtypeStruct((rows, width), BF16),
            jax.ShapeDtypeStruct((1, width), F32),
        ],
        compiler_params=params("arbitrary", "arbitrary"),
        cost_estimate=cost(2 * rows * depth * width, 2 * depth * width + 6 * rows * width),
    )(grad, weight, slope)


def attention_kernel(heads, head_dim, parts, bk, first_ref, q_ref, do_ref, start_ref, *refs):
    kv_parts, refs = refs[:parts], refs[parts:]
    att_ref, dq_ref, refs = refs[0], refs[1], refs[2:]
    grad_parts, (kv_ref, dkv_ref, s_ref, dp_ref, o_ref, sems) = refs[:parts], refs[parts:]
    block = pl.program_id(0)
    bq = q_ref.shape[0]
    width = heads * head_dim
    rows_each = kv_ref.shape[0] // parts
    ahead = rows_each * (parts - 1)
    low = first_ref[block]
    high = (ahead + (block + 1) * bq + bk - 1) // bk
    row = ahead + block * bq + lax.broadcasted_iota(jnp.int32, (bq, 1), 0)
    start = start_ref[...]
    lane = lax.broadcasted_iota(jnp.int32, (bq, bk), 1)
    chunks = bk // 128

    @pl.when(block == 0)
    def _():
        copies = [
            pltpu.make_async_copy(
                part, kv_ref.at[pl.ds(k * rows_each, rows_each)], sems.at[k]
            )
            for k, part in enumerate(kv_parts)
        ]
        for copy in copies:
            copy.start()

        def clear(j, carry):
            dkv_ref[pl.ds(pl.multiple_of(j * 128, 128), 128), :] = jnp.zeros((128, 2 * width), F32)
            return carry

        lax.fori_loop(0, dkv_ref.shape[0] // 128, clear, 0)
        for copy in copies:
            copy.wait()

    for head in range(heads):
        at = head * head_dim
        q = q_ref[:, at : at + head_dim]
        do = do_ref[:, at : at + head_dim]

        def rows_of(j):
            return pl.ds(pl.multiple_of(j * bk, bk), bk)

        def scores(j, best):
            s = dot_cols(q, kv_ref[rows_of(j), at : at + head_dim])
            column = j * bk + lane
            s = jnp.where((column >= start) & (column <= row), s, -1e30)
            s_ref[j] = s
            for c in range(chunks):
                best = jnp.maximum(best, s[:, c * 128 : (c + 1) * 128])
            return best

        best = lax.fori_loop(low, high, scores, jnp.full((bq, 128), -1e30, F32))
        best = jnp.max(best, 1, keepdims=True)

        def weigh(j, carry):
            total, mixed = carry
            e = jnp.exp(s_ref[j] - best)
            dp = dot_cols(do, kv_ref[rows_of(j), width + at : width + at + head_dim])
            s_ref[j] = e
            dp_ref[j] = dp
            both = e * dp
            for c in range(chunks):
                total = total + e[:, c * 128 : (c + 1) * 128]
                mixed = mixed + both[:, c * 128 : (c + 1) * 128]
            return total, mixed

        zero = jnp.zeros((bq, 128), F32)
        total, mixed = lax.fori_loop(low, high, weigh, (zero, zero))
        total = jnp.sum(total, 1, keepdims=True)
        scale = 1.0 / total
        delta = jnp.sum(mixed, 1, keepdims=True) * scale
        o_ref[...] = jnp.zeros_like(o_ref)

        def spread(j, carry):
            rows = rows_of(j)
            p = s_ref[j] * scale
            p_low = p.astype(BF16)
            ds = (p * (dp_ref[j] - delta)).astype(BF16)
            k = kv_ref[rows, at : at + head_dim]
            v = kv_ref[rows, width + at : width + at + head_dim]
            o_ref[:, :head_dim] += dot(p_low, v)
            o_ref[:, head_dim:] += dot(ds, k)
            dkv_ref[rows, at : at + head_dim] += dot_rows(ds, q)
            dkv_ref[rows, width + at : width + at + head_dim] += dot_rows(p_low, do)
            return carry

        lax.fori_loop(low, high, spread, 0)
        att_ref[:, at : at + head_dim] = o_ref[:, :head_dim].astype(BF16)
        dq_ref[:, at : at + head_dim] = o_ref[:, head_dim:] * (1.0 / math.sqrt(head_dim))

    @pl.when(block == pl.num_programs(0) - 1)
    def _():
        for k, part in enumerate(grad_parts):
            part[...] = dkv_ref[k * rows_each : (k + 1) * rows_each, :].astype(part.dtype)


def attention(q, kv_parts, do, positions, heads, head_dim):
    rows, width = q.shape
    parts = len(kv_parts)
    total = rows * parts
    bq = min(256, rows)
    bk = 256
    start = jnp.arange(rows, dtype=jnp.int32) - positions + (total - rows)
    first = start[::bq] // bk
    by_row = lambda i, f: (i, 0)
    whole = lambda i, f: (0, 0)
    part_types = [BF16] + [F32] * (parts - 1)
    return pl.pallas_call(
        lambda *refs: attention_kernel(heads, head_dim, parts, bk, *refs),
        name="attention",
        grid_spec=pltpu.PrefetchScalarGridSpec(
            num_scalar_prefetch=1,
            grid=(rows // bq,),
            in_specs=[
                pl.BlockSpec((bq, width), by_row),
                pl.BlockSpec((bq, width), by_row),
                pl.BlockSpec((bq, 1), by_row),
                *[pl.BlockSpec(memory_space=pl.ANY)] * parts,
            ],
            out_specs=[
                pl.BlockSpec((bq, width), by_row),
                pl.BlockSpec((bq, width), by_row),
                *[pl.BlockSpec((rows, 2 * width), whole, pipeline_mode=pl.Buffered(1))] * parts,
            ],
            scratch_shapes=[
                pltpu.VMEM((total, 2 * width), BF16),
                pltpu.VMEM((total, 2 * width), F32),
                pltpu.VMEM((total // bk, bq, bk), F32),
                pltpu.VMEM((total // bk, bq, bk), F32),
                pltpu.VMEM((bq, 2 * head_dim), F32),
                pltpu.SemaphoreType.DMA((parts,)),
            ],
        ),
        out_shape=[
            jax.ShapeDtypeStruct((rows, width), BF16),
            jax.ShapeDtypeStruct((rows, width), F32),
            *[jax.ShapeDtypeStruct((rows, 2 * width), kind) for kind in part_types],
        ],
        compiler_params=params("arbitrary"),
        cost_estimate=cost(12 * rows * MOST * width, 8 * total * width),
    )(first, q, do, start[:, None], *kv_parts)


def turn_back_kernel(heads, head_dim, dq_ref, dkv_ref, extra_ref, cos_ref, sin_ref, out_ref, sum_ref):
    cos_block, sin_block = cos_ref[...], -sin_ref[...]
    lanes = cos_block.shape[1]
    width = heads * head_dim
    for part in range(3):
        for head in range(heads):
            at = head * head_dim
            if part == 0:
                grad = dq_ref[:, at : at + head_dim]
            else:
                low = (part - 1) * width + at
                grad = dkv_ref[:, low : low + head_dim] + extra_ref[:, low : low + head_dim].astype(F32)
            to = part * width + at
            if part < 2:
                first = turn(grad[:, :lanes], cos_block, sin_block)
                out_ref[:, to : to + lanes] = first.astype(BF16)
                out_ref[:, to + lanes : to + head_dim] = grad[:, lanes:].astype(BF16)
            else:
                out_ref[:, to : to + head_dim] = grad.astype(BF16)
    total = jnp.sum(out_ref[...].astype(F32), 0, keepdims=True)

    @pl.when(pl.program_id(0) == 0)
    def _():
        sum_ref[...] = total

    @pl.when(pl.program_id(0) > 0)
    def _():
        sum_ref[...] += total


def turn_back(dq, dkv, extra, cos_table, sin_table, heads, head_dim):
    rows, width = dq.shape
    block = min(256, rows)
    by_row = lambda i: (i, 0)
    return pl.pallas_call(
        lambda *refs: turn_back_kernel(heads, head_dim, *refs),
        name="turn_back",
        grid=(rows // block,),
        in_specs=[
            pl.BlockSpec((block, width), by_row),
            pl.BlockSpec((block, 2 * width), by_row),
            pl.BlockSpec((block, 2 * width), by_row),
            pl.BlockSpec((block, cos_table.shape[1]), by_row),
            pl.BlockSpec((block, cos_table.shape[1]), by_row),
        ],
        out_specs=[
            pl.BlockSpec((block, 3 * width), by_row),
            pl.BlockSpec((1, 3 * width), lambda i: (0, 0)),
        ],
        out_shape=[
            jax.ShapeDtypeStruct((rows, 3 * width), BF16),
            jax.ShapeDtypeStruct((1, 3 * width), F32),
        ],
        compiler_params=params("arbitrary"),
        cost_estimate=cost(0, rows * width * 20),
    )(dq, dkv, extra, cos_table, sin_table)


def input_kernel(
    dqkv_ref, w1_ref, g1_ref, hg_ref, w2_ref, g2_ref, x_ref, mean_ref, inverse_ref,
    low_ref, own_ref, sums_ref,
):
    one = dot_cols(dqkv_ref[...], w1_ref[...])
    two = dot_cols(hg_ref[...], w2_ref[...])
    combined = one * g1_ref[...] + two * g2_ref[...]
    low_ref[...] = combined.astype(BF16)

    @pl.when(pl.program_id(1) == lax.axis_index("tensor"))
    def _():
        own_ref[...] = combined

    standard = (x_ref[...].astype(F32) - mean_ref[...]) * inverse_ref[...]
    add = lambda v: jnp.sum(v, 0, keepdims=True)
    sums = jnp.concatenate([add(one * standard), add(one), add(two * standard), add(two)], 0)

    @pl.when(pl.program_id(1) == 0)
    def _():
        sums_ref[...] = sums

    @pl.when(pl.program_id(1) > 0)
    def _():
        sums_ref[...] += sums


def input_grads(dqkv, w1, gain1, hg, w2, gain2, x, mean, inverse, own_rows):
    rows, depth = x.shape
    bm, bn = own_rows, min(512, depth)
    by_row = lambda j, i: (i, 0)
    by_column = lambda j, i: (j, 0)
    tile = lambda j, i: (i, j)
    column = lambda j, i: (0, j)
    return pl.pallas_call(
        input_kernel,
        name="input_grads",
        grid=(depth // bn, rows // bm),
        in_specs=[
            pl.BlockSpec((bm, dqkv.shape[1]), by_row),
            pl.BlockSpec((bn, w1.shape[1]), by_column),
            pl.BlockSpec((1, bn), column),
            pl.BlockSpec((bm, hg.shape[1]), by_row),
            pl.BlockSpec((bn, w2.shape[1]), by_column),
            pl.BlockSpec((1, bn), column),
            pl.BlockSpec((bm, bn), tile),
            pl.BlockSpec((bm, 1), by_row),
            pl.BlockSpec((bm, 1), by_row),
        ],
        out_specs=[
            pl.BlockSpec((bm, bn), tile),
            pl.BlockSpec((bm, bn), column),
            pl.BlockSpec((4, bn), column),
        ],
        out_shape=[
            jax.ShapeDtypeStruct((rows, depth), BF16),
            jax.ShapeDtypeStruct((own_rows, depth), F32),
            jax.ShapeDtypeStruct((4, depth), F32),
        ],
        compiler_params=params("arbitrary", "arbitrary"),
        cost_estimate=cost(
            2 * rows * depth * (w1.shape[1] + w2.shape[1]),
            2 * depth * (w1.shape[1] + w2.shape[1]) + 6 * rows * depth,
        ),
    )(dqkv, w1, gain1, hg, w2, gain2, x, mean, inverse)


def spread_kernel(heads, head_dim, in_ref, out_ref):
    for head in range(heads):
        block = in_ref[head * head_dim : (head + 1) * head_dim, :].astype(F32)
        out_ref[:, 0, head, :] = block.T


def spread(stacked, heads, head_dim):
    depth = stacked.shape[1]
    block = 256
    return pl.pallas_call(
        lambda *refs: spread_kernel(heads, head_dim, *refs),
        name="spread",
        grid=(depth // block, 3),
        in_specs=[pl.BlockSpec((heads * head_dim, block), lambda i, j: (j, i))],
        out_specs=pl.BlockSpec((block, 1, heads, head_dim), lambda i, j: (i, j, 0, 0)),
        out_shape=jax.ShapeDtypeStruct((depth, 3, heads, head_dim), F32),
        compiler_params=params("arbitrary", "arbitrary"),
        cost_estimate=cost(0, 6 * stacked.size),
    )(stacked)


def reduce_kernel(plan, chunks, bits, tensor, *refs):
    refs = list(refs)
    take = lambda count: [refs.pop(0) for _ in range(count)]
    a_refs = take(len(plan))
    b_refs = take(3)
    d_ref, own_ref, vec_ref, out_ref, dsum_ref, total_ref = take(6)
    abuf, full, r0, ag = take(4)
    kept, sent, got = take(bits - 1), take(bits - 1), take(bits - 1)
    dgot, vgot, vsend, vnow = take(4)
    a_sem, o_sem, send_sem, recv_sem, d_send, d_recv, v_send, v_recv = take(8)
    index, me = lax.axis_index("dp"), lax.axis_index("tensor")
    deep, wide = full.shape[1], full.shape[2]
    slots, ring = got[0].shape[0], ag.shape[0]

    def bit_of(bit):
        return (index // (1 << bit)) % 2

    def partner(bit):
        return index + (1 << bit) * (1 - 2 * bit_of(bit))

    barrier = pltpu.get_barrier_semaphore()
    for bit in range(bits):
        pl.semaphore_signal(barrier, inc=1, device_id={"dp": partner(bit)}, device_id_type=MESH)
    for k in range(1, tensor):
        other = lax.rem(me + k, tensor)
        pl.semaphore_signal(barrier, inc=1, device_id={"tensor": other}, device_id_type=MESH)
    pl.semaphore_wait(barrier, bits + tensor - 1)

    own_rows = own_ref.shape[0]

    def d_copy(k):
        other = lax.rem(me + k, tensor)
        return pltpu.make_async_remote_copy(
            src_ref=d_ref.at[pl.ds(pl.multiple_of(other * own_rows, own_rows), own_rows)],
            dst_ref=dgot.at[k - 1],
            send_sem=d_send.at[k - 1],
            recv_sem=d_recv.at[k - 1],
            device_id={"tensor": other},
            device_id_type=MESH,
        )

    def v_copy(k, to, slot):
        return pltpu.make_async_remote_copy(
            src_ref=vec_ref,
            dst_ref=vgot.at[slot],
            send_sem=v_send.at[k - 1],
            recv_sem=v_recv.at[slot],
            device_id={"tensor": to},
            device_id_type=MESH,
        )

    def v_step(bit):
        return pltpu.make_async_remote_copy(
            src_ref=vsend.at[bit],
            dst_ref=vnow.at[bit],
            send_sem=v_send.at[tensor + bit],
            recv_sem=v_recv.at[tensor + bit],
            device_id={"dp": partner(bit)},
            device_id_type=MESH,
        )

    def fetch_copy(item, c):
        column = pl.multiple_of((c - plan[item][0]) * deep, deep)
        slot = lax.rem(c, 2)
        return pltpu.make_async_copy(
            a_refs[item].at[:, pl.ds(column, deep)], abuf.at[slot], a_sem.at[slot]
        )

    def on_items(c, act):
        for item, (first, count, _) in enumerate(plan):
            @pl.when((c >= first) & (c < first + count))
            def _():
                act(item)

    even, odd = list(range(bits)), [0, *range(2, bits), 1]

    def mixed(level, parity, of):
        first, second = of(even[level]), of(odd[level])
        return first + parity * (second - first)

    def base(level, parity):
        row = 0
        for k in range(level):
            row = row + mixed(k, parity, bit_of) * (deep >> (k + 1))
        return row

    def down_copy(level, c):
        parity = lax.rem(c, 2)
        half = deep >> (level + 1)
        if level == 0:
            row = pl.multiple_of((1 - bit_of(0)) * half, half)
            source, target = full.at[parity, pl.ds(row, half)], r0.at[parity]
        else:
            source, target = sent[level - 1].at[parity], got[level - 1].at[lax.rem(c, slots)]
        return pltpu.make_async_remote_copy(
            src_ref=source,
            dst_ref=target,
            send_sem=send_sem.at[level, lax.rem(c, ring)],
            recv_sem=recv_sem.at[level, lax.rem(c, ring)],
            device_id={"dp": mixed(level, parity, partner)},
            device_id_type=MESH,
        )

    def up_copy(level, c, incoming=False):
        parity, slot = lax.rem(c, 2), lax.rem(c, ring)
        size = deep >> (level + 1)
        row = base(level + 1, parity)
        rows = pl.ds(pl.multiple_of(row, size), size)
        return pltpu.make_async_remote_copy(
            src_ref=ag.at[slot, rows],
            dst_ref=ag.at[slot, rows],
            send_sem=send_sem.at[bits + level, slot],
            recv_sem=recv_sem.at[bits + level, slot],
            device_id={"dp": mixed(level, parity, partner)},
            device_id_type=MESH,
        )

    def out_copy(c):
        slot = lax.rem(c, ring)
        row = pl.multiple_of(c * deep, deep)
        return pltpu.make_async_copy(ag.at[slot], out_ref.at[pl.ds(row, deep)], o_sem.at[slot])

    def multiply(c):
        slot = lax.rem(c, 2)

        def with_item(item):
            fetch_copy(item, c).wait()
            left = abuf[slot].T
            right = b_refs[plan[item][2]]
            step = min(512, wide)
            for column in range(0, wide, step):
                full[slot, :, column : column + step] = dot(left, right[:, column : column + step])

        on_items(c, with_item)
        down_copy(0, c).start()

    def halve(level, c):
        parity = lax.rem(c, 2)
        down_copy(level - 1, c).wait()
        size = deep >> level
        half = size // 2
        if level < bits:
            bit = mixed(level, parity, bit_of)
            keep = pl.multiple_of(bit * half, half)
            give = pl.multiple_of((1 - bit) * half, half)
            pieces = ((keep, True), (give, False))
        else:
            pieces = ((0, True),)
            half = size
        for row, stays in pieces:
            if level == 1:
                mine = full[parity, pl.ds(pl.multiple_of(bit_of(0) * size + row, half), half)]
                value = mine + r0[parity, pl.ds(row, half)]
            else:
                mine = kept[level - 2][parity, pl.ds(row, half)]
                value = mine + got[level - 2][lax.rem(c, slots), pl.ds(row, half)].astype(F32)
            if level == bits:
                at = pl.multiple_of(base(bits, parity), size)
                ag[lax.rem(c, ring), pl.ds(at, size)] = value.astype(BF16)
            elif stays:
                kept[level - 1][parity] = value
            else:
                sent[level - 1][parity] = value.astype(BF16)
        if level < bits:
            down_copy(level, c).start()
        else:
            up_copy(bits - 1, c).start()

    def widen(level, c):
        up_copy(level, c).wait()
        up_copy(level - 1, c).start()

    def finish(c):
        up_copy(0, c).wait()
        out_copy(c).start()

    on_items(0, lambda item: fetch_copy(item, 0).start())
    for k in range(1, tensor):
        v_copy(k, lax.rem(me + k, tensor), me).start()
    for k in range(1, tensor):
        d_copy(k).start()
    vgot[me] = vec_ref[...]

    def stage(t, delay, act):
        c = t - delay

        @pl.when((c >= 0) & (c < chunks))
        def _():
            act(c)

    def iteration(t, carry):
        @pl.when(t + 1 < chunks)
        def _():
            on_items(t + 1, lambda item: fetch_copy(item, t + 1).start())

        stage(t, 2 * bits + 1, lambda c: out_copy(c).wait())
        stage(t, 2 * bits, finish)
        for level in range(1, bits):
            stage(t, 2 * bits - level, lambda c, level=level: widen(level, c))
        for level in range(bits, 0, -1):
            stage(t, level, lambda c, level=level: halve(level, c))
        stage(t, 0, multiply)

        @pl.when(t == 1)
        def _():
            for k in range(1, tensor):
                other = lax.rem(me + k, tensor)
                v_copy(k, other, me).wait_send()
                v_copy(k, other, other).wait_recv()
            lane = lax.broadcasted_iota(jnp.int32, vec_ref.shape, 0)
            both = vgot[0]
            for k in range(1, tensor):
                both = both + vgot[k]
            vsend[0] = jnp.where(lane < 5, both, vec_ref[...])
            v_step(0).start()

        for bit in range(bits):
            @pl.when(t == 2 + bit)
            def _():
                v_step(bit).wait()
                both = vsend[bit] + vnow[bit]
                if bit + 1 < bits:
                    vsend[bit + 1] = both
                    v_step(bit + 1).start()
                else:
                    total_ref[...] = both

        return carry

    lax.fori_loop(0, chunks + 2 * bits + 2, iteration, 0)
    summed_rows = own_ref[...]
    for k in range(1, tensor):
        d_copy(k).wait()
        summed_rows = summed_rows + dgot[k - 1].astype(F32)
    dsum_ref[...] = summed_rows


def reduce_grads(items, rights, d_low, d_own, vectors, bits, tensor):
    deep = 256
    rows, wide = rights[0].shape
    plan, first = [], 0
    for left, which in items:
        count = left.shape[1] // deep
        plan.append((first, count, which))
        first += count
    chunks, ring, slots = first, 8, 4
    halves_of = [deep >> (level + 1) for level in range(1, bits)]
    own_rows = d_own.shape[0]
    hbm = pl.BlockSpec(memory_space=pl.ANY)
    vmem = pl.BlockSpec(memory_space=pltpu.VMEM)
    return pl.pallas_call(
        lambda *refs: reduce_kernel(plan, chunks, bits, tensor, *refs),
        name="reduce_grads",
        in_specs=[hbm] * len(items) + [vmem] * 3 + [hbm, vmem, vmem],
        out_specs=[hbm, vmem, vmem],
        out_shape=[
            jax.ShapeDtypeStruct((chunks * deep, wide), BF16),
            jax.ShapeDtypeStruct((own_rows, wide), F32),
            jax.ShapeDtypeStruct(vectors.shape, F32),
        ],
        scratch_shapes=[
            pltpu.VMEM((2, rows, deep), BF16),
            pltpu.VMEM((2, deep, wide), F32),
            pltpu.VMEM((2, deep // 2, wide), F32),
            pltpu.VMEM((ring, deep, wide), BF16),
            *[pltpu.VMEM((2, half, wide), F32) for half in halves_of],
            *[pltpu.VMEM((2, half, wide), BF16) for half in halves_of],
            *[pltpu.VMEM((slots, half, wide), BF16) for half in halves_of],
            pltpu.VMEM((tensor - 1, own_rows, wide), BF16),
            pltpu.VMEM((tensor, *vectors.shape), F32),
            pltpu.VMEM((bits, *vectors.shape), F32),
            pltpu.VMEM((bits, *vectors.shape), F32),
            pltpu.SemaphoreType.DMA((2,)),
            pltpu.SemaphoreType.DMA((ring,)),
            pltpu.SemaphoreType.DMA((2 * bits, ring)),
            pltpu.SemaphoreType.DMA((2 * bits, ring)),
            pltpu.SemaphoreType.DMA((tensor - 1,)),
            pltpu.SemaphoreType.DMA((tensor - 1,)),
            pltpu.SemaphoreType.DMA((tensor + bits,)),
            pltpu.SemaphoreType.DMA((tensor + bits,)),
        ],
        compiler_params=pltpu.CompilerParams(
            collective_id=0, has_side_effects=True, vmem_limit_bytes=62 << 20
        ),
        cost_estimate=cost(2 * rows * chunks * deep * wide, 8 * chunks * deep * wide),
    )(*[left for left, _ in items], *rights, d_low, d_own, vectors)


def body(
    tokens, out_grad, segment_ids, positions, norm1_gain, norm1_bias, norm2_gain, norm2_bias,
    qkv_weight, qkv_bias, out_weight, out_bias, fc1_weight, fc1_bias, fc2_weight, fc2_bias,
):
    model_width, heads, _, head_dim = qkv_weight.shape
    width = heads * head_dim
    hidden_width = fc1_weight.shape[1]
    own_count = tokens.shape[0]
    tie = lax.optimization_barrier
    row = lambda v: v.reshape(1, -1).astype(F32)
    rows_all = lax.all_gather(tokens, "tensor", axis=0, tiled=True)
    grads_all = lax.all_gather(out_grad, "tensor", axis=0, tiled=True)
    row_count = rows_all.shape[0]
    flat_qkv = jnp.transpose(qkv_weight, (0, 2, 1, 3)).reshape(model_width, 3 * width)
    flat_bias = jnp.transpose(qkv_bias, (1, 0, 2)).reshape(1, 3 * width).astype(F32)
    flat_out = out_weight.reshape(width, model_width)
    cos_table, sin_table = rope_tables(positions, 128)
    normed_one, normed_two, queries, kv_own, mean, inverse = project(
        rows_all, row(norm1_gain), row(norm1_bias), row(norm2_gain), row(norm2_bias),
        flat_qkv, flat_bias, cos_table, sin_table, heads, head_dim,
    )
    reach = (MOST - 2) // row_count + 1
    kv_parts = [kv_own]
    for _ in range(reach):
        kv_parts.insert(0, shifted(kv_parts[0], "dp", 1))
    activated, slope = up(normed_two, fc1_weight, row(fc1_bias))
    forward = dot(activated, fc2_weight)
    grads_all, activated, slope, forward = tie((grads_all, activated, slope, forward))

    attended_grad = dot_cols(grads_all, flat_out).astype(BF16)
    attended, query_grad, *kv_grads = attention(
        queries, kv_parts, attended_grad, positions, heads, head_dim
    )
    grads_all, attended, query_grad, *kv_grads = tie((grads_all, attended, query_grad, *kv_grads))
    partial = dot(attended, flat_out) + forward
    branch = lax.psum_scatter(partial, "tensor", scatter_dimension=0, tiled=True)
    hidden_grad, fc1_bias_grad = hidden_grads(grads_all, fc2_weight, slope)
    extra = None
    for part in kv_grads[:-1]:
        if extra is not None:
            part = (part + extra.astype(F32)).astype(BF16)
        extra = shifted(part, "dp", -1)
        extra, hidden_grad = tie((extra, hidden_grad))
    qkv_grad, qkv_bias_grad = turn_back(
        query_grad, kv_grads[-1], extra, cos_table, sin_table, heads, head_dim
    )
    d_low, d_own, sums = input_grads(
        qkv_grad, flat_qkv, row(norm1_gain), hidden_grad, fc1_weight, row(norm2_gain),
        rows_all, mean, inverse, own_count,
    )
    wide = lambda v: jnp.pad(v, ((0, 0), (0, model_width - v.shape[1])))
    own_grad = out_grad.astype(F32)
    vectors = jnp.concatenate(
        [
            sums, jnp.sum(own_grad, 0, keepdims=True), wide(fc1_bias_grad), wide(qkv_bias_grad),
            jnp.zeros((1, model_width), F32),
        ],
        0,
    )
    bits = (lax.axis_size("dp") - 1).bit_length()
    natural = hidden_width == model_width
    fc1_pair = (normed_two, hidden_grad) if natural else (hidden_grad, normed_two)
    stacked, d_sum, vectors = reduce_grads(
        [(activated, 0), (attended, 0), (fc1_pair[0], 1), (qkv_grad, 2)],
        [grads_all, fc1_pair[1], normed_one],
        d_low, d_own, vectors, bits, lax.axis_size("tensor"),
    )
    fc2_grad = stacked[:hidden_width].astype(F32)
    at = hidden_width
    out_weight_grad = stacked[at : at + width].astype(F32).reshape(heads, head_dim, model_width)
    at += width
    fc1_grad = stacked[at : at + fc1_pair[0].shape[1]].astype(F32)
    at += fc1_pair[0].shape[1]
    if not natural:
        fc1_grad = fc1_grad.T
    qkv_weight_grad = jnp.transpose(spread(stacked[at:], heads, head_dim), (0, 2, 1, 3))
    fc1_bias_grad = vectors[5, :hidden_width]
    qkv_bias_grad = vectors[6, : 3 * width].reshape(3, heads, head_dim)
    qkv_bias_grad = jnp.transpose(qkv_bias_grad, (1, 0, 2))
    own_rows = tokens.astype(F32)
    block_out = own_rows + branch + out_bias.astype(F32) + fc2_bias.astype(F32)
    own_mean, own_inverse = moments(own_rows)
    standard = (own_rows - own_mean) * own_inverse
    tokens_grad = own_grad + own_inverse * (
        d_sum
        - jnp.mean(d_sum, -1, keepdims=True)
        - standard * jnp.mean(d_sum * standard, -1, keepdims=True)
    )
    return (
        block_out.astype(BF16), tokens_grad.astype(BF16),
        vectors[0], vectors[1], vectors[2], vectors[3],
        qkv_weight_grad, qkv_bias_grad, out_weight_grad, vectors[4],
        fc1_grad, fc1_bias_grad, fc2_grad, vectors[4],
    )


def solution(mesh):
    rows = P(("dp", "tensor"), None)
    return jax.shard_map(
        body,
        mesh=mesh,
        in_specs=(
            rows, rows, P("dp"), P("dp"), P(), P(), P(), P(),
            P(None, "tensor", None, None), P("tensor", None, None), P("tensor", None, None), P(),
            P(None, "tensor"), P("tensor"), P("tensor", None), P(),
        ),
        out_specs=(
            rows, rows, P(), P(), P(), P(),
            P(None, "tensor", None, None), P("tensor", None, None), P("tensor", None, None), P(),
            P(None, "tensor"), P("tensor"), P("tensor", None), P(),
        ),
        check_vma=False,
    )
```

```python
import math

import jax
import jax.numpy as jnp
from jax import lax
from jax.experimental import pallas as pl
from jax.experimental.pallas import tpu as pltpu
from jax.sharding import PartitionSpec as P

ROT = 64
MOST = 2000
EPSILON = 1e-05
BF16 = jnp.bfloat16
F32 = jnp.float32
MESH = pl.DeviceIdType.MESH


def shifted(x, axis, by):
    length = lax.axis_size(axis)
    pairs = [(i, i + by) for i in range(length) if 0 <= i + by < length]
    return lax.ppermute(x, axis, pairs)


def swapped(x, axis, bit):
    length = lax.axis_size(axis)
    return lax.ppermute(x, axis, [(i, i ^ (1 << bit)) for i in range(length)])


def dot_rows(first, second):
    return lax.dot_general(first, second, (((0,), (0,)), ((), ())), preferred_element_type=F32)


def dot_cols(first, second):
    return lax.dot_general(first, second, (((1,), (1,)), ((), ())), preferred_element_type=F32)


def dot(first, second):
    return jnp.dot(first, second, preferred_element_type=F32)


def cost(flops, bytes_accessed):
    return pl.CostEstimate(flops=int(flops), bytes_accessed=int(bytes_accessed), transcendentals=0)


def params(*semantics):
    return pltpu.CompilerParams(dimension_semantics=semantics, vmem_limit_bytes=60 << 20)


def moments(values):
    average = jnp.mean(values, -1, keepdims=True)
    centered = values - average
    variance = jnp.mean(centered * centered, -1, keepdims=True)
    return average, lax.rsqrt(variance + EPSILON)


def rope_tables(position, lanes):
    half = ROT // 2
    frequency = jnp.power(F32(10000.0), -jnp.arange(half, dtype=F32) / F32(half))
    angles = position.astype(F32)[:, None] * frequency[None, :]
    cosine, sine = jnp.cos(angles), jnp.sin(angles)
    rows = position.shape[0]
    ones = jnp.ones((rows, lanes - ROT), F32)
    return (
        jnp.concatenate([cosine, cosine, ones], 1),
        jnp.concatenate([-sine, sine, 0 * ones], 1),
    )


def turn(values, cos_block, sin_block):
    lane = lax.broadcasted_iota(jnp.int32, values.shape, 1)
    half = ROT // 2
    up = pltpu.roll(values, values.shape[1] - half, 1)
    down = pltpu.roll(values, half, 1)
    return values * cos_block + jnp.where(lane < half, up, down) * sin_block


def project_kernel(
    heads, head_dim, x_ref, g1_ref, b1_ref, g2_ref, b2_ref, w_ref, bias_ref, cos_ref, sin_ref,
    n1_ref, n2_ref, q_ref, kv_ref, mean_ref, inverse_ref,
):
    x = x_ref[...].astype(F32)
    average, inverse = moments(x)
    mean_ref[...] = average
    inverse_ref[...] = inverse
    standard = (x - average) * inverse
    n1 = (standard * g1_ref[...] + b1_ref[...]).astype(BF16)
    n1_ref[...] = n1
    n2_ref[...] = (standard * g2_ref[...] + b2_ref[...]).astype(BF16)
    cos_block, sin_block = cos_ref[...], sin_ref[...]
    width = heads * head_dim
    lanes = cos_block.shape[1]
    for part in range(3):
        low = part * width
        projected = dot(n1, w_ref[:, low : low + width]) + bias_ref[:, low : low + width]
        if part == 2:
            kv_ref[:, width:] = projected.astype(BF16)
            continue
        for head in range(heads):
            at = head * head_dim
            turned = turn(projected[:, at : at + lanes], cos_block, sin_block)
            rest = projected[:, at + lanes : at + head_dim]
            if part == 0:
                scale = 1.0 / math.sqrt(head_dim)
                q_ref[:, at : at + lanes] = (turned * scale).astype(BF16)
                q_ref[:, at + lanes : at + head_dim] = (rest * scale).astype(BF16)
            else:
                kv_ref[:, at : at + lanes] = turned.astype(BF16)
                kv_ref[:, at + lanes : at + head_dim] = rest.astype(BF16)


def project(x, gain1, bias1, gain2, bias2, weight, bias, cos_table, sin_table, heads, head_dim):
    rows, depth = x.shape
    block = min(256, rows)
    width = heads * head_dim
    whole = lambda i: (0, 0)
    by_row = lambda i: (i, 0)
    return pl.pallas_call(
        lambda *refs: project_kernel(heads, head_dim, *refs),
        name="project",
        grid=(rows // block,),
        in_specs=[
            pl.BlockSpec((block, depth), by_row),
            *[pl.BlockSpec((1, depth), whole)] * 4,
            pl.BlockSpec((depth, 3 * width), whole, pipeline_mode=pl.Buffered(1)),
            pl.BlockSpec((1, 3 * width), whole),
            pl.BlockSpec((block, cos_table.shape[1]), by_row),
            pl.BlockSpec((block, cos_table.shape[1]), by_row),
        ],
        out_specs=[
            pl.BlockSpec((block, depth), by_row),
            pl.BlockSpec((block, depth), by_row),
            pl.BlockSpec((block, width), by_row),
            pl.BlockSpec((block, 2 * width), by_row),
            pl.BlockSpec((block, 1), by_row),
            pl.BlockSpec((block, 1), by_row),
        ],
        out_shape=[
            jax.ShapeDtypeStruct((rows, depth), BF16),
            jax.ShapeDtypeStruct((rows, depth), BF16),
            jax.ShapeDtypeStruct((rows, width), BF16),
            jax.ShapeDtypeStruct((rows, 2 * width), BF16),
            jax.ShapeDtypeStruct((rows, 1), F32),
            jax.ShapeDtypeStruct((rows, 1), F32),
        ],
        compiler_params=params("arbitrary"),
        cost_estimate=cost(2 * rows * depth * 3 * width, 2 * (3 * rows * depth + 3 * depth * width)),
    )(x, gain1, bias1, gain2, bias2, weight, bias, cos_table, sin_table)


def up_kernel(x_ref, w_ref, b_ref, act_ref, slope_ref):
    hidden = dot(x_ref[...], w_ref[...]) + b_ref[...]
    phi = (1.0 + lax.erf(hidden * F32(math.sqrt(0.5)))) * 0.5
    act_ref[...] = (hidden * phi).astype(BF16)
    density = jnp.exp(hidden * hidden * -0.5) * F32(1.0 / math.sqrt(2.0 * math.pi))
    slope_ref[...] = phi + hidden * density


def up(x, weight, bias):
    rows, depth = x.shape
    width = weight.shape[1]
    bm, bn = min(256, rows), min(512, width)
    return pl.pallas_call(
        up_kernel,
        name="up",
        grid=(width // bn, rows // bm),
        in_specs=[
            pl.BlockSpec((bm, depth), lambda j, i: (i, 0)),
            pl.BlockSpec((depth, bn), lambda j, i: (0, j)),
            pl.BlockSpec((1, bn), lambda j, i: (0, j)),
        ],
        out_specs=[pl.BlockSpec((bm, bn), lambda j, i: (i, j))] * 2,
        out_shape=[
            jax.ShapeDtypeStruct((rows, width), BF16),
            jax.ShapeDtypeStruct((rows, width), F32),
        ],
        compiler_params=params("arbitrary", "arbitrary"),
        cost_estimate=cost(2 * rows * depth * width, 2 * depth * width + 6 * rows * width),
    )(x, weight, bias)


def hidden_kernel(g_ref, w_ref, slope_ref, out_ref, sum_ref):
    grad = dot_cols(g_ref[...], w_ref[...])
    low = (grad * slope_ref[...]).astype(BF16)
    out_ref[...] = low
    total = jnp.sum(low.astype(F32), 0, keepdims=True)

    @pl.when(pl.program_id(1) == 0)
    def _():
        sum_ref[...] = total

    @pl.when(pl.program_id(1) > 0)
    def _():
        sum_ref[...] += total


def hidden_grads(grad, weight, slope):
    rows, depth = grad.shape
    width = weight.shape[0]
    bm, bn = min(256, rows), min(512, width)
    return pl.pallas_call(
        hidden_kernel,
        name="hidden_grads",
        grid=(width // bn, rows // bm),
        in_specs=[
            pl.BlockSpec((bm, depth), lambda j, i: (i, 0)),
            pl.BlockSpec((bn, depth), lambda j, i: (j, 0)),
            pl.BlockSpec((bm, bn), lambda j, i: (i, j)),
        ],
        out_specs=[
            pl.BlockSpec((bm, bn), lambda j, i: (i, j)),
            pl.BlockSpec((1, bn), lambda j, i: (0, j)),
        ],
        out_shape=[
            jax.ShapeDtypeStruct((rows, width), BF16),
            jax.ShapeDtypeStruct((1, width), F32),
        ],
        compiler_params=params("arbitrary", "arbitrary"),
        cost_estimate=cost(2 * rows * depth * width, 2 * depth * width + 6 * rows * width),
    )(grad, weight, slope)


def attention_kernel(heads, head_dim, parts, bk, first_ref, q_ref, do_ref, start_ref, *refs):
    kv_parts, refs = refs[:parts], refs[parts:]
    att_ref, dq_ref, refs = refs[0], refs[1], refs[2:]
    grad_parts, (kv_ref, dkv_ref, s_ref, dp_ref, o_ref, sems) = refs[:parts], refs[parts:]
    block = pl.program_id(0)
    bq = q_ref.shape[0]
    width = heads * head_dim
    rows_each = kv_ref.shape[0] // parts
    ahead = rows_each * (parts - 1)
    low = first_ref[block]
    high = (ahead + (block + 1) * bq + bk - 1) // bk
    row = ahead + block * bq + lax.broadcasted_iota(jnp.int32, (bq, 1), 0)
    start = start_ref[...]
    lane = lax.broadcasted_iota(jnp.int32, (bq, bk), 1)
    chunks = bk // 128

    @pl.when(block == 0)
    def _():
        copies = [
            pltpu.make_async_copy(
                part, kv_ref.at[pl.ds(k * rows_each, rows_each)], sems.at[k]
            )
            for k, part in enumerate(kv_parts)
        ]
        for copy in copies:
            copy.start()

        def clear(j, carry):
            dkv_ref[pl.ds(pl.multiple_of(j * 128, 128), 128), :] = jnp.zeros((128, 2 * width), F32)
            return carry

        lax.fori_loop(0, dkv_ref.shape[0] // 128, clear, 0)
        for copy in copies:
            copy.wait()

    for head in range(heads):
        at = head * head_dim
        q = q_ref[:, at : at + head_dim]
        do = do_ref[:, at : at + head_dim]

        def rows_of(j):
            return pl.ds(pl.multiple_of(j * bk, bk), bk)

        def scores(j, best):
            s = dot_cols(q, kv_ref[rows_of(j), at : at + head_dim])
            column = j * bk + lane
            s = jnp.where((column >= start) & (column <= row), s, -1e30)
            s_ref[j] = s
            for c in range(chunks):
                best = jnp.maximum(best, s[:, c * 128 : (c + 1) * 128])
            return best

        best = lax.fori_loop(low, high, scores, jnp.full((bq, 128), -1e30, F32))
        best = jnp.max(best, 1, keepdims=True)

        def weigh(j, carry):
            total, mixed = carry
            e = jnp.exp(s_ref[j] - best)
            dp = dot_cols(do, kv_ref[rows_of(j), width + at : width + at + head_dim])
            s_ref[j] = e
            dp_ref[j] = dp
            both = e * dp
            for c in range(chunks):
                total = total + e[:, c * 128 : (c + 1) * 128]
                mixed = mixed + both[:, c * 128 : (c + 1) * 128]
            return total, mixed

        zero = jnp.zeros((bq, 128), F32)
        total, mixed = lax.fori_loop(low, high, weigh, (zero, zero))
        total = jnp.sum(total, 1, keepdims=True)
        scale = 1.0 / total
        delta = jnp.sum(mixed, 1, keepdims=True) * scale
        o_ref[...] = jnp.zeros_like(o_ref)

        def spread(j, carry):
            rows = rows_of(j)
            p = s_ref[j] * scale
            p_low = p.astype(BF16)
            ds = (p * (dp_ref[j] - delta)).astype(BF16)
            k = kv_ref[rows, at : at + head_dim]
            v = kv_ref[rows, width + at : width + at + head_dim]
            o_ref[:, :head_dim] += dot(p_low, v)
            o_ref[:, head_dim:] += dot(ds, k)
            dkv_ref[rows, at : at + head_dim] += dot_rows(ds, q)
            dkv_ref[rows, width + at : width + at + head_dim] += dot_rows(p_low, do)
            return carry

        lax.fori_loop(low, high, spread, 0)
        att_ref[:, at : at + head_dim] = o_ref[:, :head_dim].astype(BF16)
        dq_ref[:, at : at + head_dim] = o_ref[:, head_dim:] * (1.0 / math.sqrt(head_dim))

    @pl.when(block == pl.num_programs(0) - 1)
    def _():
        for k, part in enumerate(grad_parts):
            part[...] = dkv_ref[k * rows_each : (k + 1) * rows_each, :].astype(part.dtype)


def attention(q, kv_parts, do, positions, heads, head_dim):
    rows, width = q.shape
    parts = len(kv_parts)
    total = rows * parts
    bq = min(256, rows)
    bk = 256
    start = jnp.arange(rows, dtype=jnp.int32) - positions + (total - rows)
    first = start[::bq] // bk
    by_row = lambda i, f: (i, 0)
    whole = lambda i, f: (0, 0)
    part_types = [BF16] + [F32] * (parts - 1)
    return pl.pallas_call(
        lambda *refs: attention_kernel(heads, head_dim, parts, bk, *refs),
        name="attention",
        grid_spec=pltpu.PrefetchScalarGridSpec(
            num_scalar_prefetch=1,
            grid=(rows // bq,),
            in_specs=[
                pl.BlockSpec((bq, width), by_row),
                pl.BlockSpec((bq, width), by_row),
                pl.BlockSpec((bq, 1), by_row),
                *[pl.BlockSpec(memory_space=pl.ANY)] * parts,
            ],
            out_specs=[
                pl.BlockSpec((bq, width), by_row),
                pl.BlockSpec((bq, width), by_row),
                *[pl.BlockSpec((rows, 2 * width), whole, pipeline_mode=pl.Buffered(1))] * parts,
            ],
            scratch_shapes=[
                pltpu.VMEM((total, 2 * width), BF16),
                pltpu.VMEM((total, 2 * width), F32),
                pltpu.VMEM((total // bk, bq, bk), F32),
                pltpu.VMEM((total // bk, bq, bk), F32),
                pltpu.VMEM((bq, 2 * head_dim), F32),
                pltpu.SemaphoreType.DMA((parts,)),
            ],
        ),
        out_shape=[
            jax.ShapeDtypeStruct((rows, width), BF16),
            jax.ShapeDtypeStruct((rows, width), F32),
            *[jax.ShapeDtypeStruct((rows, 2 * width), kind) for kind in part_types],
        ],
        compiler_params=params("arbitrary"),
        cost_estimate=cost(12 * rows * MOST * width, 8 * total * width),
    )(first, q, do, start[:, None], *kv_parts)


def turn_back_kernel(heads, head_dim, dq_ref, dkv_ref, extra_ref, cos_ref, sin_ref, out_ref, sum_ref):
    cos_block, sin_block = cos_ref[...], -sin_ref[...]
    lanes = cos_block.shape[1]
    width = heads * head_dim
    for part in range(3):
        for head in range(heads):
            at = head * head_dim
            if part == 0:
                grad = dq_ref[:, at : at + head_dim]
            else:
                low = (part - 1) * width + at
                grad = dkv_ref[:, low : low + head_dim] + extra_ref[:, low : low + head_dim].astype(F32)
            to = part * width + at
            if part < 2:
                first = turn(grad[:, :lanes], cos_block, sin_block)
                out_ref[:, to : to + lanes] = first.astype(BF16)
                out_ref[:, to + lanes : to + head_dim] = grad[:, lanes:].astype(BF16)
            else:
                out_ref[:, to : to + head_dim] = grad.astype(BF16)
    total = jnp.sum(out_ref[...].astype(F32), 0, keepdims=True)

    @pl.when(pl.program_id(0) == 0)
    def _():
        sum_ref[...] = total

    @pl.when(pl.program_id(0) > 0)
    def _():
        sum_ref[...] += total


def turn_back(dq, dkv, extra, cos_table, sin_table, heads, head_dim):
    rows, width = dq.shape
    block = min(256, rows)
    by_row = lambda i: (i, 0)
    return pl.pallas_call(
        lambda *refs: turn_back_kernel(heads, head_dim, *refs),
        name="turn_back",
        grid=(rows // block,),
        in_specs=[
            pl.BlockSpec((block, width), by_row),
            pl.BlockSpec((block, 2 * width), by_row),
            pl.BlockSpec((block, 2 * width), by_row),
            pl.BlockSpec((block, cos_table.shape[1]), by_row),
            pl.BlockSpec((block, cos_table.shape[1]), by_row),
        ],
        out_specs=[
            pl.BlockSpec((block, 3 * width), by_row),
            pl.BlockSpec((1, 3 * width), lambda i: (0, 0)),
        ],
        out_shape=[
            jax.ShapeDtypeStruct((rows, 3 * width), BF16),
            jax.ShapeDtypeStruct((1, 3 * width), F32),
        ],
        compiler_params=params("arbitrary"),
        cost_estimate=cost(0, rows * width * 20),
    )(dq, dkv, extra, cos_table, sin_table)


def widen_kernel(in_ref, out_ref):
    out_ref[...] = in_ref[...].astype(F32)


def widened(x):
    rows, depth = x.shape
    block = min(512, rows)
    return pl.pallas_call(
        widen_kernel,
        name="widened",
        grid=(rows // block,),
        in_specs=[pl.BlockSpec((block, depth), lambda i: (i, 0))],
        out_specs=pl.BlockSpec((block, depth), lambda i: (i, 0)),
        out_shape=jax.ShapeDtypeStruct(x.shape, F32),
        compiler_params=params("arbitrary"),
        cost_estimate=cost(0, 6 * x.size),
    )(x)


def spread_kernel(heads, head_dim, in_ref, out_ref):
    for head in range(heads):
        block = in_ref[head * head_dim : (head + 1) * head_dim, :]
        out_ref[:, 0, head, :] = block.T.astype(F32)


def spread(stacked, heads, head_dim):
    depth = stacked.shape[1]
    block = min(1024, depth)
    return pl.pallas_call(
        lambda *refs: spread_kernel(heads, head_dim, *refs),
        name="spread",
        grid=(depth // block, 3),
        in_specs=[pl.BlockSpec((heads * head_dim, block), lambda i, j: (j, i))],
        out_specs=pl.BlockSpec((block, 1, heads, head_dim), lambda i, j: (i, j, 0, 0)),
        out_shape=jax.ShapeDtypeStruct((depth, 3, heads, head_dim), F32),
        compiler_params=params("arbitrary", "arbitrary"),
        cost_estimate=cost(0, 6 * stacked.size),
    )(stacked)


def reduce_kernel(plan, chunks, bits, tensor, *refs):
    refs = list(refs)
    take = lambda count: [refs.pop(0) for _ in range(count)]
    a_refs = take(len(plan))
    b_refs = take(3)
    vec_ref, dqkv_ref, hg_ref, gain1_ref, gain2_ref, mean_ref, inverse_ref = take(7)
    w1_ref, w2_ref, x_ref = take(3)
    out_refs = take(len(plan))
    dsum_ref, total_ref = take(2)
    abuf, full, r0, ag = take(4)
    w1buf, w2buf, xbuf, zsend, mine_ref, w_sem = take(6)
    kept, sent, got = take(bits - 1), take(bits - 1), take(bits - 1)
    dgot, vgot, vsend, vnow = take(4)
    a_sem, o_sem, send_sem, recv_sem, d_send, d_recv, v_send, v_recv = take(8)
    index, me = lax.axis_index("dp"), lax.axis_index("tensor")
    deep, wide = full.shape[1], full.shape[2]
    slots, ring, lag = r0.shape[0], ag.shape[0], 2

    def bit_of(bit):
        return (index // (1 << bit)) % 2

    def partner(bit):
        return index + (1 << bit) * (1 - 2 * bit_of(bit))

    barrier = pltpu.get_barrier_semaphore()
    for bit in range(bits):
        pl.semaphore_signal(barrier, inc=1, device_id={"dp": partner(bit)}, device_id_type=MESH)
    for k in range(1, tensor):
        other = lax.rem(me + k, tensor)
        pl.semaphore_signal(barrier, inc=1, device_id={"tensor": other}, device_id_type=MESH)
    pl.semaphore_wait(barrier, bits + tensor - 1)

    own_rows = dsum_ref.shape[0]
    units = wide // deep
    zslots = zsend.shape[0]
    begin = max(chunks // 2, 1)

    def columns_of(u):
        return pl.ds(pl.multiple_of(u * deep, deep), deep)

    def d_copy(k, u):
        other = lax.rem(me + k, tensor)
        rows = pl.ds(pl.multiple_of(other * own_rows, own_rows), own_rows)
        return pltpu.make_async_remote_copy(
            src_ref=zsend.at[lax.rem(u, zslots), rows],
            dst_ref=dgot.at[k - 1, :, columns_of(u)],
            send_sem=d_send.at[k - 1, u],
            recv_sem=d_recv.at[k - 1, u],
            device_id={"tensor": other},
            device_id_type=MESH,
        )

    def unit_copies(u):
        slot = lax.rem(u, 2)
        return [
            pltpu.make_async_copy(w1_ref.at[columns_of(u)], w1buf.at[slot], w_sem.at[0, slot]),
            pltpu.make_async_copy(w2_ref.at[columns_of(u)], w2buf.at[slot], w_sem.at[1, slot]),
            pltpu.make_async_copy(x_ref.at[:, columns_of(u)], xbuf.at[slot], w_sem.at[2, slot]),
        ]

    def unit(u):
        slot, zslot = lax.rem(u, 2), lax.rem(u, zslots)
        columns = columns_of(u)

        @pl.when(u + 1 < units)
        def _():
            for copy in unit_copies(u + 1):
                copy.start()

        for copy in unit_copies(u):
            copy.wait()

        @pl.when(u >= zslots)
        def _():
            for k in range(1, tensor):
                d_copy(k, u - zslots).wait_send()

        gain1, gain2 = gain1_ref[:, columns], gain2_ref[:, columns]
        mine_ref[0:4, columns] = jnp.zeros((4, deep), F32)

        def row_block(i, carry):
            rows = pl.ds(pl.multiple_of(i * own_rows, own_rows), own_rows)
            one = dot_cols(dqkv_ref[rows, :], w1buf[slot])
            two = dot_cols(hg_ref[rows, :], w2buf[slot])
            both = one * gain1 + two * gain2
            zsend[zslot, rows] = both.astype(BF16)

            @pl.when(i == me)
            def _():
                dsum_ref[:, columns] = both

            standard = (xbuf[slot, rows].astype(F32) - mean_ref[rows, :]) * inverse_ref[rows, :]
            add = lambda v: jnp.sum(v, 0, keepdims=True)
            mine_ref[0:4, columns] += jnp.concatenate(
                [add(one * standard), add(one), add(two * standard), add(two)], 0
            )
            return carry

        lax.fori_loop(0, tensor, row_block, 0)
        for k in range(1, tensor):
            d_copy(k, u).start()

    def v_copy(k, to, slot):
        return pltpu.make_async_remote_copy(
            src_ref=mine_ref,
            dst_ref=vgot.at[slot],
            send_sem=v_send.at[k - 1],
            recv_sem=v_recv.at[slot],
            device_id={"tensor": to},
            device_id_type=MESH,
        )

    def v_step(bit):
        return pltpu.make_async_remote_copy(
            src_ref=vsend.at[bit],
            dst_ref=vnow.at[bit],
            send_sem=v_send.at[tensor + bit],
            recv_sem=v_recv.at[tensor + bit],
            device_id={"dp": partner(bit)},
            device_id_type=MESH,
        )

    def fetch_copy(item, c):
        column = pl.multiple_of((c - plan[item][0]) * deep, deep)
        slot = lax.rem(c, 2)
        return pltpu.make_async_copy(
            a_refs[item].at[:, pl.ds(column, deep)], abuf.at[slot], a_sem.at[slot]
        )

    def on_items(c, act):
        for item, (first, count, _) in enumerate(plan):
            @pl.when((c >= first) & (c < first + count))
            def _():
                act(item)

    even, odd = list(range(bits)), [0, *range(2, bits), 1]

    def mixed(level, parity, of):
        first, second = of(even[level]), of(odd[level])
        return first + parity * (second - first)

    def base(level, parity):
        row = 0
        for k in range(level):
            row = row + mixed(k, parity, bit_of) * (deep >> (k + 1))
        return row

    def down_copy(level, c):
        parity, slot = lax.rem(c, 2), lax.rem(c, slots)
        half = deep >> (level + 1)
        if level == 0:
            row = pl.multiple_of((1 - bit_of(0)) * half, half)
            source, target = full.at[lax.rem(c, 3), pl.ds(row, half)], r0.at[slot]
        else:
            source, target = sent[level - 1].at[slot], got[level - 1].at[slot]
        return pltpu.make_async_remote_copy(
            src_ref=source,
            dst_ref=target,
            send_sem=send_sem.at[level, lax.rem(c, ring)],
            recv_sem=recv_sem.at[level, lax.rem(c, ring)],
            device_id={"dp": mixed(level, parity, partner)},
            device_id_type=MESH,
        )

    def up_copy(level, c):
        parity, slot = lax.rem(c, 2), lax.rem(c, ring)
        size = deep >> (level + 1)
        row = base(level + 1, parity)
        rows = pl.ds(pl.multiple_of(row, size), size)
        return pltpu.make_async_remote_copy(
            src_ref=ag.at[slot, rows],
            dst_ref=ag.at[slot, rows],
            send_sem=send_sem.at[bits + level, slot],
            recv_sem=recv_sem.at[bits + level, slot],
            device_id={"dp": mixed(level, parity, partner)},
            device_id_type=MESH,
        )

    def out_copy(item, c):
        slot = lax.rem(c, ring)
        row = pl.multiple_of((c - plan[item][0]) * deep, deep)
        return pltpu.make_async_copy(
            ag.at[slot], out_refs[item].at[pl.ds(row, deep)], o_sem.at[slot]
        )

    def multiply(c):
        slot = lax.rem(c, 3)

        def with_item(item):
            fetch_copy(item, c).wait()
            left = abuf[lax.rem(c, 2)].T
            right = b_refs[plan[item][2]]
            step = min(512, wide)
            for column in range(0, wide, step):
                full[slot, :, column : column + step] = dot(left, right[:, column : column + step])

        on_items(c, with_item)
        down_copy(0, c).start()

    def halve(level, c):
        parity, slot = lax.rem(c, 2), lax.rem(c, slots)
        down_copy(level - 1, c).wait()
        size = deep >> level
        half = size // 2
        if level < bits:
            bit = mixed(level, parity, bit_of)
            keep = pl.multiple_of(bit * half, half)
            give = pl.multiple_of((1 - bit) * half, half)
            pieces = ((keep, True), (give, False))
        else:
            pieces = ((0, True),)
            half = size
        for row, stays in pieces:
            if level == 1:
                mine = full[
                    lax.rem(c, 3), pl.ds(pl.multiple_of(bit_of(0) * size + row, half), half)
                ]
                value = mine + r0[slot, pl.ds(row, half)]
            else:
                mine = kept[level - 2][slot, pl.ds(row, half)]
                value = mine + got[level - 2][slot, pl.ds(row, half)].astype(F32)
            if level == bits:
                at = pl.multiple_of(base(bits, parity), size)
                ag[lax.rem(c, ring), pl.ds(at, size)] = value.astype(BF16)
            elif stays:
                kept[level - 1][slot] = value
            else:
                sent[level - 1][slot] = value.astype(BF16)
        if level < bits:
            down_copy(level, c).start()
        else:
            up_copy(bits - 1, c).start()

    def widen(level, c):
        up_copy(level, c).wait()
        up_copy(level - 1, c).start()

    def finish(c):
        up_copy(0, c).wait()
        on_items(c, lambda item: out_copy(item, c).start())

    on_items(0, lambda item: fetch_copy(item, 0).start())
    for copy in unit_copies(0):
        copy.start()
    mine_ref[...] = vec_ref[...]

    def stage(t, delay, act):
        c = t - delay

        @pl.when((c >= 0) & (c < chunks))
        def _():
            act(c)

    def stage_of(t, first, count, act):
        @pl.when((t >= first) & (t < first + count))
        def _():
            act(t - first)

    def iteration(t, carry):
        @pl.when(t + 1 < chunks)
        def _():
            on_items(t + 1, lambda item: fetch_copy(item, t + 1).start())

        stage(
            t, 2 * bits * lag + 1,
            lambda c: on_items(c, lambda item: out_copy(item, c).wait()),
        )
        stage(t, 2 * bits * lag, finish)
        for level in range(1, bits):
            stage(t, (2 * bits - level) * lag, lambda c, level=level: widen(level, c))
        for level in range(bits, 0, -1):
            stage(t, level * lag, lambda c, level=level: halve(level, c))
        stage(t, 0, multiply)

        stage_of(t, begin, units, unit)

        @pl.when(t == begin + units)
        def _():
            for k in range(1, tensor):
                v_copy(k, lax.rem(me + k, tensor), me).start()
            vgot[me] = mine_ref[...]

        @pl.when(t == begin + units + 2)
        def _():
            for k in range(1, tensor):
                other = lax.rem(me + k, tensor)
                v_copy(k, other, me).wait_send()
                v_copy(k, other, other).wait_recv()
            line = lax.broadcasted_iota(jnp.int32, mine_ref.shape, 0)
            both = vgot[0]
            for k in range(1, tensor):
                both = both + vgot[k]
            vsend[0] = jnp.where(line < 5, both, mine_ref[...])
            v_step(0).start()

        for bit in range(bits):
            @pl.when(t == begin + units + 4 + 2 * bit)
            def _():
                v_step(bit).wait()
                both = vsend[bit] + vnow[bit]
                if bit + 1 < bits:
                    vsend[bit + 1] = both
                    v_step(bit + 1).start()
                else:
                    total_ref[...] = both

        return carry

    lax.fori_loop(0, max(chunks + 2 * bits * lag + 1, begin + units + 3 + 2 * bits), iteration, 0)

    def gather(u, carry):
        for k in range(1, tensor):
            d_copy(k, u).wait_recv()
        return carry

    lax.fori_loop(0, units, gather, 0)
    for u in range(max(units - zslots, 0), units):
        for k in range(1, tensor):
            d_copy(k, u).wait_send()
    rest = dsum_ref[...]
    for k in range(1, tensor):
        rest = rest + dgot[k - 1].astype(F32)
    dsum_ref[...] = rest


def reduce_grads(items, rights, vectors, moments_of, pair_one, pair_two, x, bits, tensor):
    deep = 256
    rows, wide = rights[0].shape
    plan, first = [], 0
    for left, which in items:
        count = left.shape[1] // deep
        plan.append((first, count, which))
        first += count
    chunks, ring, slots = first, 4 * bits - 2, 4
    halves_of = [deep >> (level + 1) for level in range(1, bits)]
    own_rows = rows // tensor
    (dqkv, w1, gain1), (hg, w2, gain2), (mean, inverse) = pair_one, pair_two, moments_of
    units, zslots = wide // deep, 3
    hbm = pl.BlockSpec(memory_space=pl.ANY)
    vmem = pl.BlockSpec(memory_space=pltpu.VMEM)
    return pl.pallas_call(
        lambda *refs: reduce_kernel(plan, chunks, bits, tensor, *refs),
        name="reduce_grads",
        in_specs=[hbm] * len(items) + [vmem] * 10 + [hbm] * 3,
        out_specs=[hbm] * len(items) + [vmem, vmem],
        out_shape=[
            *[jax.ShapeDtypeStruct((left.shape[1], wide), BF16) for left, _ in items],
            jax.ShapeDtypeStruct((own_rows, wide), F32),
            jax.ShapeDtypeStruct(vectors.shape, F32),
        ],
        scratch_shapes=[
            pltpu.VMEM((2, rows, deep), BF16),
            pltpu.VMEM((3, deep, wide), F32),
            pltpu.VMEM((slots, deep // 2, wide), F32),
            pltpu.VMEM((ring, deep, wide), BF16),
            pltpu.VMEM((2, deep, w1.shape[1]), BF16),
            pltpu.VMEM((2, deep, w2.shape[1]), BF16),
            pltpu.VMEM((2, rows, deep), BF16),
            pltpu.VMEM((zslots, rows, deep), BF16),
            pltpu.VMEM(vectors.shape, F32),
            pltpu.SemaphoreType.DMA((3, 2)),
            *[pltpu.VMEM((slots, half, wide), F32) for half in halves_of],
            *[pltpu.VMEM((slots, half, wide), BF16) for half in halves_of],
            *[pltpu.VMEM((slots, half, wide), BF16) for half in halves_of],
            pltpu.VMEM((tensor - 1, own_rows, wide), BF16),
            pltpu.VMEM((tensor, *vectors.shape), F32),
            pltpu.VMEM((bits, *vectors.shape), F32),
            pltpu.VMEM((bits, *vectors.shape), F32),
            pltpu.SemaphoreType.DMA((2,)),
            pltpu.SemaphoreType.DMA((ring,)),
            pltpu.SemaphoreType.DMA((2 * bits, ring)),
            pltpu.SemaphoreType.DMA((2 * bits, ring)),
            pltpu.SemaphoreType.DMA((tensor - 1, units)),
            pltpu.SemaphoreType.DMA((tensor - 1, units)),
            pltpu.SemaphoreType.DMA((tensor + bits,)),
            pltpu.SemaphoreType.DMA((tensor + bits,)),
        ],
        compiler_params=pltpu.CompilerParams(
            collective_id=0, has_side_effects=True, vmem_limit_bytes=62 << 20
        ),
        cost_estimate=cost(2 * rows * chunks * deep * wide, 8 * chunks * deep * wide),
    )(
        *[left for left, _ in items], *rights, vectors, dqkv, hg, gain1, gain2, mean, inverse,
        w1, w2, x,
    )


def body(
    tokens, out_grad, segment_ids, positions, norm1_gain, norm1_bias, norm2_gain, norm2_bias,
    qkv_weight, qkv_bias, out_weight, out_bias, fc1_weight, fc1_bias, fc2_weight, fc2_bias,
):
    model_width, heads, _, head_dim = qkv_weight.shape
    width = heads * head_dim
    hidden_width = fc1_weight.shape[1]
    own_count = tokens.shape[0]
    tie = lax.optimization_barrier
    row = lambda v: v.reshape(1, -1).astype(F32)
    rows_all = lax.all_gather(tokens, "tensor", axis=0, tiled=True)
    grads_all = lax.all_gather(out_grad, "tensor", axis=0, tiled=True)
    row_count = rows_all.shape[0]
    flat_qkv = jnp.transpose(qkv_weight, (0, 2, 1, 3)).reshape(model_width, 3 * width)
    flat_bias = jnp.transpose(qkv_bias, (1, 0, 2)).reshape(1, 3 * width).astype(F32)
    flat_out = out_weight.reshape(width, model_width)
    cos_table, sin_table = rope_tables(positions, 128)
    normed_one, normed_two, queries, kv_own, mean, inverse = project(
        rows_all, row(norm1_gain), row(norm1_bias), row(norm2_gain), row(norm2_bias),
        flat_qkv, flat_bias, cos_table, sin_table, heads, head_dim,
    )
    reach = (MOST - 2) // row_count + 1
    kv_parts = [kv_own]
    for _ in range(reach):
        kv_parts.insert(0, shifted(kv_parts[0], "dp", 1))
    activated, slope = up(normed_two, fc1_weight, row(fc1_bias))
    forward = dot(activated, fc2_weight)
    grads_all, activated, slope, forward = tie((grads_all, activated, slope, forward))

    attended_grad = dot_cols(grads_all, flat_out).astype(BF16)
    attended, query_grad, *kv_grads = attention(
        queries, kv_parts, attended_grad, positions, heads, head_dim
    )
    grads_all, attended, query_grad, *kv_grads = tie((grads_all, attended, query_grad, *kv_grads))
    partial = dot(attended, flat_out) + forward
    branch = lax.psum_scatter(partial, "tensor", scatter_dimension=0, tiled=True)
    hidden_grad, fc1_bias_grad = hidden_grads(grads_all, fc2_weight, slope)
    extra = None
    for part in kv_grads[:-1]:
        if extra is not None:
            part = (part + extra.astype(F32)).astype(BF16)
        extra = shifted(part, "dp", -1)
        extra, hidden_grad = tie((extra, hidden_grad))
    qkv_grad, qkv_bias_grad = turn_back(
        query_grad, kv_grads[-1], extra, cos_table, sin_table, heads, head_dim
    )
    wide = lambda v: jnp.pad(v, ((0, 0), (0, model_width - v.shape[1])))
    own_grad = out_grad.astype(F32)
    vectors = jnp.concatenate(
        [
            jnp.zeros((4, model_width), F32), jnp.sum(own_grad, 0, keepdims=True), wide(fc1_bias_grad), wide(qkv_bias_grad),
            jnp.zeros((1, model_width), F32),
        ],
        0,
    )
    bits = (lax.axis_size("dp") - 1).bit_length()
    natural = hidden_width == model_width
    fc1_pair = (normed_two, hidden_grad) if natural else (hidden_grad, normed_two)
    fc2_grad, out_weight_grad, fc1_grad, qkv_weight_grad, d_sum, vectors = reduce_grads(
        [(activated, 0), (attended, 0), (fc1_pair[0], 1), (qkv_grad, 2)],
        [grads_all, fc1_pair[1], normed_one],
        vectors, (mean, inverse), (qkv_grad, flat_qkv, row(norm1_gain)),
        (hidden_grad, fc1_weight, row(norm2_gain)), rows_all, bits, lax.axis_size("tensor"),
    )
    fc2_grad = widened(fc2_grad)
    out_weight_grad = out_weight_grad.astype(F32).reshape(heads, head_dim, model_width)
    fc1_grad = widened(fc1_grad) if natural else fc1_grad.T.astype(F32)
    qkv_weight_grad = jnp.transpose(spread(qkv_weight_grad, heads, head_dim), (0, 2, 1, 3))
    fc1_bias_grad = vectors[5, :hidden_width]
    qkv_bias_grad = vectors[6, : 3 * width].reshape(3, heads, head_dim)
    qkv_bias_grad = jnp.transpose(qkv_bias_grad, (1, 0, 2))
    own_rows = tokens.astype(F32)
    block_out = own_rows + branch + out_bias.astype(F32) + fc2_bias.astype(F32)
    own_mean, own_inverse = moments(own_rows)
    standard = (own_rows - own_mean) * own_inverse
    tokens_grad = own_grad + own_inverse * (
        d_sum
        - jnp.mean(d_sum, -1, keepdims=True)
        - standard * jnp.mean(d_sum * standard, -1, keepdims=True)
    )
    return (
        block_out.astype(BF16), tokens_grad.astype(BF16),
        vectors[0], vectors[1], vectors[2], vectors[3],
        qkv_weight_grad, qkv_bias_grad, out_weight_grad, vectors[4],
        fc1_grad, fc1_bias_grad, fc2_grad, vectors[4],
    )


def solution(mesh):
    rows = P(("dp", "tensor"), None)
    return jax.shard_map(
        body,
        mesh=mesh,
        in_specs=(
            rows, rows, P("dp"), P("dp"), P(), P(), P(), P(),
            P(None, "tensor", None, None), P("tensor", None, None), P("tensor", None, None), P(),
            P(None, "tensor"), P("tensor"), P("tensor", None), P(),
        ),
        out_specs=(
            rows, rows, P(), P(), P(), P(),
            P(None, "tensor", None, None), P("tensor", None, None), P("tensor", None, None), P(),
            P(None, "tensor"), P("tensor"), P("tensor", None), P(),
        ),
        check_vma=False,
    )
```

```python
import math

import jax
import jax.numpy as jnp
from jax import lax
from jax.experimental import pallas as pl
from jax.experimental.pallas import tpu as pltpu
from jax.sharding import PartitionSpec as P

ROT = 64
MOST = 2000
EPSILON = 1e-05
BF16 = jnp.bfloat16
F32 = jnp.float32
MESH = pl.DeviceIdType.MESH


def shifted(x, axis, by):
    length = lax.axis_size(axis)
    pairs = [(i, i + by) for i in range(length) if 0 <= i + by < length]
    return lax.ppermute(x, axis, pairs)


def swapped(x, axis, bit):
    length = lax.axis_size(axis)
    return lax.ppermute(x, axis, [(i, i ^ (1 << bit)) for i in range(length)])


def dot_rows(first, second):
    return lax.dot_general(first, second, (((0,), (0,)), ((), ())), preferred_element_type=F32)


def dot_cols(first, second):
    return lax.dot_general(first, second, (((1,), (1,)), ((), ())), preferred_element_type=F32)


def dot(first, second):
    return jnp.dot(first, second, preferred_element_type=F32)


def cost(flops, bytes_accessed):
    return pl.CostEstimate(flops=int(flops), bytes_accessed=int(bytes_accessed), transcendentals=0)


def params(*semantics):
    return pltpu.CompilerParams(dimension_semantics=semantics, vmem_limit_bytes=60 << 20)


def moments(values):
    average = jnp.mean(values, -1, keepdims=True)
    centered = values - average
    variance = jnp.mean(centered * centered, -1, keepdims=True)
    return average, lax.rsqrt(variance + EPSILON)


def rope_tables(position, lanes):
    half = ROT // 2
    frequency = jnp.power(F32(10000.0), -jnp.arange(half, dtype=F32) / F32(half))
    angles = position.astype(F32)[:, None] * frequency[None, :]
    cosine, sine = jnp.cos(angles), jnp.sin(angles)
    rows = position.shape[0]
    ones = jnp.ones((rows, lanes - ROT), F32)
    return (
        jnp.concatenate([cosine, cosine, ones], 1),
        jnp.concatenate([-sine, sine, 0 * ones], 1),
    )


def turn(values, cos_block, sin_block):
    lane = lax.broadcasted_iota(jnp.int32, values.shape, 1)
    half = ROT // 2
    up = pltpu.roll(values, values.shape[1] - half, 1)
    down = pltpu.roll(values, half, 1)
    return values * cos_block + jnp.where(lane < half, up, down) * sin_block


def project_kernel(
    heads, head_dim, x_ref, g1_ref, b1_ref, g2_ref, b2_ref, w_ref, bias_ref, cos_ref, sin_ref,
    n1_ref, n2_ref, q_ref, kv_ref, mean_ref, inverse_ref,
):
    x = x_ref[...].astype(F32)
    average, inverse = moments(x)
    mean_ref[...] = average
    inverse_ref[...] = inverse
    standard = (x - average) * inverse
    n1 = (standard * g1_ref[...] + b1_ref[...]).astype(BF16)
    n1_ref[...] = n1
    n2_ref[...] = (standard * g2_ref[...] + b2_ref[...]).astype(BF16)
    cos_block, sin_block = cos_ref[...], sin_ref[...]
    width = heads * head_dim
    lanes = cos_block.shape[1]
    for part in range(3):
        low = part * width
        projected = dot(n1, w_ref[:, low : low + width]) + bias_ref[:, low : low + width]
        if part == 2:
            kv_ref[:, width:] = projected.astype(BF16)
            continue
        for head in range(heads):
            at = head * head_dim
            turned = turn(projected[:, at : at + lanes], cos_block, sin_block)
            rest = projected[:, at + lanes : at + head_dim]
            if part == 0:
                scale = 1.0 / math.sqrt(head_dim)
                q_ref[:, at : at + lanes] = (turned * scale).astype(BF16)
                q_ref[:, at + lanes : at + head_dim] = (rest * scale).astype(BF16)
            else:
                kv_ref[:, at : at + lanes] = turned.astype(BF16)
                kv_ref[:, at + lanes : at + head_dim] = rest.astype(BF16)


def project(x, gain1, bias1, gain2, bias2, weight, bias, cos_table, sin_table, heads, head_dim):
    rows, depth = x.shape
    block = min(256, rows)
    width = heads * head_dim
    whole = lambda i: (0, 0)
    by_row = lambda i: (i, 0)
    return pl.pallas_call(
        lambda *refs: project_kernel(heads, head_dim, *refs),
        name="project",
        grid=(rows // block,),
        in_specs=[
            pl.BlockSpec((block, depth), by_row),
            *[pl.BlockSpec((1, depth), whole)] * 4,
            pl.BlockSpec((depth, 3 * width), whole, pipeline_mode=pl.Buffered(1)),
            pl.BlockSpec((1, 3 * width), whole),
            pl.BlockSpec((block, cos_table.shape[1]), by_row),
            pl.BlockSpec((block, cos_table.shape[1]), by_row),
        ],
        out_specs=[
            pl.BlockSpec((block, depth), by_row),
            pl.BlockSpec((block, depth), by_row),
            pl.BlockSpec((block, width), by_row),
            pl.BlockSpec((block, 2 * width), by_row),
            pl.BlockSpec((block, 1), by_row),
            pl.BlockSpec((block, 1), by_row),
        ],
        out_shape=[
            jax.ShapeDtypeStruct((rows, depth), BF16),
            jax.ShapeDtypeStruct((rows, depth), BF16),
            jax.ShapeDtypeStruct((rows, width), BF16),
            jax.ShapeDtypeStruct((rows, 2 * width), BF16),
            jax.ShapeDtypeStruct((rows, 1), F32),
            jax.ShapeDtypeStruct((rows, 1), F32),
        ],
        compiler_params=params("arbitrary"),
        cost_estimate=cost(2 * rows * depth * 3 * width, 2 * (3 * rows * depth + 3 * depth * width)),
    )(x, gain1, bias1, gain2, bias2, weight, bias, cos_table, sin_table)


def up_kernel(x_ref, w_ref, b_ref, act_ref, slope_ref):
    hidden = dot(x_ref[...], w_ref[...]) + b_ref[...]
    phi = (1.0 + lax.erf(hidden * F32(math.sqrt(0.5)))) * 0.5
    act_ref[...] = (hidden * phi).astype(BF16)
    density = jnp.exp(hidden * hidden * -0.5) * F32(1.0 / math.sqrt(2.0 * math.pi))
    slope_ref[...] = phi + hidden * density


def up(x, weight, bias):
    rows, depth = x.shape
    width = weight.shape[1]
    bm, bn = min(256, rows), min(512, width)
    return pl.pallas_call(
        up_kernel,
        name="up",
        grid=(width // bn, rows // bm),
        in_specs=[
            pl.BlockSpec((bm, depth), lambda j, i: (i, 0)),
            pl.BlockSpec((depth, bn), lambda j, i: (0, j)),
            pl.BlockSpec((1, bn), lambda j, i: (0, j)),
        ],
        out_specs=[pl.BlockSpec((bm, bn), lambda j, i: (i, j))] * 2,
        out_shape=[
            jax.ShapeDtypeStruct((rows, width), BF16),
            jax.ShapeDtypeStruct((rows, width), F32),
        ],
        compiler_params=params("arbitrary", "arbitrary"),
        cost_estimate=cost(2 * rows * depth * width, 2 * depth * width + 6 * rows * width),
    )(x, weight, bias)


def attention_kernel(heads, head_dim, parts, bk, first_ref, q_ref, do_ref, start_ref, *refs):
    kv_parts, refs = refs[:parts], refs[parts:]
    att_ref, dq_ref, refs = refs[0], refs[1], refs[2:]
    grad_parts, (kv_ref, dkv_ref, s_ref, dp_ref, o_ref, sems) = refs[:parts], refs[parts:]
    block = pl.program_id(0)
    bq = q_ref.shape[0]
    width = heads * head_dim
    rows_each = kv_ref.shape[0] // parts
    ahead = rows_each * (parts - 1)
    low = first_ref[block]
    high = (ahead + (block + 1) * bq + bk - 1) // bk
    row = ahead + block * bq + lax.broadcasted_iota(jnp.int32, (bq, 1), 0)
    start = start_ref[...]
    lane = lax.broadcasted_iota(jnp.int32, (bq, bk), 1)
    chunks = bk // 128

    @pl.when(block == 0)
    def _():
        copies = [
            pltpu.make_async_copy(
                part, kv_ref.at[pl.ds(k * rows_each, rows_each)], sems.at[k]
            )
            for k, part in enumerate(kv_parts)
        ]
        for copy in copies:
            copy.start()

        def clear(j, carry):
            dkv_ref[pl.ds(pl.multiple_of(j * 128, 128), 128), :] = jnp.zeros((128, 2 * width), F32)
            return carry

        lax.fori_loop(0, dkv_ref.shape[0] // 128, clear, 0)
        for copy in copies:
            copy.wait()

    for head in range(heads):
        at = head * head_dim
        q = q_ref[:, at : at + head_dim]
        do = do_ref[:, at : at + head_dim]

        def rows_of(j):
            return pl.ds(pl.multiple_of(j * bk, bk), bk)

        def scores(j, best):
            s = dot_cols(q, kv_ref[rows_of(j), at : at + head_dim])
            column = j * bk + lane
            s = jnp.where((column >= start) & (column <= row), s, -1e30)
            s_ref[j] = s
            for c in range(chunks):
                best = jnp.maximum(best, s[:, c * 128 : (c + 1) * 128])
            return best

        best = lax.fori_loop(low, high, scores, jnp.full((bq, 128), -1e30, F32))
        best = jnp.max(best, 1, keepdims=True)

        def weigh(j, carry):
            total, mixed = carry
            e = jnp.exp(s_ref[j] - best)
            dp = dot_cols(do, kv_ref[rows_of(j), width + at : width + at + head_dim])
            s_ref[j] = e
            dp_ref[j] = dp
            both = e * dp
            for c in range(chunks):
                total = total + e[:, c * 128 : (c + 1) * 128]
                mixed = mixed + both[:, c * 128 : (c + 1) * 128]
            return total, mixed

        zero = jnp.zeros((bq, 128), F32)
        total, mixed = lax.fori_loop(low, high, weigh, (zero, zero))
        total = jnp.sum(total, 1, keepdims=True)
        scale = 1.0 / total
        delta = jnp.sum(mixed, 1, keepdims=True) * scale
        o_ref[...] = jnp.zeros_like(o_ref)

        def spread(j, carry):
            rows = rows_of(j)
            p = s_ref[j] * scale
            p_low = p.astype(BF16)
            ds = (p * (dp_ref[j] - delta)).astype(BF16)
            k = kv_ref[rows, at : at + head_dim]
            v = kv_ref[rows, width + at : width + at + head_dim]
            o_ref[:, :head_dim] += dot(p_low, v)
            o_ref[:, head_dim:] += dot(ds, k)
            dkv_ref[rows, at : at + head_dim] += dot_rows(ds, q)
            dkv_ref[rows, width + at : width + at + head_dim] += dot_rows(p_low, do)
            return carry

        lax.fori_loop(low, high, spread, 0)
        att_ref[:, at : at + head_dim] = o_ref[:, :head_dim].astype(BF16)
        dq_ref[:, at : at + head_dim] = o_ref[:, head_dim:] * (1.0 / math.sqrt(head_dim))

    @pl.when(block == pl.num_programs(0) - 1)
    def _():
        for k, part in enumerate(grad_parts):
            part[...] = dkv_ref[k * rows_each : (k + 1) * rows_each, :].astype(part.dtype)


def attention(q, kv_parts, do, positions, heads, head_dim):
    rows, width = q.shape
    parts = len(kv_parts)
    total = rows * parts
    bq = min(256, rows)
    bk = 256
    start = jnp.arange(rows, dtype=jnp.int32) - positions + (total - rows)
    first = start[::bq] // bk
    by_row = lambda i, f: (i, 0)
    whole = lambda i, f: (0, 0)
    part_types = [BF16] + [F32] * (parts - 1)
    return pl.pallas_call(
        lambda *refs: attention_kernel(heads, head_dim, parts, bk, *refs),
        name="attention",
        grid_spec=pltpu.PrefetchScalarGridSpec(
            num_scalar_prefetch=1,
            grid=(rows // bq,),
            in_specs=[
                pl.BlockSpec((bq, width), by_row),
                pl.BlockSpec((bq, width), by_row),
                pl.BlockSpec((bq, 1), by_row),
                *[pl.BlockSpec(memory_space=pl.ANY)] * parts,
            ],
            out_specs=[
                pl.BlockSpec((bq, width), by_row),
                pl.BlockSpec((bq, width), by_row),
                *[pl.BlockSpec((rows, 2 * width), whole, pipeline_mode=pl.Buffered(1))] * parts,
            ],
            scratch_shapes=[
                pltpu.VMEM((total, 2 * width), BF16),
                pltpu.VMEM((total, 2 * width), F32),
                pltpu.VMEM((total // bk, bq, bk), F32),
                pltpu.VMEM((total // bk, bq, bk), F32),
                pltpu.VMEM((bq, 2 * head_dim), F32),
                pltpu.SemaphoreType.DMA((parts,)),
            ],
        ),
        out_shape=[
            jax.ShapeDtypeStruct((rows, width), BF16),
            jax.ShapeDtypeStruct((rows, width), F32),
            *[jax.ShapeDtypeStruct((rows, 2 * width), kind) for kind in part_types],
        ],
        compiler_params=params("arbitrary"),
        cost_estimate=cost(12 * rows * MOST * width, 8 * total * width),
    )(first, q, do, start[:, None], *kv_parts)


def widen_kernel(in_ref, out_ref):
    out_ref[...] = in_ref[...].astype(F32)


def widened(x):
    rows, depth = x.shape
    block = min(512, rows)
    return pl.pallas_call(
        widen_kernel,
        name="widened",
        grid=(rows // block,),
        in_specs=[pl.BlockSpec((block, depth), lambda i: (i, 0))],
        out_specs=pl.BlockSpec((block, depth), lambda i: (i, 0)),
        out_shape=jax.ShapeDtypeStruct(x.shape, F32),
        compiler_params=params("arbitrary"),
        cost_estimate=cost(0, 6 * x.size),
    )(x)


def spread_kernel(heads, head_dim, in_ref, out_ref):
    for head in range(heads):
        block = in_ref[head * head_dim : (head + 1) * head_dim, :]
        out_ref[:, 0, head, :] = block.T.astype(F32)


def spread(stacked, heads, head_dim):
    depth = stacked.shape[1]
    block = min(1024, depth)
    return pl.pallas_call(
        lambda *refs: spread_kernel(heads, head_dim, *refs),
        name="spread",
        grid=(depth // block, 3),
        in_specs=[pl.BlockSpec((heads * head_dim, block), lambda i, j: (j, i))],
        out_specs=pl.BlockSpec((block, 1, heads, head_dim), lambda i, j: (i, j, 0, 0)),
        out_shape=jax.ShapeDtypeStruct((depth, 3, heads, head_dim), F32),
        compiler_params=params("arbitrary", "arbitrary"),
        cost_estimate=cost(0, 6 * stacked.size),
    )(stacked)


def reduce_kernel(plan, dims, *refs):
    chunks, bits, tensor, heads, head_dim, blocks, wide_b = dims
    refs = list(refs)
    take = lambda count: [refs.pop(0) for _ in range(count)]
    g_ref, n1_ref, slope_ref, up_ref, down_ref, w1_ref, x_ref, wout_ref, forward_ref = take(9)
    far_ref, near_ref, own_ref, dq_ref = take(4)
    extra_refs = take(wide_b)
    lefts = take(sum(1 for item in plan if item[3]))
    att_ref, vec_ref, gain1_ref, gain2_ref, mean_ref, inverse_ref, cos_ref, sin_ref = take(8)
    out_refs = take(len(plan))
    down_own, dgot, branch_own, bgot, total_ref = take(5)
    abuf, full, r0, ag, gbuf, hg, dqkv = take(7)
    kept, sent, got = take(bits - 1), take(bits - 1), take(bits - 1)
    w1buf, w2buf, xbuf, sbuf, wobuf, fbuf, zsend, zown, mine_ref = take(9)
    near_buf, own_buf, dq_buf, hop_send, far_got, near_got = take(6)
    vgot, vsend, vnow = take(3)
    a_sem, o_sem, send_sem, recv_sem, d_send, d_recv, v_send, v_recv = take(8)
    w_sem, b_sem, h_sem, hop_sems, z_sem = take(5)
    index, me = lax.axis_index("dp"), lax.axis_index("tensor")
    last = (1 << bits) - 1
    deep, wide = full.shape[1], full.shape[2]
    rows_all = gbuf.shape[0]
    slots, ring, lag = r0.shape[0], ag.shape[0], 2

    def bit_of(bit):
        return (index // (1 << bit)) % 2

    def partner(bit):
        return index + (1 << bit) * (1 - 2 * bit_of(bit))

    barrier = pltpu.get_barrier_semaphore()

    def greet(axis, to):
        pl.semaphore_signal(barrier, inc=1, device_id={axis: to}, device_id_type=MESH)

    for bit in range(bits):
        greet("dp", partner(bit))
    for k in range(1, tensor):
        greet("tensor", lax.rem(me + k, tensor))

    @pl.when(index > 0)
    def _():
        greet("dp", index - 1)

    @pl.when(index < last)
    def _():
        greet("dp", index + 1)

    inner = jnp.where(index > 0, 1, 0) + jnp.where(index < last, 1, 0)
    pl.semaphore_wait(barrier, bits + tensor - 1 + inner)

    hidden_units = hg.shape[1] // deep

    def columns_of(u):
        return pl.ds(pl.multiple_of(u * deep, deep), deep)

    def hidden_copies(u):
        slot = lax.rem(u, 2)
        return [
            pltpu.make_async_copy(down_ref.at[columns_of(u)], w2buf.at[slot], w_sem.at[1, slot]),
            pltpu.make_async_copy(slope_ref.at[:, columns_of(u)], sbuf.at[slot], w_sem.at[3, slot]),
        ]

    row_step = min(256, rows_all)

    def hidden_unit(u):
        slot, columns = lax.rem(u, 2), columns_of(u)

        @pl.when(u + 1 < hidden_units)
        def _():
            for copy in hidden_copies(u + 1):
                copy.start()

        for copy in hidden_copies(u):
            copy.wait()

        def row_block(i, total):
            rows = pl.ds(pl.multiple_of(i * row_step, row_step), row_step)
            grad = dot_cols(gbuf[rows, :], w2buf[slot])
            low = (grad * sbuf[slot, rows, :]).astype(BF16)
            hg[rows, columns] = low
            return total + jnp.sum(low.astype(F32), 0, keepdims=True)

        total = lax.fori_loop(0, rows_all // row_step, row_block, jnp.zeros((1, deep), F32))
        mine_ref[5:6, columns] = total

    block = rows_all // blocks
    width = heads * head_dim

    def block_of(p):
        return pl.ds(pl.multiple_of(p * block, block), block)

    def far_copy(p):
        return pltpu.make_async_remote_copy(
            src_ref=far_ref.at[block_of(p)],
            dst_ref=far_got.at[block_of(p)],
            send_sem=hop_sems.at[0, p],
            recv_sem=hop_sems.at[1, p],
            device_id={"dp": jnp.maximum(index - 1, 0)},
            device_id_type=MESH,
        )

    def near_copy(p):
        return pltpu.make_async_remote_copy(
            src_ref=hop_send.at[lax.rem(p, 4)],
            dst_ref=near_got.at[block_of(p)],
            send_sem=hop_sems.at[2, p],
            recv_sem=hop_sems.at[3, p],
            device_id={"dp": jnp.maximum(index - 1, 0)},
            device_id_type=MESH,
        )

    def near_load(p):
        slot = lax.rem(p, 2)
        return pltpu.make_async_copy(near_ref.at[block_of(p)], near_buf.at[slot], h_sem.at[0, slot])

    def own_loads(p):
        slot = lax.rem(p, 2)
        return [
            pltpu.make_async_copy(own_ref.at[block_of(p)], own_buf.at[slot], h_sem.at[1, slot]),
            pltpu.make_async_copy(dq_ref.at[block_of(p)], dq_buf.at[slot], h_sem.at[2, slot]),
        ]

    def far_start(p):
        @pl.when(index > 0)
        def _():
            far_copy(p).start()

    def relay(p):
        slot = lax.rem(p, 2)

        @pl.when(index > 0)
        def _():
            far_copy(p).wait_send()

        near_load(p).wait()

        @pl.when(index < last)
        def _():
            far_copy(p).wait_recv()
            near_buf[slot] += far_got[block_of(p)].astype(F32)

        @pl.when(index > 0)
        def _():
            hop_send[lax.rem(p, 4)] = near_buf[slot].astype(BF16)
            near_copy(p).start()

    def turn_block(p):
        slot, rows = lax.rem(p, 2), block_of(p)

        @pl.when(index > 0)
        def _():
            near_copy(p).wait_send()

        for copy in own_loads(p):
            copy.wait()

        @pl.when(index < last)
        def _():
            near_copy(p).wait_recv()
            own_buf[slot] += near_got[rows].astype(F32)

        cos_block, sin_block = cos_ref[rows, :], -sin_ref[rows, :]
        lanes = cos_block.shape[1]
        for part in range(3):
            for head in range(heads):
                at = head * head_dim
                to = part * width + at
                if part == 0:
                    grad = dq_buf[slot, :, at : at + head_dim]
                else:
                    low = (part - 1) * width + at
                    grad = own_buf[slot, :, low : low + head_dim]
                if part < 2:
                    first = turn(grad[:, :lanes], cos_block, sin_block)
                    grad = jnp.concatenate([first, grad[:, lanes:]], 1)
                low_grad = grad.astype(BF16)
                dqkv[rows, to : to + head_dim] = low_grad
                mine_ref[6:7, to : to + head_dim] += jnp.sum(
                    low_grad.astype(F32), 0, keepdims=True
                )

    own_rows = down_own.shape[0]
    units = wide // deep
    zslots = zsend.shape[0]
    begin = max(chunks // 2, blocks + 4)

    def z_copy(k, v, target):
        other = lax.rem(me + k, tensor)
        rows = pl.ds(pl.multiple_of(other * own_rows, own_rows), own_rows)
        return pltpu.make_async_remote_copy(
            src_ref=zsend.at[lax.rem(v, zslots), rows],
            dst_ref=target.at[k - 1, :, columns_of(lax.rem(v, units))],
            send_sem=d_send.at[k - 1, v],
            recv_sem=d_recv.at[k - 1, v],
            device_id={"tensor": other},
            device_id_type=MESH,
        )

    def own_copy(v, target):
        slot = lax.rem(v, 2)
        return pltpu.make_async_copy(
            zown.at[slot], target.at[:, columns_of(lax.rem(v, units))], z_sem.at[slot]
        )

    def z_clear(v):
        @pl.when(v >= zslots)
        def _():
            for k in range(1, tensor):
                z_copy(k, v - zslots, dgot).wait_send()

        @pl.when(v >= 2)
        def _():
            own_copy(v - 2, down_own).wait()

    def z_put(v, i, rows, value):
        zsend[lax.rem(v, zslots), rows] = value.astype(BF16)

        @pl.when(i == me)
        def _():
            zown[lax.rem(v, 2)] = value

    def z_start(v, target, own_target):
        for k in range(1, tensor):
            z_copy(k, v, target).start()
        own_copy(v, own_target).start()

    def branch_copies(u):
        slot = lax.rem(u, 2)
        return [
            pltpu.make_async_copy(wout_ref.at[:, columns_of(u)], wobuf.at[slot], w_sem.at[4, slot]),
            pltpu.make_async_copy(forward_ref.at[:, columns_of(u)], fbuf.at[slot], w_sem.at[5, slot]),
        ]

    def branch_unit(u):
        slot = lax.rem(u, 2)

        @pl.when(u + 1 < units)
        def _():
            for copy in branch_copies(u + 1):
                copy.start()

        for copy in branch_copies(u):
            copy.wait()

        z_clear(u)

        def row_block(i, carry):
            rows = pl.ds(pl.multiple_of(i * own_rows, own_rows), own_rows)
            z_put(u, i, rows, dot(att_ref[rows, :], wobuf[slot]) + fbuf[slot, rows, :])
            return carry

        lax.fori_loop(0, tensor, row_block, 0)
        z_start(u, bgot, branch_own)

    def unit_copies(u):
        slot = lax.rem(u, 2)
        return [
            pltpu.make_async_copy(w1_ref.at[columns_of(u)], w1buf.at[slot], w_sem.at[0, slot]),
            pltpu.make_async_copy(
                up_ref.at[columns_of(u)], w2buf.at[slot, :, pl.ds(0, hg.shape[1])], w_sem.at[1, slot]
            ),
            pltpu.make_async_copy(x_ref.at[:, columns_of(u)], xbuf.at[slot], w_sem.at[2, slot]),
        ]

    def unit(u):
        slot, v = lax.rem(u, 2), units + u
        columns = columns_of(u)

        @pl.when(u + 1 < units)
        def _():
            for copy in unit_copies(u + 1):
                copy.start()

        for copy in unit_copies(u):
            copy.wait()

        z_clear(v)
        gain1, gain2 = gain1_ref[:, columns], gain2_ref[:, columns]
        mine_ref[0:4, columns] = jnp.zeros((4, deep), F32)

        def row_block(i, carry):
            rows = pl.ds(pl.multiple_of(i * own_rows, own_rows), own_rows)
            one = dot_cols(dqkv[rows, :], w1buf[slot])
            two = dot_cols(hg[rows, :], w2buf[slot, :, : hg.shape[1]])
            both = one * gain1 + two * gain2
            z_put(v, i, rows, both)
            standard = (xbuf[slot, rows].astype(F32) - mean_ref[rows, :]) * inverse_ref[rows, :]
            add = lambda v: jnp.sum(v, 0, keepdims=True)
            mine_ref[0:4, columns] += jnp.concatenate(
                [add(one * standard), add(one), add(two * standard), add(two)], 0
            )
            return carry

        lax.fori_loop(0, tensor, row_block, 0)
        z_start(v, dgot, down_own)

    def v_copy(k, to, slot):
        return pltpu.make_async_remote_copy(
            src_ref=mine_ref,
            dst_ref=vgot.at[slot],
            send_sem=v_send.at[k - 1],
            recv_sem=v_recv.at[slot],
            device_id={"tensor": to},
            device_id_type=MESH,
        )

    def v_step(bit):
        return pltpu.make_async_remote_copy(
            src_ref=vsend.at[bit],
            dst_ref=vnow.at[bit],
            send_sem=v_send.at[tensor + bit],
            recv_sem=v_recv.at[tensor + bit],
            device_id={"dp": partner(bit)},
            device_id_type=MESH,
        )

    left_at = {}
    for item, entry in enumerate(plan):
        if entry[3]:
            left_at[item] = lefts[len(left_at)]

    def fetch_copy(item, c):
        column = pl.multiple_of((c - plan[item][0]) * deep, deep)
        slot = lax.rem(c, 2)
        return pltpu.make_async_copy(
            left_at[item].at[:, pl.ds(column, deep)], abuf.at[slot], a_sem.at[slot]
        )

    def fetch(c):
        def start(item):
            if item in left_at:
                fetch_copy(item, c).start()

        on_items(c, start)

    def g_copy():
        return pltpu.make_async_copy(g_ref, gbuf, b_sem.at[0])

    def n1_copy():
        return pltpu.make_async_copy(n1_ref, gbuf, b_sem.at[1])

    def on_items(c, act):
        for item, (first, count, _, _, _) in enumerate(plan):
            @pl.when((c >= first) & (c < first + count))
            def _():
                act(item)

    even, odd = list(range(bits)), [0, *range(2, bits), 1]

    def mixed(level, parity, of):
        first, second = of(even[level]), of(odd[level])
        return first + parity * (second - first)

    def base(level, parity):
        row = 0
        for k in range(level):
            row = row + mixed(k, parity, bit_of) * (deep >> (k + 1))
        return row

    def down_copy(level, c):
        parity, slot = lax.rem(c, 2), lax.rem(c, slots)
        half = deep >> (level + 1)
        if level == 0:
            row = pl.multiple_of((1 - bit_of(0)) * half, half)
            source, target = full.at[lax.rem(c, 3), pl.ds(row, half)], r0.at[slot]
        else:
            source, target = sent[level - 1].at[slot], got[level - 1].at[slot]
        return pltpu.make_async_remote_copy(
            src_ref=source,
            dst_ref=target,
            send_sem=send_sem.at[level, lax.rem(c, ring)],
            recv_sem=recv_sem.at[level, lax.rem(c, ring)],
            device_id={"dp": mixed(level, parity, partner)},
            device_id_type=MESH,
        )

    def up_copy(level, c):
        parity, slot = lax.rem(c, 2), lax.rem(c, ring)
        size = deep >> (level + 1)
        row = base(level + 1, parity)
        rows = pl.ds(pl.multiple_of(row, size), size)
        return pltpu.make_async_remote_copy(
            src_ref=ag.at[slot, rows],
            dst_ref=ag.at[slot, rows],
            send_sem=send_sem.at[bits + level, slot],
            recv_sem=recv_sem.at[bits + level, slot],
            device_id={"dp": mixed(level, parity, partner)},
            device_id_type=MESH,
        )

    def out_copy(item, c):
        slot = lax.rem(c, ring)
        row = pl.multiple_of((c - plan[item][0]) * deep, deep)
        return pltpu.make_async_copy(
            ag.at[slot], out_refs[item].at[pl.ds(row, deep)], o_sem.at[slot]
        )

    def multiply(c):
        slot = lax.rem(c, 3)

        def with_item(item):
            _, _, right, _, local = plan[item]
            right = gbuf if right is None else hg if right == "hidden" else extra_refs[right]
            if item in left_at:
                fetch_copy(item, c).wait()
                left = abuf[lax.rem(c, 2)].T
            else:
                column = pl.multiple_of((c - plan[item][0]) * deep, deep)
                held = {"hidden": hg, "projected": dqkv, "attended": att_ref}[local]
                left = held[:, pl.ds(column, deep)].T
            step = min(512, wide)
            for column in range(0, wide, step):
                full[slot, :, column : column + step] = dot(left, right[:, column : column + step])

        on_items(c, with_item)
        down_copy(0, c).start()

    def halve(level, c):
        parity, slot = lax.rem(c, 2), lax.rem(c, slots)
        down_copy(level - 1, c).wait()
        size = deep >> level
        half = size // 2
        if level < bits:
            bit = mixed(level, parity, bit_of)
            keep = pl.multiple_of(bit * half, half)
            give = pl.multiple_of((1 - bit) * half, half)
            pieces = ((keep, True), (give, False))
        else:
            pieces = ((0, True),)
            half = size
        for row, stays in pieces:
            if level == 1:
                mine = full[
                    lax.rem(c, 3), pl.ds(pl.multiple_of(bit_of(0) * size + row, half), half)
                ]
                value = mine + r0[slot, pl.ds(row, half)]
            else:
                mine = kept[level - 2][slot, pl.ds(row, half)]
                value = mine + got[level - 2][slot, pl.ds(row, half)].astype(F32)
            if level == bits:
                at = pl.multiple_of(base(bits, parity), size)
                ag[lax.rem(c, ring), pl.ds(at, size)] = value.astype(BF16)
            elif stays:
                kept[level - 1][slot] = value
            else:
                sent[level - 1][slot] = value.astype(BF16)
        if level < bits:
            down_copy(level, c).start()
        else:
            up_copy(bits - 1, c).start()

    def widen(level, c):
        up_copy(level, c).wait()
        up_copy(level - 1, c).start()

    def finish(c):
        up_copy(0, c).wait()
        on_items(c, lambda item: out_copy(item, c).start())

    fetch(0)
    g_copy().start()
    for copy in hidden_copies(0) + branch_copies(0):
        copy.start()
    mine_ref[...] = vec_ref[...]
    g_copy().wait()

    def stage(t, delay, act):
        c = t - delay

        @pl.when((c >= 0) & (c < chunks))
        def _():
            act(c)

    def stage_of(t, first, count, act):
        @pl.when((t >= first) & (t < first + count))
        def _():
            act(t - first)

    def iteration(t, carry):
        @pl.when(t + 1 < chunks)
        def _():
            fetch(t + 1)

        @pl.when(t == plan[2][0])
        def _():
            n1_copy().start()

        @pl.when(t == plan[3][0])
        def _():
            n1_copy().wait()

        @pl.when(t == begin - 1)
        def _():
            for copy in unit_copies(0):
                copy.start()

        stage_of(t, 0, blocks, far_start)
        stage(
            t, 2 * bits * lag + 1,
            lambda c: on_items(c, lambda item: out_copy(item, c).wait()),
        )
        stage(t, 2 * bits * lag, finish)
        for level in range(1, bits):
            stage(t, (2 * bits - level) * lag, lambda c, level=level: widen(level, c))
        for level in range(bits, 0, -1):
            stage(t, level * lag, lambda c, level=level: halve(level, c))
        stage(t, 0, multiply)

        stage_of(t, 1, blocks, lambda p: near_load(p).start())
        stage_of(t, 2, blocks, relay)
        stage_of(t, 3, blocks, lambda p: [copy.start() for copy in own_loads(p)])
        stage_of(t, 4, blocks, turn_block)
        stage_of(t, 0, hidden_units, hidden_unit)
        stage_of(t, 0, units, branch_unit)
        stage_of(t, begin, units, unit)

        @pl.when(t == begin + units)
        def _():
            for k in range(1, tensor):
                v_copy(k, lax.rem(me + k, tensor), me).start()
            vgot[me] = mine_ref[...]

        @pl.when(t == begin + units + 2)
        def _():
            for k in range(1, tensor):
                other = lax.rem(me + k, tensor)
                v_copy(k, other, me).wait_send()
                v_copy(k, other, other).wait_recv()
            line = lax.broadcasted_iota(jnp.int32, mine_ref.shape, 0)
            both = vgot[0]
            for k in range(1, tensor):
                both = both + vgot[k]
            vsend[0] = jnp.where(line < 5, both, mine_ref[...])
            v_step(0).start()

        for bit in range(bits):
            @pl.when(t == begin + units + 4 + 2 * bit)
            def _():
                v_step(bit).wait()
                both = vsend[bit] + vnow[bit]
                if bit + 1 < bits:
                    vsend[bit + 1] = both
                    v_step(bit + 1).start()
                else:
                    total_ref[...] = both

        return carry

    lax.fori_loop(0, max(chunks + 2 * bits * lag + 1, begin + units + 3 + 2 * bits), iteration, 0)

    def gather(u, carry):
        for k in range(1, tensor):
            z_copy(k, u, bgot).wait_recv()
            z_copy(k, units + u, dgot).wait_recv()
        return carry

    lax.fori_loop(0, units, gather, 0)
    for v in range(2 * units - zslots, 2 * units):
        for k in range(1, tensor):
            z_copy(k, v, dgot).wait_send()
    for v in range(2 * units - 2, 2 * units):
        own_copy(v, down_own).wait()


def reduce_grads(pairs, kv_grads, dq, vectors, tables, moments_of, gains, weights, x, sizes):
    act, att, n2, grads, n1, slope, forward = pairs
    bits, tensor, heads, head_dim = sizes
    fc1_weight, fc2_weight, w1, flat_out = weights
    deep = 256
    rows, wide = grads.shape
    hidden_width, width = act.shape[1], heads * head_dim
    natural = hidden_width == wide
    shapes = [
        (hidden_width, None, True, None),
        (width, None, False, "attended"),
        (wide, "hidden", True, None) if natural else (hidden_width, 0, False, "hidden"),
        (3 * width, None, False, "projected"),
    ]
    plan, first = [], 0
    for size, right, fetched, local in shapes:
        plan.append((first, size // deep, right, fetched, local))
        first += size // deep
    chunks, ring, slots, zslots = first, 4 * bits - 2, 4, 3
    blocks = 8 if chunks >= 20 else 4
    block = rows // blocks
    own_rows, units = rows // tensor, wide // deep
    halves_of = [deep >> (level + 1) for level in range(1, bits)]
    hbm = pl.BlockSpec(memory_space=pl.ANY)
    vmem = pl.BlockSpec(memory_space=pltpu.VMEM)
    lefts = [act, n2] if natural else [act]
    extra = [] if natural else [n2]
    dims = (chunks, bits, tensor, heads, head_dim, blocks, len(extra))
    return pl.pallas_call(
        lambda *refs: reduce_kernel(plan, dims, *refs),
        name="reduce_grads",
        in_specs=[hbm] * 13 + [vmem] * len(extra) + [hbm] * len(lefts) + [vmem] * 8,
        out_specs=[hbm] * 8 + [vmem],
        out_shape=[
            *[jax.ShapeDtypeStruct((item[0], wide), BF16) for item in shapes],
            *[
                jax.ShapeDtypeStruct((own_rows, wide), F32),
                jax.ShapeDtypeStruct((tensor - 1, own_rows, wide), BF16),
            ]
            * 2,
            jax.ShapeDtypeStruct(vectors.shape, F32),
        ],
        scratch_shapes=[
            pltpu.VMEM((2, rows, deep), BF16),
            pltpu.VMEM((3, deep, wide), F32),
            pltpu.VMEM((slots, deep // 2, wide), F32),
            pltpu.VMEM((ring, deep, wide), BF16),
            pltpu.VMEM((rows, wide), BF16),
            pltpu.VMEM((rows, hidden_width), BF16),
            pltpu.VMEM((rows, 3 * width), BF16),
            *[pltpu.VMEM((slots, half, wide), F32) for half in halves_of],
            *[pltpu.VMEM((slots, half, wide), BF16) for half in halves_of],
            *[pltpu.VMEM((slots, half, wide), BF16) for half in halves_of],
            pltpu.VMEM((2, deep, 3 * width), BF16),
            pltpu.VMEM((2, deep, wide), BF16),
            pltpu.VMEM((2, rows, deep), BF16),
            pltpu.VMEM((2, rows, deep), F32),
            pltpu.VMEM((2, width, deep), BF16),
            pltpu.VMEM((2, rows, deep), F32),
            pltpu.VMEM((zslots, rows, deep), BF16),
            pltpu.VMEM((2, own_rows, deep), F32),
            pltpu.VMEM(vectors.shape, F32),
            pltpu.VMEM((2, block, 2 * width), F32),
            pltpu.VMEM((2, block, 2 * width), F32),
            pltpu.VMEM((2, block, width), F32),
            pltpu.VMEM((4, block, 2 * width), BF16),
            pltpu.VMEM((rows, 2 * width), BF16),
            pltpu.VMEM((rows, 2 * width), BF16),
            pltpu.VMEM((tensor, *vectors.shape), F32),
            pltpu.VMEM((bits, *vectors.shape), F32),
            pltpu.VMEM((bits, *vectors.shape), F32),
            pltpu.SemaphoreType.DMA((2,)),
            pltpu.SemaphoreType.DMA((ring,)),
            pltpu.SemaphoreType.DMA((2 * bits, ring)),
            pltpu.SemaphoreType.DMA((2 * bits, ring)),
            pltpu.SemaphoreType.DMA((tensor - 1, 2 * units)),
            pltpu.SemaphoreType.DMA((tensor - 1, 2 * units)),
            pltpu.SemaphoreType.DMA((tensor + bits,)),
            pltpu.SemaphoreType.DMA((tensor + bits,)),
            pltpu.SemaphoreType.DMA((6, 2)),
            pltpu.SemaphoreType.DMA((2,)),
            pltpu.SemaphoreType.DMA((3, 2)),
            pltpu.SemaphoreType.DMA((4, blocks)),
            pltpu.SemaphoreType.DMA((2,)),
        ],
        compiler_params=pltpu.CompilerParams(
            collective_id=0, has_side_effects=True, vmem_limit_bytes=63 << 20
        ),
        cost_estimate=cost(
            2 * rows * wide * (chunks * deep + 2 * hidden_width + 3 * width), 8 * chunks * deep * wide
        ),
    )(
        grads, n1, slope, fc1_weight, fc2_weight, w1, x, flat_out, forward, *kv_grads, dq,
        *extra, *lefts, att, vectors, *gains, *moments_of, *tables,
    )


def body(
    tokens, out_grad, segment_ids, positions, norm1_gain, norm1_bias, norm2_gain, norm2_bias,
    qkv_weight, qkv_bias, out_weight, out_bias, fc1_weight, fc1_bias, fc2_weight, fc2_bias,
):
    model_width, heads, _, head_dim = qkv_weight.shape
    width = heads * head_dim
    hidden_width = fc1_weight.shape[1]
    own_count = tokens.shape[0]
    tie = lax.optimization_barrier
    row = lambda v: v.reshape(1, -1).astype(F32)
    rows_all = lax.all_gather(tokens, "tensor", axis=0, tiled=True)
    grads_all = lax.all_gather(out_grad, "tensor", axis=0, tiled=True)
    row_count = rows_all.shape[0]
    flat_qkv = jnp.transpose(qkv_weight, (0, 2, 1, 3)).reshape(model_width, 3 * width)
    flat_bias = jnp.transpose(qkv_bias, (1, 0, 2)).reshape(1, 3 * width).astype(F32)
    flat_out = out_weight.reshape(width, model_width)
    cos_table, sin_table = rope_tables(positions, 128)
    normed_one, normed_two, queries, kv_own, mean, inverse = project(
        rows_all, row(norm1_gain), row(norm1_bias), row(norm2_gain), row(norm2_bias),
        flat_qkv, flat_bias, cos_table, sin_table, heads, head_dim,
    )
    reach = (MOST - 2) // row_count + 1
    kv_parts = [kv_own]
    for _ in range(reach):
        kv_parts.insert(0, shifted(kv_parts[0], "dp", 1))
    activated, slope = up(normed_two, fc1_weight, row(fc1_bias))
    forward = dot(activated, fc2_weight)
    grads_all, activated, slope, forward = tie((grads_all, activated, slope, forward))

    attended_grad = dot_cols(grads_all, flat_out).astype(BF16)
    attended, query_grad, *kv_grads = attention(
        queries, kv_parts, attended_grad, positions, heads, head_dim
    )
    own_grad = out_grad.astype(F32)
    vectors = jnp.pad(jnp.sum(own_grad, 0, keepdims=True), ((4, 3), (0, 0)))
    bits = (lax.axis_size("dp") - 1).bit_length()
    *stacked, d_sum, d_got, branch, b_got, vectors = reduce_grads(
        (activated, attended, normed_two, grads_all, normed_one, slope, forward), kv_grads, query_grad,
        vectors, (cos_table, sin_table), (mean, inverse), (row(norm1_gain), row(norm2_gain)),
        (fc1_weight, fc2_weight, flat_qkv, flat_out), rows_all,
        (bits, lax.axis_size("tensor"), heads, head_dim),
    )
    for k in range(d_got.shape[0]):
        d_sum = d_sum + d_got[k].astype(F32)
        branch = branch + b_got[k].astype(F32)
    fc2_grad, out_weight_grad, fc1_grad, qkv_weight_grad = stacked
    natural = hidden_width == model_width
    fc2_grad = widened(fc2_grad)
    out_weight_grad = out_weight_grad.astype(F32).reshape(heads, head_dim, model_width)
    fc1_grad = widened(fc1_grad) if natural else fc1_grad.T.astype(F32)
    qkv_weight_grad = jnp.transpose(spread(qkv_weight_grad, heads, head_dim), (0, 2, 1, 3))
    fc1_bias_grad = vectors[5, :hidden_width]
    qkv_bias_grad = vectors[6, : 3 * width].reshape(3, heads, head_dim)
    qkv_bias_grad = jnp.transpose(qkv_bias_grad, (1, 0, 2))
    own_rows = tokens.astype(F32)
    block_out = own_rows + branch + out_bias.astype(F32) + fc2_bias.astype(F32)
    own_mean, own_inverse = moments(own_rows)
    standard = (own_rows - own_mean) * own_inverse
    tokens_grad = own_grad + own_inverse * (
        d_sum
        - jnp.mean(d_sum, -1, keepdims=True)
        - standard * jnp.mean(d_sum * standard, -1, keepdims=True)
    )
    return (
        block_out.astype(BF16), tokens_grad.astype(BF16),
        vectors[0], vectors[1], vectors[2], vectors[3],
        qkv_weight_grad, qkv_bias_grad, out_weight_grad, vectors[4],
        fc1_grad, fc1_bias_grad, fc2_grad, vectors[4],
    )


def solution(mesh):
    rows = P(("dp", "tensor"), None)
    return jax.shard_map(
        body,
        mesh=mesh,
        in_specs=(
            rows, rows, P("dp"), P("dp"), P(), P(), P(), P(),
            P(None, "tensor", None, None), P("tensor", None, None), P("tensor", None, None), P(),
            P(None, "tensor"), P("tensor"), P("tensor", None), P(),
        ),
        out_specs=(
            rows, rows, P(), P(), P(), P(),
            P(None, "tensor", None, None), P("tensor", None, None), P("tensor", None, None), P(),
            P(None, "tensor"), P("tensor"), P("tensor", None), P(),
        ),
        check_vma=False,
    )
```

```python
import math

import jax
import jax.numpy as jnp
from jax import lax
from jax.experimental import pallas as pl
from jax.experimental.pallas import tpu as pltpu
from jax.sharding import PartitionSpec as P

ROT = 64
MOST = 2000
EPSILON = 1e-05
BF16 = jnp.bfloat16
F32 = jnp.float32
MESH = pl.DeviceIdType.MESH


def dot_rows(first, second):
    return lax.dot_general(first, second, (((0,), (0,)), ((), ())), preferred_element_type=F32)


def dot_cols(first, second):
    return lax.dot_general(first, second, (((1,), (1,)), ((), ())), preferred_element_type=F32)


def dot(first, second):
    return jnp.dot(first, second, preferred_element_type=F32)


def cost(flops, bytes_accessed):
    return pl.CostEstimate(flops=int(flops), bytes_accessed=int(bytes_accessed), transcendentals=0)


def params(*semantics):
    return pltpu.CompilerParams(dimension_semantics=semantics, vmem_limit_bytes=60 << 20)


def moments(values):
    average = jnp.mean(values, -1, keepdims=True)
    centered = values - average
    variance = jnp.mean(centered * centered, -1, keepdims=True)
    return average, lax.rsqrt(variance + EPSILON)


def rope_tables(position, lanes):
    half = ROT // 2
    frequency = jnp.power(F32(10000.0), -jnp.arange(half, dtype=F32) / F32(half))
    angles = position.astype(F32)[:, None] * frequency[None, :]
    cosine, sine = jnp.cos(angles), jnp.sin(angles)
    rows = position.shape[0]
    ones = jnp.ones((rows, lanes - ROT), F32)
    return (
        jnp.concatenate([cosine, cosine, ones], 1),
        jnp.concatenate([-sine, sine, 0 * ones], 1),
    )


def turn(values, cos_block, sin_block):
    lane = lax.broadcasted_iota(jnp.int32, values.shape, 1)
    half = ROT // 2
    up = pltpu.roll(values, values.shape[1] - half, 1)
    down = pltpu.roll(values, half, 1)
    return values * cos_block + jnp.where(lane < half, up, down) * sin_block


PIECES = 4


def front_kernel(dims, *refs):
    tensor, last, heads, head_dim = dims
    refs = list(refs)
    take = lambda count: [refs.pop(0) for _ in range(count)]
    tokens_ref, grads_ref, w4_ref, up_ref, down_ref, out_ref = take(6)
    g1_ref, b1_ref, g2_ref, b2_ref, qb_ref, ub_ref, cos_ref, sin_ref = take(8)
    rows_out, grads_out, flat_out, n1_out, n2_out, q_out, kv_own, kv_near, kv_far = take(9)
    act_out, slope_out, forward_out, agrad_out, mean_ref, inverse_ref = take(6)
    both, wq, w_up, w_down, w_out, wstage = take(6)
    n1s, n2s, qs, kvs, acts, slopes, forwards, agrads = take(8)
    own_sem, w_sem, q_sem, send_sem, recv_sem, kv_sems, s_sem = take(7)
    index, me = lax.axis_index("dp"), lax.axis_index("tensor")
    own = tokens_ref.shape[0]
    piece = own // PIECES
    width, depth = heads * head_dim, tokens_ref.shape[1]
    hidden_width = act_out.shape[1]
    span = tensor * PIECES

    barrier = pltpu.get_barrier_semaphore()

    def greet(axis, to):
        pl.semaphore_signal(barrier, inc=1, device_id={axis: to}, device_id_type=MESH)

    sides = [
        (me < tensor - 1, "tensor", me + 1),
        (me > 0, "tensor", me - 1),
        (index < last, "dp", index + 1),
        (index > 0, "dp", index - 1),
    ]
    for there, axis, to in sides:
        @pl.when(there)
        def _():
            greet(axis, to)

    pl.semaphore_wait(barrier, sum(jnp.where(there, 1, 0) for there, _, _ in sides))

    def rows_of(shard):
        return pl.ds(pl.multiple_of(shard * own, own), own)

    own_copies = [
        pltpu.make_async_copy(source, both.at[a, rows_of(me)], own_sem.at[a])
        for a, source in enumerate((tokens_ref, grads_ref))
    ]
    weight_copies = [
        pltpu.make_async_copy(up_ref, w_up, w_sem.at[0]),
        pltpu.make_async_copy(down_ref, w_down, w_sem.at[1]),
        pltpu.make_async_copy(out_ref, w_out, w_sem.at[2]),
    ]
    wrows = wstage.shape[1]

    def wq_copy(b):
        return pltpu.make_async_copy(
            w4_ref.at[pl.ds(pl.multiple_of(b * wrows, wrows), wrows)],
            wstage.at[lax.rem(b, 2)], q_sem.at[lax.rem(b, 2)],
        )

    flat_copy = pltpu.make_async_copy(wq, flat_out, w_sem.at[3])
    for copy in own_copies:
        copy.start()
    wq_copy(0).start()
    wq_copy(1).start()
    for copy in weight_copies:
        copy.start()
    for copy in own_copies:
        copy.wait()

    def hop(t, shard, p, direction):
        rows = pl.ds(pl.multiple_of(shard * own + p * piece, piece), piece)
        here = both.at[t // span, rows]
        to = me + 1 if direction == 0 else me - 1
        return pltpu.make_async_remote_copy(
            src_ref=here,
            dst_ref=here,
            send_sem=send_sem.at[direction, t],
            recv_sem=recv_sem.at[direction, t],
            device_id={"tensor": jnp.clip(to, 0, tensor - 1)},
            device_id_type=MESH,
        )

    def passing(t):
        k, p = lax.rem(t // PIECES, tensor), lax.rem(t, PIECES)
        return k, p, ((me - k, me - k >= 0, me < tensor - 1), (me + k, me + k < tensor, me > 0))

    def relay(t):
        k, p, ways = passing(t)
        for direction, (shard, held, onward) in enumerate(ways):
            @pl.when(held & (k > 0))
            def _():
                hop(t - PIECES, shard, p, direction).wait_recv()

            @pl.when(held & onward)
            def _():
                hop(t, shard, p, direction).start()

    def drain(t, carry):
        k, p, ways = passing(t)
        for direction, (shard, held, onward) in enumerate(ways):
            @pl.when(held & onward)
            def _():
                hop(t, shard, p, direction).wait_send()

        return carry

    tables = []
    for m in range(tensor):
        near = sorted(range(tensor), key=lambda shard: (abs(shard - m), shard))
        tables.append(near)

    def shard_at(j):
        found = 0
        for m in range(tensor):
            for place in range(tensor):
                hit = (me == m) & (j == place)
                found = found + jnp.where(hit, tables[m][place], 0)
        return found

    def outs_project(shard):
        rows = rows_of(shard)
        return [
            pltpu.make_async_copy(both.at[0, rows], rows_out.at[rows], s_sem.at[0]),
            pltpu.make_async_copy(n1s, n1_out.at[rows], s_sem.at[1]),
            pltpu.make_async_copy(n2s, n2_out.at[rows], s_sem.at[2]),
            pltpu.make_async_copy(qs, q_out.at[rows], s_sem.at[3]),
            pltpu.make_async_copy(kvs, kv_own.at[rows], s_sem.at[4]),
        ]

    def outs_up(shard):
        rows = rows_of(shard)
        return [
            pltpu.make_async_copy(acts, act_out.at[rows], s_sem.at[5]),
            pltpu.make_async_copy(slopes, slope_out.at[rows], s_sem.at[6]),
        ]

    def out_forward(shard):
        return pltpu.make_async_copy(forwards, forward_out.at[rows_of(shard)], s_sem.at[7])

    def outs_agrad(shard):
        rows = rows_of(shard)
        return [
            pltpu.make_async_copy(both.at[1, rows], grads_out.at[rows], s_sem.at[8]),
            pltpu.make_async_copy(agrads, agrad_out.at[rows], s_sem.at[9]),
        ]

    def near_copy(j):
        rows = rows_of(shard_at(j))
        return pltpu.make_async_remote_copy(
            src_ref=kvs,
            dst_ref=kv_near.at[rows],
            send_sem=kv_sems.at[0, j],
            recv_sem=kv_sems.at[1, j],
            device_id={"dp": jnp.minimum(index + 1, last)},
            device_id_type=MESH,
        )

    def far_copy(j):
        rows = rows_of(shard_at(j))
        return pltpu.make_async_remote_copy(
            src_ref=kv_near.at[rows],
            dst_ref=kv_far.at[rows],
            send_sem=kv_sems.at[2, j],
            recv_sem=kv_sems.at[3, j],
            device_id={"dp": jnp.minimum(index + 1, last)},
            device_id_type=MESH,
        )

    def project_shard(j):
        shard = shard_at(j)
        rows = rows_of(shard)

        @pl.when(j > 0)
        def _():
            for copy in outs_project(shard_at(j - 1)):
                copy.wait()

            @pl.when(index < last)
            def _():
                near_copy(j - 1).wait_send()

        x = both[0, rows].astype(F32)
        average, inverse = moments(x)
        mean_ref[rows, :] = average
        inverse_ref[rows, :] = inverse
        standard = (x - average) * inverse
        n1s[...] = (standard * g1_ref[...] + b1_ref[...]).astype(BF16)
        n2s[...] = (standard * g2_ref[...] + b2_ref[...]).astype(BF16)
        cos_block, sin_block = cos_ref[rows, :], sin_ref[rows, :]
        lanes = cos_block.shape[1]
        scale = 1.0 / math.sqrt(head_dim)
        for part in range(3):
            low = part * width
            projected = dot(n1s[...], wq[:, low : low + width]) + qb_ref[:, low : low + width]
            if part == 2:
                kvs[:, width:] = projected.astype(BF16)
                continue
            for head in range(heads):
                at = head * head_dim
                turned = turn(projected[:, at : at + lanes], cos_block, sin_block)
                other = projected[:, at + lanes : at + head_dim]
                if part == 0:
                    qs[:, at : at + lanes] = (turned * scale).astype(BF16)
                    qs[:, at + lanes : at + head_dim] = (other * scale).astype(BF16)
                else:
                    kvs[:, at : at + lanes] = turned.astype(BF16)
                    kvs[:, at + lanes : at + head_dim] = other.astype(BF16)
        for copy in outs_project(shard):
            copy.start()

        @pl.when(index < last)
        def _():
            near_copy(j).start()

    def up_half(j, half):
        if half == 0:
            @pl.when(j > 0)
            def _():
                for copy in outs_up(shard_at(j - 1)):
                    copy.wait()

        size = hidden_width // 2
        step = min(512, size)
        for column in range(half * size, (half + 1) * size, step):
            part = slice(column, column + step)
            hidden = dot(n2s[...], w_up[:, part]) + ub_ref[:, part]
            phi = (1.0 + lax.erf(hidden * F32(math.sqrt(0.5)))) * 0.5
            acts[:, part] = (hidden * phi).astype(BF16)
            density = jnp.exp(hidden * hidden * -0.5) * F32(1.0 / math.sqrt(2.0 * math.pi))
            slopes[:, part] = phi + hidden * density
        if half == 1:
            for copy in outs_up(shard_at(j)):
                copy.start()

    def forward_shard(j):
        @pl.when(j > 0)
        def _():
            out_forward(shard_at(j - 1)).wait()

        step = min(512, depth)
        for column in range(0, depth, step):
            part = slice(column, column + step)
            forwards[:, part] = dot(acts[...], w_down[:, part])
        out_forward(shard_at(j)).start()

    def pass_kv(j):
        @pl.when(index > 0)
        def _():
            near_copy(j).wait_recv()

            @pl.when(index < last)
            def _():
                far_copy(j).start()

    def agrad_shard(j):
        @pl.when(j > 0)
        def _():
            for copy in outs_agrad(shard_at(j - 1)):
                copy.wait()

        shard = shard_at(j)
        agrads[...] = dot_cols(both[1, rows_of(shard)], w_out[...]).astype(BF16)
        for copy in outs_agrad(shard):
            copy.start()

    def on(condition, act):
        @pl.when(condition)
        def _():
            act()

    def slot(t, carry):
        on(t < 2 * span, lambda: relay(t))

        @pl.when(t == 2)
        def _():
            for b in range(depth // wrows):
                wq_copy(b).wait()
                for part in range(3):
                    wq[b * wrows : (b + 1) * wrows, part * width : (part + 1) * width] = wstage[
                        b % 2, :, part
                    ].reshape(wrows, width)
                if b + 2 < depth // wrows:
                    wq_copy(b + 2).start()
            flat_copy.start()

        j, sub = t // PIECES - 1, lax.rem(t, PIECES)
        working = (j >= 0) & (j < tensor)
        on(working & (sub == 0), lambda: project_shard(j))

        @pl.when(t == PIECES + 1)
        def _():
            weight_copies[0].wait()

        on(working & (sub == 1), lambda: up_half(j, 0))
        on(working & (sub == 2), lambda: up_half(j, 1))

        @pl.when(t == PIECES + 3)
        def _():
            weight_copies[1].wait()

        on(working & (sub == 3), lambda: forward_shard(j))
        before = j - 1
        on((before >= 0) & (before < tensor) & (sub == 1), lambda: pass_kv(before))

        @pl.when(t == span + PIECES)
        def _():
            weight_copies[2].wait()

        late = j - tensor
        on((late >= 0) & (late < tensor) & (sub == 0), lambda: agrad_shard(late))
        return carry

    lax.fori_loop(0, 2 * span + 1, slot, 0)
    final = shard_at(tensor - 1)
    for copy in outs_project(final) + outs_up(final) + [out_forward(final)] + outs_agrad(final):
        copy.wait()
    flat_copy.wait()

    @pl.when(index < last)
    def _():
        near_copy(tensor - 1).wait_send()

    def kv_drain(j, carry):
        @pl.when((index > 0) & (index < last))
        def _():
            far_copy(j).wait_send()

        @pl.when(index > 1)
        def _():
            far_copy(j).wait_recv()

        return carry

    lax.fori_loop(0, tensor, kv_drain, 0)
    lax.fori_loop(0, 2 * span, drain, 0)


def front(tokens, grads, w4, fc1_weight, fc2_weight, flat_out, small, tables, sizes):
    tensor, last, heads, head_dim = sizes
    own, depth = tokens.shape
    rows, width, hidden_width = own * tensor, heads * head_dim, fc1_weight.shape[1]
    span, wrows = tensor * PIECES, 256
    hbm = pl.BlockSpec(memory_space=pl.ANY)
    vmem = pl.BlockSpec(memory_space=pltpu.VMEM)
    shape = jax.ShapeDtypeStruct
    return pl.pallas_call(
        lambda *refs: front_kernel(sizes, *refs),
        name="front",
        in_specs=[hbm] * 6 + [vmem] * 8,
        out_specs=[hbm] * 13 + [vmem] * 2,
        out_shape=[
            shape((rows, depth), BF16),
            shape((rows, depth), BF16),
            shape((depth, 3 * width), BF16),
            shape((rows, depth), BF16),
            shape((rows, depth), BF16),
            shape((rows, width), BF16),
            *[shape((rows, 2 * width), BF16)] * 3,
            shape((rows, hidden_width), BF16),
            shape((rows, hidden_width), F32),
            shape((rows, depth), F32),
            shape((rows, width), BF16),
            shape((rows, 1), F32),
            shape((rows, 1), F32),
        ],
        scratch_shapes=[
            pltpu.VMEM((2, rows, depth), BF16),
            pltpu.VMEM((depth, 3 * width), BF16),
            pltpu.VMEM((depth, hidden_width), BF16),
            pltpu.VMEM((hidden_width, depth), BF16),
            pltpu.VMEM((width, depth), BF16),
            pltpu.VMEM((2, wrows, 3, heads, head_dim), BF16),
            pltpu.VMEM((own, depth), BF16),
            pltpu.VMEM((own, depth), BF16),
            pltpu.VMEM((own, width), BF16),
            pltpu.VMEM((own, 2 * width), BF16),
            pltpu.VMEM((own, hidden_width), BF16),
            pltpu.VMEM((own, hidden_width), F32),
            pltpu.VMEM((own, depth), F32),
            pltpu.VMEM((own, width), BF16),
            pltpu.SemaphoreType.DMA((2,)),
            pltpu.SemaphoreType.DMA((4,)),
            pltpu.SemaphoreType.DMA((2,)),
            pltpu.SemaphoreType.DMA((2, 2 * span)),
            pltpu.SemaphoreType.DMA((2, 2 * span)),
            pltpu.SemaphoreType.DMA((4, tensor)),
            pltpu.SemaphoreType.DMA((10,)),
        ],
        compiler_params=pltpu.CompilerParams(
            collective_id=1, has_side_effects=True, vmem_limit_bytes=62 << 20
        ),
        cost_estimate=cost(
            2 * rows * depth * (3 * width + 2 * hidden_width + width),
            2 * rows * (6 * depth + 4 * hidden_width),
        ),
    )(tokens, grads, w4, fc1_weight, fc2_weight, flat_out, *small, *tables)


def attention_kernel(heads, head_dim, parts, bk, first_ref, q_ref, do_ref, start_ref, *refs):
    kv_parts, refs = refs[:parts], refs[parts:]
    att_ref, dq_ref, refs = refs[0], refs[1], refs[2:]
    grad_parts, (kv_ref, dkv_ref, s_ref, dp_ref, o_ref, sems) = refs[:parts], refs[parts:]
    block = pl.program_id(0)
    bq = q_ref.shape[0]
    width = heads * head_dim
    rows_each = kv_ref.shape[0] // parts
    ahead = rows_each * (parts - 1)
    low = first_ref[block]
    high = (ahead + (block + 1) * bq + bk - 1) // bk
    row = ahead + block * bq + lax.broadcasted_iota(jnp.int32, (bq, 1), 0)
    start = start_ref[...]
    lane = lax.broadcasted_iota(jnp.int32, (bq, bk), 1)
    chunks = bk // 128

    @pl.when(block == 0)
    def _():
        copies = [
            pltpu.make_async_copy(
                part, kv_ref.at[pl.ds(k * rows_each, rows_each)], sems.at[k]
            )
            for k, part in enumerate(kv_parts)
        ]
        for copy in copies:
            copy.start()

        def clear(j, carry):
            dkv_ref[pl.ds(pl.multiple_of(j * 128, 128), 128), :] = jnp.zeros((128, 2 * width), F32)
            return carry

        lax.fori_loop(0, dkv_ref.shape[0] // 128, clear, 0)
        for copy in copies:
            copy.wait()

    for head in range(heads):
        at = head * head_dim
        q = q_ref[:, at : at + head_dim]
        do = do_ref[:, at : at + head_dim]

        def rows_of(j):
            return pl.ds(pl.multiple_of(j * bk, bk), bk)

        def scores(j, best):
            s = dot_cols(q, kv_ref[rows_of(j), at : at + head_dim])
            column = j * bk + lane
            s = jnp.where((column >= start) & (column <= row), s, -1e30)
            s_ref[j] = s
            for c in range(chunks):
                best = jnp.maximum(best, s[:, c * 128 : (c + 1) * 128])
            return best

        best = lax.fori_loop(low, high, scores, jnp.full((bq, 128), -1e30, F32))
        best = jnp.max(best, 1, keepdims=True)

        def weigh(j, carry):
            total, mixed = carry
            e = jnp.exp(s_ref[j] - best)
            dp = dot_cols(do, kv_ref[rows_of(j), width + at : width + at + head_dim])
            s_ref[j] = e
            dp_ref[j] = dp
            both = e * dp
            for c in range(chunks):
                total = total + e[:, c * 128 : (c + 1) * 128]
                mixed = mixed + both[:, c * 128 : (c + 1) * 128]
            return total, mixed

        zero = jnp.zeros((bq, 128), F32)
        total, mixed = lax.fori_loop(low, high, weigh, (zero, zero))
        total = jnp.sum(total, 1, keepdims=True)
        scale = 1.0 / total
        delta = jnp.sum(mixed, 1, keepdims=True) * scale
        o_ref[...] = jnp.zeros_like(o_ref)

        def spread(j, carry):
            rows = rows_of(j)
            p = s_ref[j] * scale
            p_low = p.astype(BF16)
            ds = (p * (dp_ref[j] - delta)).astype(BF16)
            k = kv_ref[rows, at : at + head_dim]
            v = kv_ref[rows, width + at : width + at + head_dim]
            o_ref[:, :head_dim] += dot(p_low, v)
            o_ref[:, head_dim:] += dot(ds, k)
            dkv_ref[rows, at : at + head_dim] += dot_rows(ds, q)
            dkv_ref[rows, width + at : width + at + head_dim] += dot_rows(p_low, do)
            return carry

        lax.fori_loop(low, high, spread, 0)
        att_ref[:, at : at + head_dim] = o_ref[:, :head_dim].astype(BF16)
        dq_ref[:, at : at + head_dim] = o_ref[:, head_dim:] * (1.0 / math.sqrt(head_dim))

    @pl.when(block == pl.num_programs(0) - 1)
    def _():
        for k, part in enumerate(grad_parts):
            part[...] = dkv_ref[k * rows_each : (k + 1) * rows_each, :].astype(part.dtype)


def attention(q, kv_parts, do, positions, heads, head_dim):
    rows, width = q.shape
    parts = len(kv_parts)
    total = rows * parts
    bq = min(256, rows)
    bk = 256
    start = jnp.arange(rows, dtype=jnp.int32) - positions + (total - rows)
    first = start[::bq] // bk
    by_row = lambda i, f: (i, 0)
    whole = lambda i, f: (0, 0)
    part_types = [BF16] + [F32] * (parts - 1)
    return pl.pallas_call(
        lambda *refs: attention_kernel(heads, head_dim, parts, bk, *refs),
        name="attention",
        grid_spec=pltpu.PrefetchScalarGridSpec(
            num_scalar_prefetch=1,
            grid=(rows // bq,),
            in_specs=[
                pl.BlockSpec((bq, width), by_row),
                pl.BlockSpec((bq, width), by_row),
                pl.BlockSpec((bq, 1), by_row),
                *[pl.BlockSpec(memory_space=pl.ANY)] * parts,
            ],
            out_specs=[
                pl.BlockSpec((bq, width), by_row),
                pl.BlockSpec((bq, width), by_row),
                *[pl.BlockSpec((rows, 2 * width), whole, pipeline_mode=pl.Buffered(1))] * parts,
            ],
            scratch_shapes=[
                pltpu.VMEM((total, 2 * width), BF16),
                pltpu.VMEM((total, 2 * width), F32),
                pltpu.VMEM((total // bk, bq, bk), F32),
                pltpu.VMEM((total // bk, bq, bk), F32),
                pltpu.VMEM((bq, 2 * head_dim), F32),
                pltpu.SemaphoreType.DMA((parts,)),
            ],
        ),
        out_shape=[
            jax.ShapeDtypeStruct((rows, width), BF16),
            jax.ShapeDtypeStruct((rows, width), F32),
            *[jax.ShapeDtypeStruct((rows, 2 * width), kind) for kind in part_types],
        ],
        compiler_params=params("arbitrary"),
        cost_estimate=cost(12 * rows * MOST * width, 8 * total * width),
    )(first, q, do, start[:, None], *kv_parts)


def widen_kernel(in_ref, out_ref):
    out_ref[...] = in_ref[...].astype(F32)


def widened(x):
    rows, depth = x.shape
    block = min(512, rows)
    return pl.pallas_call(
        widen_kernel,
        name="widened",
        grid=(rows // block,),
        in_specs=[pl.BlockSpec((block, depth), lambda i: (i, 0))],
        out_specs=pl.BlockSpec((block, depth), lambda i: (i, 0)),
        out_shape=jax.ShapeDtypeStruct(x.shape, F32),
        compiler_params=params("arbitrary"),
        cost_estimate=cost(0, 6 * x.size),
    )(x)


def spread_kernel(heads, head_dim, in_ref, out_ref):
    for head in range(heads):
        block = in_ref[head * head_dim : (head + 1) * head_dim, :]
        out_ref[:, 0, head, :] = block.T.astype(F32)


def spread(stacked, heads, head_dim):
    depth = stacked.shape[1]
    block = min(1024, depth)
    return pl.pallas_call(
        lambda *refs: spread_kernel(heads, head_dim, *refs),
        name="spread",
        grid=(depth // block, 3),
        in_specs=[pl.BlockSpec((heads * head_dim, block), lambda i, j: (j, i))],
        out_specs=pl.BlockSpec((block, 1, heads, head_dim), lambda i, j: (i, j, 0, 0)),
        out_shape=jax.ShapeDtypeStruct((depth, 3, heads, head_dim), F32),
        compiler_params=params("arbitrary", "arbitrary"),
        cost_estimate=cost(0, 6 * stacked.size),
    )(stacked)


def reduce_kernel(plan, dims, *refs):
    chunks, bits, tensor, heads, head_dim, blocks, wide_b = dims
    refs = list(refs)
    take = lambda count: [refs.pop(0) for _ in range(count)]
    g_ref, n1_ref, slope_ref, up_ref, down_ref, w1_ref, x_ref, wout_ref, forward_ref = take(9)
    far_ref, near_ref, own_ref, dq_ref = take(4)
    extra_refs = take(wide_b)
    lefts = take(sum(1 for item in plan if item[3]))
    att_ref, vec_ref, gain1_ref, gain2_ref, mean_ref, inverse_ref, cos_ref, sin_ref = take(8)
    out_refs = take(len(plan))
    down_own, dgot, branch_own, bgot, total_ref = take(5)
    abuf, full, r0, ag, gbuf, hg, dqkv = take(7)
    kept, sent, got = take(bits - 1), take(bits - 1), take(bits - 1)
    w1buf, w2buf, xbuf, sbuf, wobuf, fbuf, zsend, zown, mine_ref = take(9)
    near_buf, own_buf, dq_buf, hop_send, far_got, near_got = take(6)
    vgot, vsend, vnow = take(3)
    a_sem, o_sem, send_sem, recv_sem, d_send, d_recv, v_send, v_recv = take(8)
    w_sem, b_sem, h_sem, hop_sems, z_sem = take(5)
    index, me = lax.axis_index("dp"), lax.axis_index("tensor")
    last = (1 << bits) - 1
    deep, wide = full.shape[1], full.shape[2]
    rows_all = gbuf.shape[0]
    slots, ring, lag = r0.shape[0], ag.shape[0], 2

    def bit_of(bit):
        return (index // (1 << bit)) % 2

    def partner(bit):
        return index + (1 << bit) * (1 - 2 * bit_of(bit))

    barrier = pltpu.get_barrier_semaphore()

    def greet(axis, to):
        pl.semaphore_signal(barrier, inc=1, device_id={axis: to}, device_id_type=MESH)

    for bit in range(bits):
        greet("dp", partner(bit))
    for k in range(1, tensor):
        greet("tensor", lax.rem(me + k, tensor))

    @pl.when(index > 0)
    def _():
        greet("dp", index - 1)

    @pl.when(index < last)
    def _():
        greet("dp", index + 1)

    inner = jnp.where(index > 0, 1, 0) + jnp.where(index < last, 1, 0)
    pl.semaphore_wait(barrier, bits + tensor - 1 + inner)

    hidden_units = hg.shape[1] // deep

    def columns_of(u):
        return pl.ds(pl.multiple_of(u * deep, deep), deep)

    def hidden_copies(u):
        slot = lax.rem(u, 2)
        return [
            pltpu.make_async_copy(down_ref.at[columns_of(u)], w2buf.at[slot], w_sem.at[1, slot]),
            pltpu.make_async_copy(slope_ref.at[:, columns_of(u)], sbuf.at[slot], w_sem.at[3, slot]),
        ]

    row_step = min(256, rows_all)

    def hidden_unit(u):
        slot, columns = lax.rem(u, 2), columns_of(u)

        @pl.when(u + 1 < hidden_units)
        def _():
            for copy in hidden_copies(u + 1):
                copy.start()

        for copy in hidden_copies(u):
            copy.wait()

        def row_block(i, total):
            rows = pl.ds(pl.multiple_of(i * row_step, row_step), row_step)
            grad = dot_cols(gbuf[rows, :], w2buf[slot])
            low = (grad * sbuf[slot, rows, :]).astype(BF16)
            hg[rows, columns] = low
            return total + jnp.sum(low.astype(F32), 0, keepdims=True)

        total = lax.fori_loop(0, rows_all // row_step, row_block, jnp.zeros((1, deep), F32))
        mine_ref[5:6, columns] = total

    block = rows_all // blocks
    width = heads * head_dim

    def block_of(p):
        return pl.ds(pl.multiple_of(p * block, block), block)

    def far_copy(p):
        return pltpu.make_async_remote_copy(
            src_ref=far_ref.at[block_of(p)],
            dst_ref=far_got.at[block_of(p)],
            send_sem=hop_sems.at[0, p],
            recv_sem=hop_sems.at[1, p],
            device_id={"dp": jnp.maximum(index - 1, 0)},
            device_id_type=MESH,
        )

    def near_copy(p):
        return pltpu.make_async_remote_copy(
            src_ref=hop_send.at[lax.rem(p, 4)],
            dst_ref=near_got.at[block_of(p)],
            send_sem=hop_sems.at[2, p],
            recv_sem=hop_sems.at[3, p],
            device_id={"dp": jnp.maximum(index - 1, 0)},
            device_id_type=MESH,
        )

    def near_load(p):
        slot = lax.rem(p, 2)
        return pltpu.make_async_copy(near_ref.at[block_of(p)], near_buf.at[slot], h_sem.at[0, slot])

    def own_loads(p):
        slot = lax.rem(p, 2)
        return [
            pltpu.make_async_copy(own_ref.at[block_of(p)], own_buf.at[slot], h_sem.at[1, slot]),
            pltpu.make_async_copy(dq_ref.at[block_of(p)], dq_buf.at[slot], h_sem.at[2, slot]),
        ]

    def far_start(p):
        @pl.when(index > 0)
        def _():
            far_copy(p).start()

    def relay(p):
        slot = lax.rem(p, 2)

        @pl.when(index > 0)
        def _():
            far_copy(p).wait_send()

        near_load(p).wait()

        @pl.when(index < last)
        def _():
            far_copy(p).wait_recv()
            near_buf[slot] += far_got[block_of(p)].astype(F32)

        @pl.when(index > 0)
        def _():
            hop_send[lax.rem(p, 4)] = near_buf[slot].astype(BF16)
            near_copy(p).start()

    def turn_block(p):
        slot, rows = lax.rem(p, 2), block_of(p)

        @pl.when(index > 0)
        def _():
            near_copy(p).wait_send()

        for copy in own_loads(p):
            copy.wait()

        @pl.when(index < last)
        def _():
            near_copy(p).wait_recv()
            own_buf[slot] += near_got[rows].astype(F32)

        cos_block, sin_block = cos_ref[rows, :], -sin_ref[rows, :]
        lanes = cos_block.shape[1]
        for part in range(3):
            for head in range(heads):
                at = head * head_dim
                to = part * width + at
                if part == 0:
                    grad = dq_buf[slot, :, at : at + head_dim]
                else:
                    low = (part - 1) * width + at
                    grad = own_buf[slot, :, low : low + head_dim]
                if part < 2:
                    first = turn(grad[:, :lanes], cos_block, sin_block)
                    grad = jnp.concatenate([first, grad[:, lanes:]], 1)
                low_grad = grad.astype(BF16)
                dqkv[rows, to : to + head_dim] = low_grad
                mine_ref[6:7, to : to + head_dim] += jnp.sum(
                    low_grad.astype(F32), 0, keepdims=True
                )

    own_rows = down_own.shape[0]
    units = wide // deep
    zslots = zsend.shape[0]
    begin = max(chunks // 2, blocks + 4)

    def z_copy(k, v, target):
        other = lax.rem(me + k, tensor)
        rows = pl.ds(pl.multiple_of(other * own_rows, own_rows), own_rows)
        return pltpu.make_async_remote_copy(
            src_ref=zsend.at[lax.rem(v, zslots), rows],
            dst_ref=target.at[k - 1, :, columns_of(lax.rem(v, units))],
            send_sem=d_send.at[k - 1, v],
            recv_sem=d_recv.at[k - 1, v],
            device_id={"tensor": other},
            device_id_type=MESH,
        )

    def own_copy(v, target):
        slot = lax.rem(v, 2)
        return pltpu.make_async_copy(
            zown.at[slot], target.at[:, columns_of(lax.rem(v, units))], z_sem.at[slot]
        )

    def z_clear(v):
        @pl.when(v >= zslots)
        def _():
            for k in range(1, tensor):
                z_copy(k, v - zslots, dgot).wait_send()

        @pl.when(v >= 2)
        def _():
            own_copy(v - 2, down_own).wait()

    def z_put(v, i, rows, value):
        zsend[lax.rem(v, zslots), rows] = value.astype(BF16)

        @pl.when(i == me)
        def _():
            zown[lax.rem(v, 2)] = value

    def z_start(v, target, own_target):
        for k in range(1, tensor):
            z_copy(k, v, target).start()
        own_copy(v, own_target).start()

    def branch_copies(u):
        slot = lax.rem(u, 2)
        return [
            pltpu.make_async_copy(wout_ref.at[:, columns_of(u)], wobuf.at[slot], w_sem.at[4, slot]),
            pltpu.make_async_copy(forward_ref.at[:, columns_of(u)], fbuf.at[slot], w_sem.at[5, slot]),
        ]

    def branch_unit(u):
        slot = lax.rem(u, 2)

        @pl.when(u + 1 < units)
        def _():
            for copy in branch_copies(u + 1):
                copy.start()

        for copy in branch_copies(u):
            copy.wait()

        z_clear(u)

        def row_block(i, carry):
            rows = pl.ds(pl.multiple_of(i * own_rows, own_rows), own_rows)
            z_put(u, i, rows, dot(att_ref[rows, :], wobuf[slot]) + fbuf[slot, rows, :])
            return carry

        lax.fori_loop(0, tensor, row_block, 0)
        z_start(u, bgot, branch_own)

    def unit_copies(u):
        slot = lax.rem(u, 2)
        return [
            pltpu.make_async_copy(w1_ref.at[columns_of(u)], w1buf.at[slot], w_sem.at[0, slot]),
            pltpu.make_async_copy(
                up_ref.at[columns_of(u)], w2buf.at[slot, :, pl.ds(0, hg.shape[1])], w_sem.at[1, slot]
            ),
            pltpu.make_async_copy(x_ref.at[:, columns_of(u)], xbuf.at[slot], w_sem.at[2, slot]),
        ]

    def unit(u):
        slot, v = lax.rem(u, 2), units + u
        columns = columns_of(u)

        @pl.when(u + 1 < units)
        def _():
            for copy in unit_copies(u + 1):
                copy.start()

        for copy in unit_copies(u):
            copy.wait()

        z_clear(v)
        gain1, gain2 = gain1_ref[:, columns], gain2_ref[:, columns]
        mine_ref[0:4, columns] = jnp.zeros((4, deep), F32)

        def row_block(i, carry):
            rows = pl.ds(pl.multiple_of(i * own_rows, own_rows), own_rows)
            one = dot_cols(dqkv[rows, :], w1buf[slot])
            two = dot_cols(hg[rows, :], w2buf[slot, :, : hg.shape[1]])
            both = one * gain1 + two * gain2
            z_put(v, i, rows, both)
            standard = (xbuf[slot, rows].astype(F32) - mean_ref[rows, :]) * inverse_ref[rows, :]
            add = lambda v: jnp.sum(v, 0, keepdims=True)
            mine_ref[0:4, columns] += jnp.concatenate(
                [add(one * standard), add(one), add(two * standard), add(two)], 0
            )
            return carry

        lax.fori_loop(0, tensor, row_block, 0)
        z_start(v, dgot, down_own)

    def v_copy(k, to, slot):
        return pltpu.make_async_remote_copy(
            src_ref=mine_ref,
            dst_ref=vgot.at[slot],
            send_sem=v_send.at[k - 1],
            recv_sem=v_recv.at[slot],
            device_id={"tensor": to},
            device_id_type=MESH,
        )

    def v_step(bit):
        return pltpu.make_async_remote_copy(
            src_ref=vsend.at[bit],
            dst_ref=vnow.at[bit],
            send_sem=v_send.at[tensor + bit],
            recv_sem=v_recv.at[tensor + bit],
            device_id={"dp": partner(bit)},
            device_id_type=MESH,
        )

    left_at = {}
    for item, entry in enumerate(plan):
        if entry[3]:
            left_at[item] = lefts[len(left_at)]

    def fetch_copy(item, c):
        column = pl.multiple_of((c - plan[item][0]) * deep, deep)
        slot = lax.rem(c, 2)
        return pltpu.make_async_copy(
            left_at[item].at[:, pl.ds(column, deep)], abuf.at[slot], a_sem.at[slot]
        )

    def fetch(c):
        def start(item):
            if item in left_at:
                fetch_copy(item, c).start()

        on_items(c, start)

    def g_copy():
        return pltpu.make_async_copy(g_ref, gbuf, b_sem.at[0])

    def n1_copy():
        return pltpu.make_async_copy(n1_ref, gbuf, b_sem.at[1])

    def on_items(c, act):
        for item, (first, count, _, _, _) in enumerate(plan):
            @pl.when((c >= first) & (c < first + count))
            def _():
                act(item)

    even, odd = list(range(bits)), [0, *range(2, bits), 1]

    def mixed(level, parity, of):
        first, second = of(even[level]), of(odd[level])
        return first + parity * (second - first)

    def base(level, parity):
        row = 0
        for k in range(level):
            row = row + mixed(k, parity, bit_of) * (deep >> (k + 1))
        return row

    def down_copy(level, c):
        parity, slot = lax.rem(c, 2), lax.rem(c, slots)
        half = deep >> (level + 1)
        if level == 0:
            row = pl.multiple_of((1 - bit_of(0)) * half, half)
            source, target = full.at[lax.rem(c, 3), pl.ds(row, half)], r0.at[slot]
        else:
            source, target = sent[level - 1].at[slot], got[level - 1].at[slot]
        return pltpu.make_async_remote_copy(
            src_ref=source,
            dst_ref=target,
            send_sem=send_sem.at[level, lax.rem(c, ring)],
            recv_sem=recv_sem.at[level, lax.rem(c, ring)],
            device_id={"dp": mixed(level, parity, partner)},
            device_id_type=MESH,
        )

    def up_copy(level, c):
        parity, slot = lax.rem(c, 2), lax.rem(c, ring)
        size = deep >> (level + 1)
        row = base(level + 1, parity)
        rows = pl.ds(pl.multiple_of(row, size), size)
        return pltpu.make_async_remote_copy(
            src_ref=ag.at[slot, rows],
            dst_ref=ag.at[slot, rows],
            send_sem=send_sem.at[bits + level, slot],
            recv_sem=recv_sem.at[bits + level, slot],
            device_id={"dp": mixed(level, parity, partner)},
            device_id_type=MESH,
        )

    def out_copy(item, c):
        slot = lax.rem(c, ring)
        row = pl.multiple_of((c - plan[item][0]) * deep, deep)
        return pltpu.make_async_copy(
            ag.at[slot], out_refs[item].at[pl.ds(row, deep)], o_sem.at[slot]
        )

    def multiply(c):
        slot = lax.rem(c, 3)

        def with_item(item):
            _, _, right, _, local = plan[item]
            right = gbuf if right is None else hg if right == "hidden" else extra_refs[right]
            if item in left_at:
                fetch_copy(item, c).wait()
                left = abuf[lax.rem(c, 2)].T
            else:
                column = pl.multiple_of((c - plan[item][0]) * deep, deep)
                held = {"hidden": hg, "projected": dqkv, "attended": att_ref}[local]
                left = held[:, pl.ds(column, deep)].T
            step = min(512, wide)
            for column in range(0, wide, step):
                full[slot, :, column : column + step] = dot(left, right[:, column : column + step])

        on_items(c, with_item)
        down_copy(0, c).start()

    def halve(level, c):
        parity, slot = lax.rem(c, 2), lax.rem(c, slots)
        down_copy(level - 1, c).wait()
        size = deep >> level
        half = size // 2
        if level < bits:
            bit = mixed(level, parity, bit_of)
            keep = pl.multiple_of(bit * half, half)
            give = pl.multiple_of((1 - bit) * half, half)
            pieces = ((keep, True), (give, False))
        else:
            pieces = ((0, True),)
            half = size
        for row, stays in pieces:
            if level == 1:
                mine = full[
                    lax.rem(c, 3), pl.ds(pl.multiple_of(bit_of(0) * size + row, half), half)
                ]
                value = mine + r0[slot, pl.ds(row, half)]
            else:
                mine = kept[level - 2][slot, pl.ds(row, half)]
                value = mine + got[level - 2][slot, pl.ds(row, half)].astype(F32)
            if level == bits:
                at = pl.multiple_of(base(bits, parity), size)
                ag[lax.rem(c, ring), pl.ds(at, size)] = value.astype(BF16)
            elif stays:
                kept[level - 1][slot] = value
            else:
                sent[level - 1][slot] = value.astype(BF16)
        if level < bits:
            down_copy(level, c).start()
        else:
            up_copy(bits - 1, c).start()

    def widen(level, c):
        up_copy(level, c).wait()
        up_copy(level - 1, c).start()

    def finish(c):
        up_copy(0, c).wait()
        on_items(c, lambda item: out_copy(item, c).start())

    fetch(0)
    g_copy().start()
    for copy in hidden_copies(0) + branch_copies(0):
        copy.start()
    mine_ref[...] = vec_ref[...]
    g_copy().wait()

    def stage(t, delay, act):
        c = t - delay

        @pl.when((c >= 0) & (c < chunks))
        def _():
            act(c)

    def stage_of(t, first, count, act):
        @pl.when((t >= first) & (t < first + count))
        def _():
            act(t - first)

    def iteration(t, carry):
        @pl.when(t + 1 < chunks)
        def _():
            fetch(t + 1)

        @pl.when(t == plan[2][0])
        def _():
            n1_copy().start()

        @pl.when(t == plan[3][0])
        def _():
            n1_copy().wait()

        @pl.when(t == begin - 1)
        def _():
            for copy in unit_copies(0):
                copy.start()

        stage_of(t, 0, blocks, far_start)
        stage(
            t, 2 * bits * lag + 1,
            lambda c: on_items(c, lambda item: out_copy(item, c).wait()),
        )
        stage(t, 2 * bits * lag, finish)
        for level in range(1, bits):
            stage(t, (2 * bits - level) * lag, lambda c, level=level: widen(level, c))
        for level in range(bits, 0, -1):
            stage(t, level * lag, lambda c, level=level: halve(level, c))
        stage(t, 0, multiply)

        stage_of(t, 1, blocks, lambda p: near_load(p).start())
        stage_of(t, 2, blocks, relay)
        stage_of(t, 3, blocks, lambda p: [copy.start() for copy in own_loads(p)])
        stage_of(t, 4, blocks, turn_block)
        stage_of(t, 0, hidden_units, hidden_unit)
        stage_of(t, 0, units, branch_unit)
        stage_of(t, begin, units, unit)

        @pl.when(t == begin + units)
        def _():
            for k in range(1, tensor):
                v_copy(k, lax.rem(me + k, tensor), me).start()
            vgot[me] = mine_ref[...]

        @pl.when(t == begin + units + 2)
        def _():
            for k in range(1, tensor):
                other = lax.rem(me + k, tensor)
                v_copy(k, other, me).wait_send()
                v_copy(k, other, other).wait_recv()
            line = lax.broadcasted_iota(jnp.int32, mine_ref.shape, 0)
            both = vgot[0]
            for k in range(1, tensor):
                both = both + vgot[k]
            vsend[0] = jnp.where(line < 5, both, mine_ref[...])
            v_step(0).start()

        for bit in range(bits):
            @pl.when(t == begin + units + 4 + 2 * bit)
            def _():
                v_step(bit).wait()
                both = vsend[bit] + vnow[bit]
                if bit + 1 < bits:
                    vsend[bit + 1] = both
                    v_step(bit + 1).start()
                else:
                    total_ref[...] = both

        return carry

    lax.fori_loop(0, max(chunks + 2 * bits * lag + 1, begin + units + 3 + 2 * bits), iteration, 0)

    def gather(u, carry):
        for k in range(1, tensor):
            z_copy(k, u, bgot).wait_recv()
            z_copy(k, units + u, dgot).wait_recv()
        return carry

    lax.fori_loop(0, units, gather, 0)
    for v in range(2 * units - zslots, 2 * units):
        for k in range(1, tensor):
            z_copy(k, v, dgot).wait_send()
    for v in range(2 * units - 2, 2 * units):
        own_copy(v, down_own).wait()


def reduce_grads(pairs, kv_grads, dq, vectors, tables, moments_of, gains, weights, x, sizes):
    act, att, n2, grads, n1, slope, forward = pairs
    bits, tensor, heads, head_dim = sizes
    fc1_weight, fc2_weight, w1, flat_out = weights
    deep = 256
    rows, wide = grads.shape
    hidden_width, width = act.shape[1], heads * head_dim
    natural = hidden_width == wide
    shapes = [
        (hidden_width, None, True, None),
        (width, None, False, "attended"),
        (wide, "hidden", True, None) if natural else (hidden_width, 0, False, "hidden"),
        (3 * width, None, False, "projected"),
    ]
    plan, first = [], 0
    for size, right, fetched, local in shapes:
        plan.append((first, size // deep, right, fetched, local))
        first += size // deep
    chunks, ring, slots, zslots = first, 4 * bits - 2, 4, 3
    blocks = 8 if chunks >= 20 else 4
    block = rows // blocks
    own_rows, units = rows // tensor, wide // deep
    halves_of = [deep >> (level + 1) for level in range(1, bits)]
    hbm = pl.BlockSpec(memory_space=pl.ANY)
    vmem = pl.BlockSpec(memory_space=pltpu.VMEM)
    lefts = [act, n2] if natural else [act]
    extra = [] if natural else [n2]
    dims = (chunks, bits, tensor, heads, head_dim, blocks, len(extra))
    return pl.pallas_call(
        lambda *refs: reduce_kernel(plan, dims, *refs),
        name="reduce_grads",
        in_specs=[hbm] * 13 + [vmem] * len(extra) + [hbm] * len(lefts) + [vmem] * 8,
        out_specs=[hbm] * 8 + [vmem],
        out_shape=[
            *[jax.ShapeDtypeStruct((item[0], wide), BF16) for item in shapes],
            *[
                jax.ShapeDtypeStruct((own_rows, wide), F32),
                jax.ShapeDtypeStruct((tensor - 1, own_rows, wide), BF16),
            ]
            * 2,
            jax.ShapeDtypeStruct(vectors.shape, F32),
        ],
        scratch_shapes=[
            pltpu.VMEM((2, rows, deep), BF16),
            pltpu.VMEM((3, deep, wide), F32),
            pltpu.VMEM((slots, deep // 2, wide), F32),
            pltpu.VMEM((ring, deep, wide), BF16),
            pltpu.VMEM((rows, wide), BF16),
            pltpu.VMEM((rows, hidden_width), BF16),
            pltpu.VMEM((rows, 3 * width), BF16),
            *[pltpu.VMEM((slots, half, wide), F32) for half in halves_of],
            *[pltpu.VMEM((slots, half, wide), BF16) for half in halves_of],
            *[pltpu.VMEM((slots, half, wide), BF16) for half in halves_of],
            pltpu.VMEM((2, deep, 3 * width), BF16),
            pltpu.VMEM((2, deep, wide), BF16),
            pltpu.VMEM((2, rows, deep), BF16),
            pltpu.VMEM((2, rows, deep), F32),
            pltpu.VMEM((2, width, deep), BF16),
            pltpu.VMEM((2, rows, deep), F32),
            pltpu.VMEM((zslots, rows, deep), BF16),
            pltpu.VMEM((2, own_rows, deep), F32),
            pltpu.VMEM(vectors.shape, F32),
            pltpu.VMEM((2, block, 2 * width), F32),
            pltpu.VMEM((2, block, 2 * width), F32),
            pltpu.VMEM((2, block, width), F32),
            pltpu.VMEM((4, block, 2 * width), BF16),
            pltpu.VMEM((rows, 2 * width), BF16),
            pltpu.VMEM((rows, 2 * width), BF16),
            pltpu.VMEM((tensor, *vectors.shape), F32),
            pltpu.VMEM((bits, *vectors.shape), F32),
            pltpu.VMEM((bits, *vectors.shape), F32),
            pltpu.SemaphoreType.DMA((2,)),
            pltpu.SemaphoreType.DMA((ring,)),
            pltpu.SemaphoreType.DMA((2 * bits, ring)),
            pltpu.SemaphoreType.DMA((2 * bits, ring)),
            pltpu.SemaphoreType.DMA((tensor - 1, 2 * units)),
            pltpu.SemaphoreType.DMA((tensor - 1, 2 * units)),
            pltpu.SemaphoreType.DMA((tensor + bits,)),
            pltpu.SemaphoreType.DMA((tensor + bits,)),
            pltpu.SemaphoreType.DMA((6, 2)),
            pltpu.SemaphoreType.DMA((2,)),
            pltpu.SemaphoreType.DMA((3, 2)),
            pltpu.SemaphoreType.DMA((4, blocks)),
            pltpu.SemaphoreType.DMA((2,)),
        ],
        compiler_params=pltpu.CompilerParams(
            collective_id=0, has_side_effects=True, vmem_limit_bytes=63 << 20
        ),
        cost_estimate=cost(
            2 * rows * wide * (chunks * deep + 2 * hidden_width + 3 * width), 8 * chunks * deep * wide
        ),
    )(
        grads, n1, slope, fc1_weight, fc2_weight, w1, x, flat_out, forward, *kv_grads, dq,
        *extra, *lefts, att, vectors, *gains, *moments_of, *tables,
    )


def body(
    tokens, out_grad, segment_ids, positions, norm1_gain, norm1_bias, norm2_gain, norm2_bias,
    qkv_weight, qkv_bias, out_weight, out_bias, fc1_weight, fc1_bias, fc2_weight, fc2_bias,
):
    model_width, heads, _, head_dim = qkv_weight.shape
    width = heads * head_dim
    hidden_width = fc1_weight.shape[1]
    row = lambda v: v.reshape(1, -1).astype(F32)
    w4 = jnp.transpose(qkv_weight, (0, 2, 1, 3))
    flat_bias = jnp.transpose(qkv_bias, (1, 0, 2)).reshape(1, 3 * width).astype(F32)
    flat_out = out_weight.reshape(width, model_width)
    tables = rope_tables(positions, 128)
    small = [
        row(norm1_gain), row(norm1_bias), row(norm2_gain), row(norm2_bias), flat_bias, row(fc1_bias)
    ]
    tensor, last = lax.axis_size("tensor"), lax.axis_size("dp") - 1
    (
        rows_all, grads_all, flat_qkv, normed_one, normed_two, queries, kv_own, kv_near, kv_far,
        activated, slope, forward, attended_grad, mean, inverse,
    ) = front(
        tokens, out_grad, w4, fc1_weight, fc2_weight, flat_out, small, tables,
        (tensor, last, heads, head_dim),
    )
    assert MOST - 2 < 2 * rows_all.shape[0]
    attended, query_grad, *kv_grads = attention(
        queries, [kv_far, kv_near, kv_own], attended_grad, positions, heads, head_dim
    )
    own_grad = out_grad.astype(F32)
    vectors = jnp.pad(jnp.sum(own_grad, 0, keepdims=True), ((4, 3), (0, 0)))
    bits = last.bit_length()
    *stacked, d_sum, d_got, branch, b_got, vectors = reduce_grads(
        (activated, attended, normed_two, grads_all, normed_one, slope, forward), kv_grads, query_grad,
        vectors, tables, (mean, inverse), (row(norm1_gain), row(norm2_gain)),
        (fc1_weight, fc2_weight, flat_qkv, flat_out), rows_all,
        (bits, tensor, heads, head_dim),
    )
    for k in range(d_got.shape[0]):
        d_sum = d_sum + d_got[k].astype(F32)
        branch = branch + b_got[k].astype(F32)
    fc2_grad, out_weight_grad, fc1_grad, qkv_weight_grad = stacked
    natural = hidden_width == model_width
    fc2_grad = widened(fc2_grad)
    out_weight_grad = out_weight_grad.astype(F32).reshape(heads, head_dim, model_width)
    fc1_grad = widened(fc1_grad) if natural else fc1_grad.T.astype(F32)
    qkv_weight_grad = jnp.transpose(spread(qkv_weight_grad, heads, head_dim), (0, 2, 1, 3))
    fc1_bias_grad = vectors[5, :hidden_width]
    qkv_bias_grad = vectors[6, : 3 * width].reshape(3, heads, head_dim)
    qkv_bias_grad = jnp.transpose(qkv_bias_grad, (1, 0, 2))
    own_rows = tokens.astype(F32)
    block_out = own_rows + branch + out_bias.astype(F32) + fc2_bias.astype(F32)
    own_mean, own_inverse = moments(own_rows)
    standard = (own_rows - own_mean) * own_inverse
    tokens_grad = own_grad + own_inverse * (
        d_sum
        - jnp.mean(d_sum, -1, keepdims=True)
        - standard * jnp.mean(d_sum * standard, -1, keepdims=True)
    )
    return (
        block_out.astype(BF16), tokens_grad.astype(BF16),
        vectors[0], vectors[1], vectors[2], vectors[3],
        qkv_weight_grad, qkv_bias_grad, out_weight_grad, vectors[4],
        fc1_grad, fc1_bias_grad, fc2_grad, vectors[4],
    )


def solution(mesh):
    rows = P(("dp", "tensor"), None)
    return jax.shard_map(
        body,
        mesh=mesh,
        in_specs=(
            rows, rows, P("dp"), P("dp"), P(), P(), P(), P(),
            P(None, "tensor", None, None), P("tensor", None, None), P("tensor", None, None), P(),
            P(None, "tensor"), P("tensor"), P("tensor", None), P(),
        ),
        out_specs=(
            rows, rows, P(), P(), P(), P(),
            P(None, "tensor", None, None), P("tensor", None, None), P("tensor", None, None), P(),
            P(None, "tensor"), P("tensor"), P("tensor", None), P(),
        ),
        check_vma=False,
    )
```

```python
import functools
import math

import jax
import jax.numpy as jnp
from jax import lax
from jax.experimental import pallas as pl
from jax.experimental.pallas import tpu as pltpu
from jax.sharding import PartitionSpec as P

ROT = 64
MOST = 2000
EPSILON = 1e-05
BF16 = jnp.bfloat16
F32 = jnp.float32
MESH = pl.DeviceIdType.MESH


def dot_rows(first, second):
    return lax.dot_general(first, second, (((0,), (0,)), ((), ())), preferred_element_type=F32)


def dot_cols(first, second):
    return lax.dot_general(first, second, (((1,), (1,)), ((), ())), preferred_element_type=F32)


def dot(first, second):
    return jnp.dot(first, second, preferred_element_type=F32)


def cost(flops, bytes_accessed):
    return pl.CostEstimate(flops=int(flops), bytes_accessed=int(bytes_accessed), transcendentals=0)


def params(*semantics):
    return pltpu.CompilerParams(dimension_semantics=semantics, vmem_limit_bytes=60 << 20)


def moments(values):
    average = jnp.mean(values, -1, keepdims=True)
    centered = values - average
    variance = jnp.mean(centered * centered, -1, keepdims=True)
    return average, lax.rsqrt(variance + EPSILON)


def rope_tables(position, lanes):
    half = ROT // 2
    frequency = jnp.power(F32(10000.0), -jnp.arange(half, dtype=F32) / F32(half))
    angles = position.astype(F32)[:, None] * frequency[None, :]
    cosine, sine = jnp.cos(angles), jnp.sin(angles)
    rows = position.shape[0]
    ones = jnp.ones((rows, lanes - ROT), F32)
    return (
        jnp.concatenate([cosine, cosine, ones], 1),
        jnp.concatenate([-sine, sine, 0 * ones], 1),
    )


def turn(values, cos_block, sin_block):
    lane = lax.broadcasted_iota(jnp.int32, values.shape, 1)
    half = ROT // 2
    up = pltpu.roll(values, values.shape[1] - half, 1)
    down = pltpu.roll(values, half, 1)
    return values * cos_block + jnp.where(lane < half, up, down) * sin_block


PIECES = 4


def front_kernel(dims, *refs):
    tensor, last, heads, head_dim = dims
    refs = list(refs)
    take = lambda count: [refs.pop(0) for _ in range(count)]
    tokens_ref, grads_ref, w4_ref, up_ref, down_ref, out_ref = take(6)
    g1_ref, b1_ref, g2_ref, b2_ref, qb_ref, ub_ref, cos_ref, sin_ref = take(8)
    rows_out, grads_out, flat_out, n1_out, n2_out, q_out, kv_own, kv_near, kv_far = take(9)
    act_out, slope_out, forward_out, agrad_out, mean_ref, inverse_ref = take(6)
    both, wq, w_up, w_down, w_out, wstage = take(6)
    n1s, n2s, qs, kvs, acts, slopes, forwards, agrads = take(8)
    own_sem, w_sem, q_sem, send_sem, recv_sem, kv_sems, s_sem = take(7)
    index, me = lax.axis_index("dp"), lax.axis_index("tensor")
    own = tokens_ref.shape[0]
    piece = own // PIECES
    width, depth = heads * head_dim, tokens_ref.shape[1]
    hidden_width = act_out.shape[1]
    span = tensor * PIECES

    barrier = pltpu.get_barrier_semaphore()

    def greet(axis, to):
        pl.semaphore_signal(barrier, inc=1, device_id={axis: to}, device_id_type=MESH)

    sides = [
        (me < tensor - 1, "tensor", me + 1),
        (me > 0, "tensor", me - 1),
        (index < last, "dp", index + 1),
        (index > 0, "dp", index - 1),
    ]
    for there, axis, to in sides:
        @pl.when(there)
        def _():
            greet(axis, to)

    pl.semaphore_wait(barrier, sum(jnp.where(there, 1, 0) for there, _, _ in sides))

    def rows_of(shard):
        return pl.ds(pl.multiple_of(shard * own, own), own)

    own_copies = [
        pltpu.make_async_copy(source, both.at[a, rows_of(me)], own_sem.at[a])
        for a, source in enumerate((tokens_ref, grads_ref))
    ]
    weight_copies = [
        pltpu.make_async_copy(up_ref, w_up, w_sem.at[0]),
        pltpu.make_async_copy(down_ref, w_down, w_sem.at[1]),
        pltpu.make_async_copy(out_ref, w_out, w_sem.at[2]),
    ]
    wrows = wstage.shape[1]

    def wq_copy(b):
        return pltpu.make_async_copy(
            w4_ref.at[pl.ds(pl.multiple_of(b * wrows, wrows), wrows)],
            wstage.at[lax.rem(b, 2)], q_sem.at[lax.rem(b, 2)],
        )

    flat_copy = pltpu.make_async_copy(wq, flat_out, w_sem.at[3])
    for copy in own_copies:
        copy.start()
    wq_copy(0).start()
    wq_copy(1).start()
    for copy in weight_copies:
        copy.start()
    for copy in own_copies:
        copy.wait()

    def hop(t, shard, p, direction):
        rows = pl.ds(pl.multiple_of(shard * own + p * piece, piece), piece)
        here = both.at[t // span, rows]
        to = me + 1 if direction == 0 else me - 1
        return pltpu.make_async_remote_copy(
            src_ref=here,
            dst_ref=here,
            send_sem=send_sem.at[direction, t],
            recv_sem=recv_sem.at[direction, t],
            device_id={"tensor": jnp.clip(to, 0, tensor - 1)},
            device_id_type=MESH,
        )

    def passing(t):
        k, p = lax.rem(t // PIECES, tensor), lax.rem(t, PIECES)
        return k, p, ((me - k, me - k >= 0, me < tensor - 1), (me + k, me + k < tensor, me > 0))

    def relay(t):
        k, p, ways = passing(t)
        for direction, (shard, held, onward) in enumerate(ways):
            @pl.when(held & (k > 0))
            def _():
                hop(t - PIECES, shard, p, direction).wait_recv()

            @pl.when(held & onward)
            def _():
                hop(t, shard, p, direction).start()

    def drain(t, carry):
        k, p, ways = passing(t)
        for direction, (shard, held, onward) in enumerate(ways):
            @pl.when(held & onward)
            def _():
                hop(t, shard, p, direction).wait_send()

        return carry

    tables = []
    for m in range(tensor):
        near = sorted(range(tensor), key=lambda shard: (abs(shard - m), shard))
        tables.append(near)

    def shard_at(j):
        found = 0
        for m in range(tensor):
            for place in range(tensor):
                hit = (me == m) & (j == place)
                found = found + jnp.where(hit, tables[m][place], 0)
        return found

    def outs_project(shard):
        rows = rows_of(shard)
        return [
            pltpu.make_async_copy(both.at[0, rows], rows_out.at[rows], s_sem.at[0]),
            pltpu.make_async_copy(n1s, n1_out.at[rows], s_sem.at[1]),
            pltpu.make_async_copy(n2s, n2_out.at[rows], s_sem.at[2]),
            pltpu.make_async_copy(qs, q_out.at[rows], s_sem.at[3]),
            pltpu.make_async_copy(kvs, kv_own.at[rows], s_sem.at[4]),
        ]

    def outs_up(shard):
        rows = rows_of(shard)
        return [
            pltpu.make_async_copy(acts, act_out.at[rows], s_sem.at[5]),
            pltpu.make_async_copy(slopes, slope_out.at[rows], s_sem.at[6]),
        ]

    def out_forward(shard):
        return pltpu.make_async_copy(forwards, forward_out.at[rows_of(shard)], s_sem.at[7])

    def outs_agrad(shard):
        rows = rows_of(shard)
        return [
            pltpu.make_async_copy(both.at[1, rows], grads_out.at[rows], s_sem.at[8]),
            pltpu.make_async_copy(agrads, agrad_out.at[rows], s_sem.at[9]),
        ]

    def near_copy(j):
        rows = rows_of(shard_at(j))
        return pltpu.make_async_remote_copy(
            src_ref=kvs,
            dst_ref=kv_near.at[rows],
            send_sem=kv_sems.at[0, j],
            recv_sem=kv_sems.at[1, j],
            device_id={"dp": jnp.minimum(index + 1, last)},
            device_id_type=MESH,
        )

    def far_copy(j):
        rows = rows_of(shard_at(j))
        return pltpu.make_async_remote_copy(
            src_ref=kv_near.at[rows],
            dst_ref=kv_far.at[rows],
            send_sem=kv_sems.at[2, j],
            recv_sem=kv_sems.at[3, j],
            device_id={"dp": jnp.minimum(index + 1, last)},
            device_id_type=MESH,
        )

    def project_shard(j):
        shard = shard_at(j)
        rows = rows_of(shard)

        @pl.when(j > 0)
        def _():
            for copy in outs_project(shard_at(j - 1)):
                copy.wait()

            @pl.when(index < last)
            def _():
                near_copy(j - 1).wait_send()

        x = both[0, rows].astype(F32)
        average, inverse = moments(x)
        mean_ref[rows, :] = average
        inverse_ref[rows, :] = inverse
        standard = (x - average) * inverse
        n1s[...] = (standard * g1_ref[...] + b1_ref[...]).astype(BF16)
        n2s[...] = (standard * g2_ref[...] + b2_ref[...]).astype(BF16)
        cos_block, sin_block = cos_ref[rows, :], sin_ref[rows, :]
        lanes = cos_block.shape[1]
        scale = 1.0 / math.sqrt(head_dim)
        for part in range(3):
            low = part * width
            projected = dot(n1s[...], wq[:, low : low + width]) + qb_ref[:, low : low + width]
            if part == 2:
                kvs[:, width:] = projected.astype(BF16)
                continue
            for head in range(heads):
                at = head * head_dim
                turned = turn(projected[:, at : at + lanes], cos_block, sin_block)
                other = projected[:, at + lanes : at + head_dim]
                if part == 0:
                    qs[:, at : at + lanes] = (turned * scale).astype(BF16)
                    qs[:, at + lanes : at + head_dim] = (other * scale).astype(BF16)
                else:
                    kvs[:, at : at + lanes] = turned.astype(BF16)
                    kvs[:, at + lanes : at + head_dim] = other.astype(BF16)
        for copy in outs_project(shard):
            copy.start()

        @pl.when(index < last)
        def _():
            near_copy(j).start()

    def up_half(j, half):
        if half == 0:
            @pl.when(j > 0)
            def _():
                for copy in outs_up(shard_at(j - 1)):
                    copy.wait()

        size = hidden_width // 2
        step = min(512, size)
        for column in range(half * size, (half + 1) * size, step):
            part = slice(column, column + step)
            hidden = dot(n2s[...], w_up[:, part]) + ub_ref[:, part]
            phi = (1.0 + lax.erf(hidden * F32(math.sqrt(0.5)))) * 0.5
            acts[:, part] = (hidden * phi).astype(BF16)
            density = jnp.exp(hidden * hidden * -0.5) * F32(1.0 / math.sqrt(2.0 * math.pi))
            slopes[:, part] = phi + hidden * density
        if half == 1:
            for copy in outs_up(shard_at(j)):
                copy.start()

    def forward_shard(j):
        @pl.when(j > 0)
        def _():
            out_forward(shard_at(j - 1)).wait()

        step = min(512, depth)
        for column in range(0, depth, step):
            part = slice(column, column + step)
            forwards[:, part] = dot(acts[...], w_down[:, part])
        out_forward(shard_at(j)).start()

    def pass_kv(j):
        @pl.when(index > 0)
        def _():
            near_copy(j).wait_recv()

            @pl.when(index < last)
            def _():
                far_copy(j).start()

    def agrad_shard(j):
        @pl.when(j > 0)
        def _():
            for copy in outs_agrad(shard_at(j - 1)):
                copy.wait()

        shard = shard_at(j)
        agrads[...] = dot_cols(both[1, rows_of(shard)], w_out[...]).astype(BF16)
        for copy in outs_agrad(shard):
            copy.start()

    def on(condition, act):
        @pl.when(condition)
        def _():
            act()

    def slot(t, carry):
        on(t < 2 * span, lambda: relay(t))

        @pl.when(t == 2)
        def _():
            for b in range(depth // wrows):
                wq_copy(b).wait()
                for part in range(3):
                    wq[b * wrows : (b + 1) * wrows, part * width : (part + 1) * width] = wstage[
                        b % 2, :, part
                    ].reshape(wrows, width)
                if b + 2 < depth // wrows:
                    wq_copy(b + 2).start()
            flat_copy.start()

        j, sub = t // PIECES - 1, lax.rem(t, PIECES)
        working = (j >= 0) & (j < tensor)
        on(working & (sub == 0), lambda: project_shard(j))

        @pl.when(t == PIECES + 1)
        def _():
            weight_copies[0].wait()

        on(working & (sub == 1), lambda: up_half(j, 0))
        on(working & (sub == 2), lambda: up_half(j, 1))

        @pl.when(t == PIECES + 3)
        def _():
            weight_copies[1].wait()

        on(working & (sub == 3), lambda: forward_shard(j))
        before = j - 1
        on((before >= 0) & (before < tensor) & (sub == 1), lambda: pass_kv(before))

        @pl.when(t == span + PIECES)
        def _():
            weight_copies[2].wait()

        late = j - tensor
        on((late >= 0) & (late < tensor) & (sub == 0), lambda: agrad_shard(late))
        return carry

    lax.fori_loop(0, 2 * span + 1, slot, 0)
    final = shard_at(tensor - 1)
    for copy in outs_project(final) + outs_up(final) + [out_forward(final)] + outs_agrad(final):
        copy.wait()
    flat_copy.wait()

    @pl.when(index < last)
    def _():
        near_copy(tensor - 1).wait_send()

    def kv_drain(j, carry):
        @pl.when((index > 0) & (index < last))
        def _():
            far_copy(j).wait_send()

        @pl.when(index > 1)
        def _():
            far_copy(j).wait_recv()

        return carry

    lax.fori_loop(0, tensor, kv_drain, 0)
    lax.fori_loop(0, 2 * span, drain, 0)


def front(tokens, grads, w4, fc1_weight, fc2_weight, flat_out, small, tables, sizes):
    tensor, last, heads, head_dim = sizes
    own, depth = tokens.shape
    rows, width, hidden_width = own * tensor, heads * head_dim, fc1_weight.shape[1]
    span, wrows = tensor * PIECES, 256
    hbm = pl.BlockSpec(memory_space=pl.ANY)
    vmem = pl.BlockSpec(memory_space=pltpu.VMEM)
    shape = jax.ShapeDtypeStruct
    return pl.pallas_call(
        lambda *refs: front_kernel(sizes, *refs),
        name="front",
        in_specs=[hbm] * 6 + [vmem] * 8,
        out_specs=[hbm] * 13 + [vmem] * 2,
        out_shape=[
            shape((rows, depth), BF16),
            shape((rows, depth), BF16),
            shape((depth, 3 * width), BF16),
            shape((rows, depth), BF16),
            shape((rows, depth), BF16),
            shape((rows, width), BF16),
            *[shape((rows, 2 * width), BF16)] * 3,
            shape((rows, hidden_width), BF16),
            shape((rows, hidden_width), F32),
            shape((rows, depth), F32),
            shape((rows, width), BF16),
            shape((rows, 1), F32),
            shape((rows, 1), F32),
        ],
        scratch_shapes=[
            pltpu.VMEM((2, rows, depth), BF16),
            pltpu.VMEM((depth, 3 * width), BF16),
            pltpu.VMEM((depth, hidden_width), BF16),
            pltpu.VMEM((hidden_width, depth), BF16),
            pltpu.VMEM((width, depth), BF16),
            pltpu.VMEM((2, wrows, 3, heads, head_dim), BF16),
            pltpu.VMEM((own, depth), BF16),
            pltpu.VMEM((own, depth), BF16),
            pltpu.VMEM((own, width), BF16),
            pltpu.VMEM((own, 2 * width), BF16),
            pltpu.VMEM((own, hidden_width), BF16),
            pltpu.VMEM((own, hidden_width), F32),
            pltpu.VMEM((own, depth), F32),
            pltpu.VMEM((own, width), BF16),
            pltpu.SemaphoreType.DMA((2,)),
            pltpu.SemaphoreType.DMA((4,)),
            pltpu.SemaphoreType.DMA((2,)),
            pltpu.SemaphoreType.DMA((2, 2 * span)),
            pltpu.SemaphoreType.DMA((2, 2 * span)),
            pltpu.SemaphoreType.DMA((4, tensor)),
            pltpu.SemaphoreType.DMA((10,)),
        ],
        compiler_params=pltpu.CompilerParams(
            collective_id=1, has_side_effects=True, vmem_limit_bytes=62 << 20
        ),
        cost_estimate=cost(
            2 * rows * depth * (3 * width + 2 * hidden_width + width),
            2 * rows * (6 * depth + 4 * hidden_width),
        ),
    )(tokens, grads, w4, fc1_weight, fc2_weight, flat_out, *small, *tables)


def attention_kernel(heads, head_dim, parts, bk, first_ref, q_ref, do_ref, start_ref, *refs):
    kv_parts, refs = refs[:parts], refs[parts:]
    att_ref, dq_ref, refs = refs[0], refs[1], refs[2:]
    grad_parts, (kv_ref, dkv_ref, s_ref, dp_ref, o_ref, sems) = refs[:parts], refs[parts:]
    block = pl.program_id(0)
    bq = q_ref.shape[0]
    width = heads * head_dim
    rows_each = kv_ref.shape[0] // parts
    ahead = rows_each * (parts - 1)
    low = first_ref[block]
    high = (ahead + (block + 1) * bq + bk - 1) // bk
    row = ahead + block * bq + lax.broadcasted_iota(jnp.int32, (bq, 1), 0)
    start = start_ref[...]
    lane = lax.broadcasted_iota(jnp.int32, (bq, bk), 1)
    chunks = bk // 128

    @pl.when(block == 0)
    def _():
        copies = [
            pltpu.make_async_copy(
                part, kv_ref.at[pl.ds(k * rows_each, rows_each)], sems.at[k]
            )
            for k, part in enumerate(kv_parts)
        ]
        for copy in copies:
            copy.start()

        def clear(j, carry):
            dkv_ref[pl.ds(pl.multiple_of(j * 128, 128), 128), :] = jnp.zeros((128, 2 * width), F32)
            return carry

        lax.fori_loop(0, dkv_ref.shape[0] // 128, clear, 0)
        for copy in copies:
            copy.wait()

    def rows_of(j):
        return pl.ds(pl.multiple_of(j * bk, bk), bk)

    at = [head * head_dim for head in range(heads)]
    head_of = lambda ref, head: ref[:, at[head] : at[head] + head_dim]
    folded = lambda x, fold: functools.reduce(
        fold, [x[:, c * 128 : (c + 1) * 128] for c in range(chunks)]
    )

    def scores(j, best):
        rows = rows_of(j)
        column = j * bk + lane
        allowed = (column >= start) & (column <= row)
        out = []
        for head in range(heads):
            key = kv_ref[rows, at[head] : at[head] + head_dim]
            s = jnp.where(allowed, dot_cols(head_of(q_ref, head), key), -1e30)
            s_ref[head, j] = s
            out.append(jnp.maximum(best[head], folded(s, jnp.maximum)))
        for head in range(heads):
            value = kv_ref[rows, width + at[head] : width + at[head] + head_dim]
            dp_ref[head, j] = dot_cols(head_of(do_ref, head), value)
        return tuple(out)

    low_best = jnp.full((bq, 128), -1e30, F32)
    best = lax.fori_loop(low, high, scores, (low_best,) * heads)
    best = [jnp.max(b, 1, keepdims=True) for b in best]

    def weigh(j, carry):
        out = []
        for head in range(heads):
            total, mixed = carry[head]
            e = jnp.exp(s_ref[head, j] - best[head])
            s_ref[head, j] = e
            out.append(
                (total + folded(e, jnp.add), mixed + folded(e * dp_ref[head, j], jnp.add))
            )
        return tuple(out)

    zero = jnp.zeros((bq, 128), F32)
    sums = lax.fori_loop(low, high, weigh, ((zero, zero),) * heads)
    scale = [1.0 / jnp.sum(total, 1, keepdims=True) for total, _ in sums]
    delta = [jnp.sum(mixed, 1, keepdims=True) * k for (_, mixed), k in zip(sums, scale)]
    o_ref[...] = jnp.zeros_like(o_ref)

    def spread_back(j, carry):
        rows = rows_of(j)
        for head in range(heads):
            p = s_ref[head, j] * scale[head]
            p_low = p.astype(BF16)
            ds = (p * (dp_ref[head, j] - delta[head])).astype(BF16)
            keys = slice(at[head], at[head] + head_dim)
            values = slice(width + at[head], width + at[head] + head_dim)
            o_ref[head, :, :head_dim] += dot(p_low, kv_ref[rows, values])
            o_ref[head, :, head_dim:] += dot(ds, kv_ref[rows, keys])
            dkv_ref[rows, keys] += dot_rows(ds, head_of(q_ref, head))
            dkv_ref[rows, values] += dot_rows(p_low, head_of(do_ref, head))
        return carry

    lax.fori_loop(low, high, spread_back, 0)
    for head in range(heads):
        keys = slice(at[head], at[head] + head_dim)
        att_ref[:, keys] = o_ref[head, :, :head_dim].astype(BF16)
        dq_ref[:, keys] = o_ref[head, :, head_dim:] * (1.0 / math.sqrt(head_dim))

    @pl.when(block == pl.num_programs(0) - 1)
    def _():
        for k, part in enumerate(grad_parts):
            part[...] = dkv_ref[k * rows_each : (k + 1) * rows_each, :].astype(part.dtype)


def attention(q, kv_parts, do, positions, heads, head_dim):
    rows, width = q.shape
    parts = len(kv_parts)
    total = rows * parts
    bq = min(256, rows)
    bk = 256
    start = jnp.arange(rows, dtype=jnp.int32) - positions + (total - rows)
    first = start[::bq] // bk
    by_row = lambda i, f: (i, 0)
    whole = lambda i, f: (0, 0)
    part_types = [BF16] + [F32] * (parts - 1)
    return pl.pallas_call(
        lambda *refs: attention_kernel(heads, head_dim, parts, bk, *refs),
        name="attention",
        grid_spec=pltpu.PrefetchScalarGridSpec(
            num_scalar_prefetch=1,
            grid=(rows // bq,),
            in_specs=[
                pl.BlockSpec((bq, width), by_row),
                pl.BlockSpec((bq, width), by_row),
                pl.BlockSpec((bq, 1), by_row),
                *[pl.BlockSpec(memory_space=pl.ANY)] * parts,
            ],
            out_specs=[
                pl.BlockSpec((bq, width), by_row),
                pl.BlockSpec((bq, width), by_row),
                *[pl.BlockSpec((rows, 2 * width), whole, pipeline_mode=pl.Buffered(1))] * parts,
            ],
            scratch_shapes=[
                pltpu.VMEM((total, 2 * width), BF16),
                pltpu.VMEM((total, 2 * width), F32),
                pltpu.VMEM((heads, total // bk, bq, bk), F32),
                pltpu.VMEM((heads, total // bk, bq, bk), F32),
                pltpu.VMEM((heads, bq, 2 * head_dim), F32),
                pltpu.SemaphoreType.DMA((parts,)),
            ],
        ),
        out_shape=[
            jax.ShapeDtypeStruct((rows, width), BF16),
            jax.ShapeDtypeStruct((rows, width), F32),
            *[jax.ShapeDtypeStruct((rows, 2 * width), kind) for kind in part_types],
        ],
        compiler_params=params("arbitrary"),
        cost_estimate=cost(12 * rows * MOST * width, 8 * total * width),
    )(first, q, do, start[:, None], *kv_parts)


def finish_kernel(heads, head_dim, natural, *refs):
    fc2_ref, out_ref, fc1_ref, qkv_ref, fc2_to, out_to, fc1_to, qkv_to = refs
    fc2_to[...] = fc2_ref[...].astype(F32)
    out_to[...] = out_ref[...].astype(F32)
    fc1_to[...] = (fc1_ref[...] if natural else fc1_ref[...].T).astype(F32)
    for part in range(3):
        for head in range(heads):
            at = (part * heads + head) * head_dim
            qkv_to[:, part, head, :] = qkv_ref[at : at + head_dim, :].T.astype(F32)


def finish(fc2, out, fc1, qkv, heads, head_dim, natural):
    depth = fc2.shape[1]
    steps = 8
    by_row = lambda i: (i, 0)
    by_column = lambda i: (0, i)
    rows_of = lambda x: pl.BlockSpec((x.shape[0] // steps, x.shape[1]), by_row)
    columns_of = lambda x: pl.BlockSpec((x.shape[0], depth // steps), by_column)
    shape = lambda *dims: jax.ShapeDtypeStruct(dims, F32)
    fc1_shape = fc1.shape if natural else fc1.shape[::-1]
    return pl.pallas_call(
        lambda *refs: finish_kernel(heads, head_dim, natural, *refs),
        name="finish",
        grid=(steps,),
        in_specs=[
            rows_of(fc2), rows_of(out), rows_of(fc1) if natural else columns_of(fc1), columns_of(qkv)
        ],
        out_specs=[
            rows_of(fc2),
            rows_of(out),
            pl.BlockSpec((fc1_shape[0] // steps, fc1_shape[1]), by_row),
            pl.BlockSpec((depth // steps, 3, heads, head_dim), lambda i: (i, 0, 0, 0)),
        ],
        out_shape=[
            shape(*fc2.shape), shape(*out.shape), shape(*fc1_shape), shape(depth, 3, heads, head_dim)
        ],
        compiler_params=params("arbitrary"),
        cost_estimate=cost(0, 6 * (fc2.size + out.size + fc1.size + qkv.size)),
    )(fc2, out, fc1, qkv)


def reduce_kernel(plan, dims, *refs):
    chunks, bits, tensor, heads, head_dim, blocks, wide_b = dims
    refs = list(refs)
    take = lambda count: [refs.pop(0) for _ in range(count)]
    g_ref, n1_ref, slope_ref, up_ref, down_ref, w1_ref, x_ref, wout_ref, forward_ref = take(9)
    far_ref, near_ref, own_ref, dq_ref = take(4)
    extra_refs = take(wide_b)
    lefts = take(sum(1 for item in plan if item[3]))
    att_ref, vec_ref, gain1_ref, gain2_ref, mean_ref, inverse_ref, cos_ref, sin_ref = take(8)
    out_refs = take(len(plan))
    down_own, dgot, branch_own, bgot, total_ref = take(5)
    abuf, full, r0, ag, gbuf, hg, dqkv = take(7)
    kept, sent, got = take(bits - 1), take(bits - 1), take(bits - 1)
    w1buf, w2buf, xbuf, sbuf, wobuf, fbuf, zsend, zown, mine_ref = take(9)
    near_buf, own_buf, dq_buf, hop_send, far_got, near_got = take(6)
    vgot, vsend, vnow = take(3)
    a_sem, o_sem, send_sem, recv_sem, d_send, d_recv, v_send, v_recv = take(8)
    w_sem, b_sem, h_sem, hop_sems, z_sem = take(5)
    index, me = lax.axis_index("dp"), lax.axis_index("tensor")
    last = (1 << bits) - 1
    deep, wide = full.shape[1], full.shape[2]
    rows_all = gbuf.shape[0]
    slots, ring, lag = r0.shape[0], ag.shape[0], 2

    def bit_of(bit):
        return (index // (1 << bit)) % 2

    def partner(bit):
        return index + (1 << bit) * (1 - 2 * bit_of(bit))

    barrier = pltpu.get_barrier_semaphore()

    def greet(axis, to):
        pl.semaphore_signal(barrier, inc=1, device_id={axis: to}, device_id_type=MESH)

    for bit in range(bits):
        greet("dp", partner(bit))
    for k in range(1, tensor):
        greet("tensor", lax.rem(me + k, tensor))

    @pl.when(index > 0)
    def _():
        greet("dp", index - 1)

    @pl.when(index < last)
    def _():
        greet("dp", index + 1)

    inner = jnp.where(index > 0, 1, 0) + jnp.where(index < last, 1, 0)
    pl.semaphore_wait(barrier, bits + tensor - 1 + inner)

    hidden_units = hg.shape[1] // deep

    def columns_of(u):
        return pl.ds(pl.multiple_of(u * deep, deep), deep)

    def hidden_copies(u):
        slot = lax.rem(u, 2)
        return [
            pltpu.make_async_copy(down_ref.at[columns_of(u)], w2buf.at[slot], w_sem.at[1, slot]),
            pltpu.make_async_copy(slope_ref.at[:, columns_of(u)], sbuf.at[slot], w_sem.at[3, slot]),
        ]

    row_step = min(256, rows_all)

    def hidden_unit(u):
        slot, columns = lax.rem(u, 2), columns_of(u)

        @pl.when(u + 1 < hidden_units)
        def _():
            for copy in hidden_copies(u + 1):
                copy.start()

        for copy in hidden_copies(u):
            copy.wait()

        def row_block(i, total):
            rows = pl.ds(pl.multiple_of(i * row_step, row_step), row_step)
            grad = dot_cols(gbuf[rows, :], w2buf[slot])
            low = (grad * sbuf[slot, rows, :]).astype(BF16)
            hg[rows, columns] = low
            return total + jnp.sum(low.astype(F32), 0, keepdims=True)

        total = lax.fori_loop(0, rows_all // row_step, row_block, jnp.zeros((1, deep), F32))
        mine_ref[5:6, columns] = total

    block = rows_all // blocks
    width = heads * head_dim

    def block_of(p):
        return pl.ds(pl.multiple_of(p * block, block), block)

    def far_copy(p):
        return pltpu.make_async_remote_copy(
            src_ref=far_ref.at[block_of(p)],
            dst_ref=far_got.at[block_of(p)],
            send_sem=hop_sems.at[0, p],
            recv_sem=hop_sems.at[1, p],
            device_id={"dp": jnp.maximum(index - 1, 0)},
            device_id_type=MESH,
        )

    def near_copy(p):
        return pltpu.make_async_remote_copy(
            src_ref=hop_send.at[lax.rem(p, 4)],
            dst_ref=near_got.at[block_of(p)],
            send_sem=hop_sems.at[2, p],
            recv_sem=hop_sems.at[3, p],
            device_id={"dp": jnp.maximum(index - 1, 0)},
            device_id_type=MESH,
        )

    def near_load(p):
        slot = lax.rem(p, 2)
        return pltpu.make_async_copy(near_ref.at[block_of(p)], near_buf.at[slot], h_sem.at[0, slot])

    def own_loads(p):
        slot = lax.rem(p, 2)
        return [
            pltpu.make_async_copy(own_ref.at[block_of(p)], own_buf.at[slot], h_sem.at[1, slot]),
            pltpu.make_async_copy(dq_ref.at[block_of(p)], dq_buf.at[slot], h_sem.at[2, slot]),
        ]

    def far_start(p):
        @pl.when(index > 0)
        def _():
            far_copy(p).start()

    def relay(p):
        slot = lax.rem(p, 2)

        @pl.when(index > 0)
        def _():
            far_copy(p).wait_send()

        near_load(p).wait()

        @pl.when(index < last)
        def _():
            far_copy(p).wait_recv()
            near_buf[slot] += far_got[block_of(p)].astype(F32)

        @pl.when(index > 0)
        def _():
            hop_send[lax.rem(p, 4)] = near_buf[slot].astype(BF16)
            near_copy(p).start()

    def turn_block(p):
        slot, rows = lax.rem(p, 2), block_of(p)

        @pl.when(index > 0)
        def _():
            near_copy(p).wait_send()

        for copy in own_loads(p):
            copy.wait()

        @pl.when(index < last)
        def _():
            near_copy(p).wait_recv()
            own_buf[slot] += near_got[rows].astype(F32)

        cos_block, sin_block = cos_ref[rows, :], -sin_ref[rows, :]
        lanes = cos_block.shape[1]
        for part in range(3):
            for head in range(heads):
                at = head * head_dim
                to = part * width + at
                if part == 0:
                    grad = dq_buf[slot, :, at : at + head_dim]
                else:
                    low = (part - 1) * width + at
                    grad = own_buf[slot, :, low : low + head_dim]
                if part < 2:
                    first = turn(grad[:, :lanes], cos_block, sin_block)
                    grad = jnp.concatenate([first, grad[:, lanes:]], 1)
                low_grad = grad.astype(BF16)
                dqkv[rows, to : to + head_dim] = low_grad
                mine_ref[6:7, to : to + head_dim] += jnp.sum(
                    low_grad.astype(F32), 0, keepdims=True
                )

    own_rows = down_own.shape[0]
    units = wide // deep
    zslots = zsend.shape[0]
    begin = max(chunks // 2 + 3, blocks + 4)

    def z_copy(k, v, target):
        other = lax.rem(me + k, tensor)
        rows = pl.ds(pl.multiple_of(other * own_rows, own_rows), own_rows)
        return pltpu.make_async_remote_copy(
            src_ref=zsend.at[lax.rem(v, zslots), rows],
            dst_ref=target.at[k - 1, :, columns_of(lax.rem(v, units))],
            send_sem=d_send.at[k - 1, v],
            recv_sem=d_recv.at[k - 1, v],
            device_id={"tensor": other},
            device_id_type=MESH,
        )

    def own_copy(v, target):
        slot = lax.rem(v, 2)
        return pltpu.make_async_copy(
            zown.at[slot], target.at[:, columns_of(lax.rem(v, units))], z_sem.at[slot]
        )

    def z_clear(v):
        @pl.when(v >= zslots)
        def _():
            for k in range(1, tensor):
                z_copy(k, v - zslots, dgot).wait_send()

        @pl.when(v >= 2)
        def _():
            own_copy(v - 2, down_own).wait()

    def z_put(v, i, rows, value):
        zsend[lax.rem(v, zslots), rows] = value.astype(BF16)

        @pl.when(i == me)
        def _():
            zown[lax.rem(v, 2)] = value

    def z_start(v, target, own_target):
        for k in range(1, tensor):
            z_copy(k, v, target).start()
        own_copy(v, own_target).start()

    def branch_copies(u):
        slot = lax.rem(u, 2)
        return [
            pltpu.make_async_copy(wout_ref.at[:, columns_of(u)], wobuf.at[slot], w_sem.at[4, slot]),
            pltpu.make_async_copy(forward_ref.at[:, columns_of(u)], fbuf.at[slot], w_sem.at[5, slot]),
        ]

    def branch_unit(u):
        slot = lax.rem(u, 2)

        @pl.when(u + 1 < units)
        def _():
            for copy in branch_copies(u + 1):
                copy.start()

        for copy in branch_copies(u):
            copy.wait()

        z_clear(u)

        def row_block(i, carry):
            rows = pl.ds(pl.multiple_of(i * own_rows, own_rows), own_rows)
            z_put(u, i, rows, dot(att_ref[rows, :], wobuf[slot]) + fbuf[slot, rows, :])
            return carry

        lax.fori_loop(0, tensor, row_block, 0)
        z_start(u, bgot, branch_own)

    def unit_copies(u):
        slot = lax.rem(u, 2)
        return [
            pltpu.make_async_copy(w1_ref.at[columns_of(u)], w1buf.at[slot], w_sem.at[0, slot]),
            pltpu.make_async_copy(
                up_ref.at[columns_of(u)], w2buf.at[slot, :, pl.ds(0, hg.shape[1])], w_sem.at[1, slot]
            ),
            pltpu.make_async_copy(x_ref.at[:, columns_of(u)], xbuf.at[slot], w_sem.at[2, slot]),
        ]

    def unit(u):
        slot, v = lax.rem(u, 2), units + u
        columns = columns_of(u)

        @pl.when(u + 1 < units)
        def _():
            for copy in unit_copies(u + 1):
                copy.start()

        for copy in unit_copies(u):
            copy.wait()

        z_clear(v)
        gain1, gain2 = gain1_ref[:, columns], gain2_ref[:, columns]
        mine_ref[0:4, columns] = jnp.zeros((4, deep), F32)

        def row_block(i, carry):
            rows = pl.ds(pl.multiple_of(i * own_rows, own_rows), own_rows)
            one = dot_cols(dqkv[rows, :], w1buf[slot])
            two = dot_cols(hg[rows, :], w2buf[slot, :, : hg.shape[1]])
            both = one * gain1 + two * gain2
            z_put(v, i, rows, both)
            standard = (xbuf[slot, rows].astype(F32) - mean_ref[rows, :]) * inverse_ref[rows, :]
            add = lambda v: jnp.sum(v, 0, keepdims=True)
            mine_ref[0:4, columns] += jnp.concatenate(
                [add(one * standard), add(one), add(two * standard), add(two)], 0
            )
            return carry

        lax.fori_loop(0, tensor, row_block, 0)
        z_start(v, dgot, down_own)

    def v_copy(k, to, slot):
        return pltpu.make_async_remote_copy(
            src_ref=mine_ref,
            dst_ref=vgot.at[slot],
            send_sem=v_send.at[k - 1],
            recv_sem=v_recv.at[slot],
            device_id={"tensor": to},
            device_id_type=MESH,
        )

    def v_step(bit):
        return pltpu.make_async_remote_copy(
            src_ref=vsend.at[bit],
            dst_ref=vnow.at[bit],
            send_sem=v_send.at[tensor + bit],
            recv_sem=v_recv.at[tensor + bit],
            device_id={"dp": partner(bit)},
            device_id_type=MESH,
        )

    left_at = {}
    for item, entry in enumerate(plan):
        if entry[3]:
            left_at[item] = lefts[len(left_at)]

    def fetch_copy(item, c):
        column = pl.multiple_of((c - plan[item][0]) * deep, deep)
        slot = lax.rem(c, 2)
        return pltpu.make_async_copy(
            left_at[item].at[:, pl.ds(column, deep)], abuf.at[slot], a_sem.at[slot]
        )

    def fetch(c):
        def start(item):
            if item in left_at:
                fetch_copy(item, c).start()

        on_items(c, start)

    def g_copy():
        return pltpu.make_async_copy(g_ref, gbuf, b_sem.at[0])

    def n1_copy():
        return pltpu.make_async_copy(n1_ref, gbuf, b_sem.at[1])

    def on_items(c, act):
        for item, (first, count, _, _, _) in enumerate(plan):
            @pl.when((c >= first) & (c < first + count))
            def _():
                act(item)

    even, odd = list(range(bits)), [0, *range(2, bits), 1]

    def mixed(level, parity, of):
        first, second = of(even[level]), of(odd[level])
        return first + parity * (second - first)

    def base(level, parity):
        row = 0
        for k in range(level):
            row = row + mixed(k, parity, bit_of) * (deep >> (k + 1))
        return row

    def down_copy(level, c):
        parity, slot = lax.rem(c, 2), lax.rem(c, slots)
        half = deep >> (level + 1)
        if level == 0:
            row = pl.multiple_of((1 - bit_of(0)) * half, half)
            source, target = full.at[lax.rem(c, 3), pl.ds(row, half)], r0.at[slot]
        else:
            source, target = sent[level - 1].at[slot], got[level - 1].at[slot]
        return pltpu.make_async_remote_copy(
            src_ref=source,
            dst_ref=target,
            send_sem=send_sem.at[level, lax.rem(c, ring)],
            recv_sem=recv_sem.at[level, lax.rem(c, ring)],
            device_id={"dp": mixed(level, parity, partner)},
            device_id_type=MESH,
        )

    def up_copy(level, c):
        parity, slot = lax.rem(c, 2), lax.rem(c, ring)
        size = deep >> (level + 1)
        row = base(level + 1, parity)
        rows = pl.ds(pl.multiple_of(row, size), size)
        return pltpu.make_async_remote_copy(
            src_ref=ag.at[slot, rows],
            dst_ref=ag.at[slot, rows],
            send_sem=send_sem.at[bits + level, slot],
            recv_sem=recv_sem.at[bits + level, slot],
            device_id={"dp": mixed(level, parity, partner)},
            device_id_type=MESH,
        )

    def out_copy(item, c):
        slot = lax.rem(c, ring)
        row = pl.multiple_of((c - plan[item][0]) * deep, deep)
        return pltpu.make_async_copy(
            ag.at[slot], out_refs[item].at[pl.ds(row, deep)], o_sem.at[slot]
        )

    def multiply(c):
        slot = lax.rem(c, 3)

        def with_item(item):
            _, _, right, _, local = plan[item]
            right = gbuf if right is None else hg if right == "hidden" else extra_refs[right]
            if item in left_at:
                fetch_copy(item, c).wait()
                left = abuf[lax.rem(c, 2)].T
            else:
                column = pl.multiple_of((c - plan[item][0]) * deep, deep)
                held = {"hidden": hg, "projected": dqkv, "attended": att_ref}[local]
                left = held[:, pl.ds(column, deep)].T
            step = min(512, wide)
            for column in range(0, wide, step):
                full[slot, :, column : column + step] = dot(left, right[:, column : column + step])

        on_items(c, with_item)
        down_copy(0, c).start()

    def halve(level, c):
        parity, slot = lax.rem(c, 2), lax.rem(c, slots)
        down_copy(level - 1, c).wait()
        size = deep >> level
        half = size // 2
        if level < bits:
            bit = mixed(level, parity, bit_of)
            keep = pl.multiple_of(bit * half, half)
            give = pl.multiple_of((1 - bit) * half, half)
            pieces = ((keep, True), (give, False))
        else:
            pieces = ((0, True),)
            half = size
        for row, stays in pieces:
            if level == 1:
                mine = full[
                    lax.rem(c, 3), pl.ds(pl.multiple_of(bit_of(0) * size + row, half), half)
                ]
                value = mine + r0[slot, pl.ds(row, half)]
            else:
                mine = kept[level - 2][slot, pl.ds(row, half)]
                value = mine + got[level - 2][slot, pl.ds(row, half)].astype(F32)
            if level == bits:
                at = pl.multiple_of(base(bits, parity), size)
                ag[lax.rem(c, ring), pl.ds(at, size)] = value.astype(BF16)
            elif stays:
                kept[level - 1][slot] = value
            else:
                sent[level - 1][slot] = value.astype(BF16)
        if level < bits:
            down_copy(level, c).start()
        else:
            up_copy(bits - 1, c).start()

    def widen(level, c):
        up_copy(level, c).wait()
        up_copy(level - 1, c).start()

    def finish(c):
        up_copy(0, c).wait()
        on_items(c, lambda item: out_copy(item, c).start())

    fetch(0)
    g_copy().start()
    for copy in hidden_copies(0) + branch_copies(0):
        copy.start()
    mine_ref[...] = vec_ref[...]
    g_copy().wait()

    def stage(t, delay, act):
        c = t - delay

        @pl.when((c >= 0) & (c < chunks))
        def _():
            act(c)

    def stage_of(t, first, count, act):
        @pl.when((t >= first) & (t < first + count))
        def _():
            act(t - first)

    def iteration(t, carry):
        @pl.when(t + 1 < chunks)
        def _():
            fetch(t + 1)

        @pl.when(t == plan[2][0])
        def _():
            n1_copy().start()

        @pl.when(t == plan[3][0])
        def _():
            n1_copy().wait()

        @pl.when(t == begin - 1)
        def _():
            for copy in unit_copies(0):
                copy.start()

        stage_of(t, 0, blocks, far_start)
        stage(
            t, 2 * bits * lag + 1,
            lambda c: on_items(c, lambda item: out_copy(item, c).wait()),
        )
        stage(t, 2 * bits * lag, finish)
        for level in range(1, bits):
            stage(t, (2 * bits - level) * lag, lambda c, level=level: widen(level, c))
        for level in range(bits, 0, -1):
            stage(t, level * lag, lambda c, level=level: halve(level, c))
        stage(t, 0, multiply)

        stage_of(t, 1, blocks, lambda p: near_load(p).start())
        stage_of(t, 2, blocks, relay)
        stage_of(t, 3, blocks, lambda p: [copy.start() for copy in own_loads(p)])
        stage_of(t, 4, blocks, turn_block)
        stage_of(t, 0, hidden_units, hidden_unit)
        stage_of(t, 0, units, branch_unit)
        stage_of(t, begin, units, unit)

        @pl.when(t == begin + units)
        def _():
            for k in range(1, tensor):
                v_copy(k, lax.rem(me + k, tensor), me).start()
            vgot[me] = mine_ref[...]

        @pl.when(t == begin + units + 2)
        def _():
            for k in range(1, tensor):
                other = lax.rem(me + k, tensor)
                v_copy(k, other, me).wait_send()
                v_copy(k, other, other).wait_recv()
            line = lax.broadcasted_iota(jnp.int32, mine_ref.shape, 0)
            both = vgot[0]
            for k in range(1, tensor):
                both = both + vgot[k]
            vsend[0] = jnp.where(line < 5, both, mine_ref[...])
            v_step(0).start()

        for bit in range(bits):
            @pl.when(t == begin + units + 4 + 2 * bit)
            def _():
                v_step(bit).wait()
                both = vsend[bit] + vnow[bit]
                if bit + 1 < bits:
                    vsend[bit + 1] = both
                    v_step(bit + 1).start()
                else:
                    total_ref[...] = both

        return carry

    lax.fori_loop(0, max(chunks + 2 * bits * lag + 1, begin + units + 3 + 2 * bits), iteration, 0)

    def gather(u, carry):
        for k in range(1, tensor):
            z_copy(k, u, bgot).wait_recv()
            z_copy(k, units + u, dgot).wait_recv()
        return carry

    lax.fori_loop(0, units, gather, 0)
    for v in range(2 * units - zslots, 2 * units):
        for k in range(1, tensor):
            z_copy(k, v, dgot).wait_send()
    for v in range(2 * units - 2, 2 * units):
        own_copy(v, down_own).wait()


def reduce_grads(pairs, kv_grads, dq, vectors, tables, moments_of, gains, weights, x, sizes):
    act, att, n2, grads, n1, slope, forward = pairs
    bits, tensor, heads, head_dim = sizes
    fc1_weight, fc2_weight, w1, flat_out = weights
    deep = 256
    rows, wide = grads.shape
    hidden_width, width = act.shape[1], heads * head_dim
    natural = hidden_width == wide
    shapes = [
        (hidden_width, None, True, None),
        (width, None, False, "attended"),
        (wide, "hidden", True, None) if natural else (hidden_width, 0, False, "hidden"),
        (3 * width, None, False, "projected"),
    ]
    plan, first = [], 0
    for size, right, fetched, local in shapes:
        plan.append((first, size // deep, right, fetched, local))
        first += size // deep
    chunks, ring, slots, zslots = first, 2 * bits + 4, 4, 5
    blocks = 8 if chunks >= 20 else 4
    block = rows // blocks
    own_rows, units = rows // tensor, wide // deep
    halves_of = [deep >> (level + 1) for level in range(1, bits)]
    hbm = pl.BlockSpec(memory_space=pl.ANY)
    vmem = pl.BlockSpec(memory_space=pltpu.VMEM)
    lefts = [act, n2] if natural else [act]
    extra = [] if natural else [n2]
    dims = (chunks, bits, tensor, heads, head_dim, blocks, len(extra))
    return pl.pallas_call(
        lambda *refs: reduce_kernel(plan, dims, *refs),
        name="reduce_grads",
        in_specs=[hbm] * 13 + [vmem] * len(extra) + [hbm] * len(lefts) + [vmem] * 8,
        out_specs=[hbm] * 8 + [vmem],
        out_shape=[
            *[jax.ShapeDtypeStruct((item[0], wide), BF16) for item in shapes],
            *[
                jax.ShapeDtypeStruct((own_rows, wide), F32),
                jax.ShapeDtypeStruct((tensor - 1, own_rows, wide), BF16),
            ]
            * 2,
            jax.ShapeDtypeStruct(vectors.shape, F32),
        ],
        scratch_shapes=[
            pltpu.VMEM((2, rows, deep), BF16),
            pltpu.VMEM((3, deep, wide), F32),
            pltpu.VMEM((slots, deep // 2, wide), F32),
            pltpu.VMEM((ring, deep, wide), BF16),
            pltpu.VMEM((rows, wide), BF16),
            pltpu.VMEM((rows, hidden_width), BF16),
            pltpu.VMEM((rows, 3 * width), BF16),
            *[pltpu.VMEM((slots, half, wide), F32) for half in halves_of],
            *[pltpu.VMEM((slots, half, wide), BF16) for half in halves_of],
            *[pltpu.VMEM((slots, half, wide), BF16) for half in halves_of],
            pltpu.VMEM((2, deep, 3 * width), BF16),
            pltpu.VMEM((2, deep, wide), BF16),
            pltpu.VMEM((2, rows, deep), BF16),
            pltpu.VMEM((2, rows, deep), F32),
            pltpu.VMEM((2, width, deep), BF16),
            pltpu.VMEM((2, rows, deep), F32),
            pltpu.VMEM((zslots, rows, deep), BF16),
            pltpu.VMEM((2, own_rows, deep), F32),
            pltpu.VMEM(vectors.shape, F32),
            pltpu.VMEM((2, block, 2 * width), F32),
            pltpu.VMEM((2, block, 2 * width), F32),
            pltpu.VMEM((2, block, width), F32),
            pltpu.VMEM((4, block, 2 * width), BF16),
            pltpu.VMEM((rows, 2 * width), BF16),
            pltpu.VMEM((rows, 2 * width), BF16),
            pltpu.VMEM((tensor, *vectors.shape), F32),
            pltpu.VMEM((bits, *vectors.shape), F32),
            pltpu.VMEM((bits, *vectors.shape), F32),
            pltpu.SemaphoreType.DMA((2,)),
            pltpu.SemaphoreType.DMA((ring,)),
            pltpu.SemaphoreType.DMA((2 * bits, ring)),
            pltpu.SemaphoreType.DMA((2 * bits, ring)),
            pltpu.SemaphoreType.DMA((tensor - 1, 2 * units)),
            pltpu.SemaphoreType.DMA((tensor - 1, 2 * units)),
            pltpu.SemaphoreType.DMA((tensor + bits,)),
            pltpu.SemaphoreType.DMA((tensor + bits,)),
            pltpu.SemaphoreType.DMA((6, 2)),
            pltpu.SemaphoreType.DMA((2,)),
            pltpu.SemaphoreType.DMA((3, 2)),
            pltpu.SemaphoreType.DMA((4, blocks)),
            pltpu.SemaphoreType.DMA((2,)),
        ],
        compiler_params=pltpu.CompilerParams(
            collective_id=0, has_side_effects=True, vmem_limit_bytes=63 << 20
        ),
        cost_estimate=cost(
            2 * rows * wide * (chunks * deep + 2 * hidden_width + 3 * width), 8 * chunks * deep * wide
        ),
    )(
        grads, n1, slope, fc1_weight, fc2_weight, w1, x, flat_out, forward, *kv_grads, dq,
        *extra, *lefts, att, vectors, *gains, *moments_of, *tables,
    )


def body(
    tokens, out_grad, segment_ids, positions, norm1_gain, norm1_bias, norm2_gain, norm2_bias,
    qkv_weight, qkv_bias, out_weight, out_bias, fc1_weight, fc1_bias, fc2_weight, fc2_bias,
):
    model_width, heads, _, head_dim = qkv_weight.shape
    width = heads * head_dim
    hidden_width = fc1_weight.shape[1]
    row = lambda v: v.reshape(1, -1).astype(F32)
    w4 = jnp.transpose(qkv_weight, (0, 2, 1, 3))
    flat_bias = jnp.transpose(qkv_bias, (1, 0, 2)).reshape(1, 3 * width).astype(F32)
    flat_out = out_weight.reshape(width, model_width)
    tables = rope_tables(positions, 128)
    small = [
        row(norm1_gain), row(norm1_bias), row(norm2_gain), row(norm2_bias), flat_bias, row(fc1_bias)
    ]
    tensor, last = lax.axis_size("tensor"), lax.axis_size("dp") - 1
    (
        rows_all, grads_all, flat_qkv, normed_one, normed_two, queries, kv_own, kv_near, kv_far,
        activated, slope, forward, attended_grad, mean, inverse,
    ) = front(
        tokens, out_grad, w4, fc1_weight, fc2_weight, flat_out, small, tables,
        (tensor, last, heads, head_dim),
    )
    assert MOST - 2 < 2 * rows_all.shape[0]
    attended, query_grad, *kv_grads = attention(
        queries, [kv_far, kv_near, kv_own], attended_grad, positions, heads, head_dim
    )
    own_grad = out_grad.astype(F32)
    vectors = jnp.pad(jnp.sum(own_grad, 0, keepdims=True), ((4, 3), (0, 0)))
    bits = last.bit_length()
    *stacked, d_sum, d_got, branch, b_got, vectors = reduce_grads(
        (activated, attended, normed_two, grads_all, normed_one, slope, forward), kv_grads, query_grad,
        vectors, tables, (mean, inverse), (row(norm1_gain), row(norm2_gain)),
        (fc1_weight, fc2_weight, flat_qkv, flat_out), rows_all,
        (bits, tensor, heads, head_dim),
    )
    for k in range(d_got.shape[0]):
        d_sum = d_sum + d_got[k].astype(F32)
        branch = branch + b_got[k].astype(F32)
    natural = hidden_width == model_width
    fc2_grad, out_weight_grad, fc1_grad, qkv_weight_grad = finish(
        *stacked, heads, head_dim, natural
    )
    out_weight_grad = out_weight_grad.reshape(heads, head_dim, model_width)
    qkv_weight_grad = jnp.transpose(qkv_weight_grad, (0, 2, 1, 3))
    fc1_bias_grad = vectors[5, :hidden_width]
    qkv_bias_grad = vectors[6, : 3 * width].reshape(3, heads, head_dim)
    qkv_bias_grad = jnp.transpose(qkv_bias_grad, (1, 0, 2))
    own_rows = tokens.astype(F32)
    block_out = own_rows + branch + out_bias.astype(F32) + fc2_bias.astype(F32)
    own_mean, own_inverse = moments(own_rows)
    standard = (own_rows - own_mean) * own_inverse
    tokens_grad = own_grad + own_inverse * (
        d_sum
        - jnp.mean(d_sum, -1, keepdims=True)
        - standard * jnp.mean(d_sum * standard, -1, keepdims=True)
    )
    return (
        block_out.astype(BF16), tokens_grad.astype(BF16),
        vectors[0], vectors[1], vectors[2], vectors[3],
        qkv_weight_grad, qkv_bias_grad, out_weight_grad, vectors[4],
        fc1_grad, fc1_bias_grad, fc2_grad, vectors[4],
    )


def solution(mesh):
    rows = P(("dp", "tensor"), None)
    return jax.shard_map(
        body,
        mesh=mesh,
        in_specs=(
            rows, rows, P("dp"), P("dp"), P(), P(), P(), P(),
            P(None, "tensor", None, None), P("tensor", None, None), P("tensor", None, None), P(),
            P(None, "tensor"), P("tensor"), P("tensor", None), P(),
        ),
        out_specs=(
            rows, rows, P(), P(), P(), P(),
            P(None, "tensor", None, None), P("tensor", None, None), P("tensor", None, None), P(),
            P(None, "tensor"), P("tensor"), P("tensor", None), P(),
        ),
        check_vma=False,
    )
```

```python
import functools
import math

import jax
import jax.numpy as jnp
from jax import lax
from jax.experimental import pallas as pl
from jax.experimental.pallas import tpu as pltpu
from jax.sharding import PartitionSpec as P

ROT = 64
MOST = 2000
EPSILON = 1e-05
BF16 = jnp.bfloat16
F32 = jnp.float32
MESH = pl.DeviceIdType.MESH


def dot_rows(first, second):
    return lax.dot_general(first, second, (((0,), (0,)), ((), ())), preferred_element_type=F32)


def dot_cols(first, second):
    return lax.dot_general(first, second, (((1,), (1,)), ((), ())), preferred_element_type=F32)


def dot(first, second):
    return jnp.dot(first, second, preferred_element_type=F32)


def cost(flops, bytes_accessed):
    return pl.CostEstimate(flops=int(flops), bytes_accessed=int(bytes_accessed), transcendentals=0)


def params(*semantics):
    return pltpu.CompilerParams(dimension_semantics=semantics, vmem_limit_bytes=60 << 20)


def moments(values):
    average = jnp.mean(values, -1, keepdims=True)
    centered = values - average
    variance = jnp.mean(centered * centered, -1, keepdims=True)
    return average, lax.rsqrt(variance + EPSILON)


def rope_tables(position, lanes):
    half = ROT // 2
    frequency = jnp.power(F32(10000.0), -jnp.arange(half, dtype=F32) / F32(half))
    angles = position.astype(F32)[:, None] * frequency[None, :]
    cosine, sine = jnp.cos(angles), jnp.sin(angles)
    rows = position.shape[0]
    ones = jnp.ones((rows, lanes - ROT), F32)
    return (
        jnp.concatenate([cosine, cosine, ones], 1),
        jnp.concatenate([-sine, sine, 0 * ones], 1),
    )


def turn(values, cos_block, sin_block):
    lane = lax.broadcasted_iota(jnp.int32, values.shape, 1)
    half = ROT // 2
    up = pltpu.roll(values, values.shape[1] - half, 1)
    down = pltpu.roll(values, half, 1)
    return values * cos_block + jnp.where(lane < half, up, down) * sin_block


PIECES = 4


def front_kernel(dims, *refs):
    tensor, last, heads, head_dim = dims
    refs = list(refs)
    take = lambda count: [refs.pop(0) for _ in range(count)]
    tokens_ref, grads_ref, w4_ref, up_ref, down_ref, out_ref = take(6)
    g1_ref, b1_ref, g2_ref, b2_ref, qb_ref, ub_ref, cos_ref, sin_ref = take(8)
    rows_out, grads_out, flat_out, n1_out, n2_out, q_out, kv_own, kv_near, kv_far = take(9)
    act_out, slope_out, forward_out, agrad_out, mean_ref, inverse_ref = take(6)
    both, wq, w_up, w_down, w_out, wstage = take(6)
    n1s, n2s, qs, kvs, acts, slopes, forwards, agrads = take(8)
    own_sem, w_sem, q_sem, send_sem, recv_sem, kv_sems, s_sem = take(7)
    index, me = lax.axis_index("dp"), lax.axis_index("tensor")
    own = tokens_ref.shape[0]
    piece = own // PIECES
    width, depth = heads * head_dim, tokens_ref.shape[1]
    hidden_width = act_out.shape[1]
    span = tensor * PIECES

    barrier = pltpu.get_barrier_semaphore()

    def greet(axis, to):
        pl.semaphore_signal(barrier, inc=1, device_id={axis: to}, device_id_type=MESH)

    sides = [
        (me < tensor - 1, "tensor", me + 1),
        (me > 0, "tensor", me - 1),
        (index < last, "dp", index + 1),
        (index > 0, "dp", index - 1),
    ]
    for there, axis, to in sides:
        @pl.when(there)
        def _():
            greet(axis, to)

    pl.semaphore_wait(barrier, sum(jnp.where(there, 1, 0) for there, _, _ in sides))

    def rows_of(shard):
        return pl.ds(pl.multiple_of(shard * own, own), own)

    own_copies = [
        pltpu.make_async_copy(source, both.at[a, rows_of(me)], own_sem.at[a])
        for a, source in enumerate((tokens_ref, grads_ref))
    ]
    weight_copies = [
        pltpu.make_async_copy(up_ref, w_up, w_sem.at[0]),
        pltpu.make_async_copy(down_ref, w_down, w_sem.at[1]),
        pltpu.make_async_copy(out_ref, w_out, w_sem.at[2]),
    ]
    wrows = wstage.shape[1]

    def wq_copy(b):
        return pltpu.make_async_copy(
            w4_ref.at[pl.ds(pl.multiple_of(b * wrows, wrows), wrows)],
            wstage.at[lax.rem(b, 2)], q_sem.at[lax.rem(b, 2)],
        )

    flat_copy = pltpu.make_async_copy(wq, flat_out, w_sem.at[3])
    for copy in own_copies:
        copy.start()
    wq_copy(0).start()
    wq_copy(1).start()
    for copy in weight_copies:
        copy.start()
    for copy in own_copies:
        copy.wait()

    def hop(t, shard, p, direction):
        rows = pl.ds(pl.multiple_of(shard * own + p * piece, piece), piece)
        here = both.at[t // span, rows]
        to = me + 1 if direction == 0 else me - 1
        return pltpu.make_async_remote_copy(
            src_ref=here,
            dst_ref=here,
            send_sem=send_sem.at[direction, t],
            recv_sem=recv_sem.at[direction, t],
            device_id={"tensor": jnp.clip(to, 0, tensor - 1)},
            device_id_type=MESH,
        )

    def passing(t):
        k, p = lax.rem(t // PIECES, tensor), lax.rem(t, PIECES)
        return k, p, ((me - k, me - k >= 0, me < tensor - 1), (me + k, me + k < tensor, me > 0))

    def relay(t):
        k, p, ways = passing(t)
        for direction, (shard, held, onward) in enumerate(ways):
            @pl.when(held & (k > 0))
            def _():
                hop(t - PIECES, shard, p, direction).wait_recv()

            @pl.when(held & onward)
            def _():
                hop(t, shard, p, direction).start()

    def drain(t, carry):
        k, p, ways = passing(t)
        for direction, (shard, held, onward) in enumerate(ways):
            @pl.when(held & onward)
            def _():
                hop(t, shard, p, direction).wait_send()

        return carry

    tables = []
    for m in range(tensor):
        near = sorted(range(tensor), key=lambda shard: (abs(shard - m), shard))
        tables.append(near)

    def shard_at(j):
        found = 0
        for m in range(tensor):
            for place in range(tensor):
                hit = (me == m) & (j == place)
                found = found + jnp.where(hit, tables[m][place], 0)
        return found

    def outs_project(shard):
        rows = rows_of(shard)
        return [
            pltpu.make_async_copy(both.at[0, rows], rows_out.at[rows], s_sem.at[0]),
            pltpu.make_async_copy(n1s, n1_out.at[rows], s_sem.at[1]),
            pltpu.make_async_copy(n2s, n2_out.at[rows], s_sem.at[2]),
            pltpu.make_async_copy(qs, q_out.at[rows], s_sem.at[3]),
            pltpu.make_async_copy(kvs, kv_own.at[rows], s_sem.at[4]),
        ]

    def outs_up(shard):
        rows = rows_of(shard)
        return [
            pltpu.make_async_copy(acts, act_out.at[rows], s_sem.at[5]),
            pltpu.make_async_copy(slopes, slope_out.at[rows], s_sem.at[6]),
        ]

    def out_forward(shard):
        return pltpu.make_async_copy(forwards, forward_out.at[rows_of(shard)], s_sem.at[7])

    def outs_agrad(shard):
        rows = rows_of(shard)
        return [
            pltpu.make_async_copy(both.at[1, rows], grads_out.at[rows], s_sem.at[8]),
            pltpu.make_async_copy(agrads, agrad_out.at[rows], s_sem.at[9]),
        ]

    def near_copy(j):
        rows = rows_of(shard_at(j))
        return pltpu.make_async_remote_copy(
            src_ref=kvs,
            dst_ref=kv_near.at[rows],
            send_sem=kv_sems.at[0, j],
            recv_sem=kv_sems.at[1, j],
            device_id={"dp": jnp.minimum(index + 1, last)},
            device_id_type=MESH,
        )

    def far_copy(j):
        rows = rows_of(shard_at(j))
        return pltpu.make_async_remote_copy(
            src_ref=kv_near.at[rows],
            dst_ref=kv_far.at[rows],
            send_sem=kv_sems.at[2, j],
            recv_sem=kv_sems.at[3, j],
            device_id={"dp": jnp.minimum(index + 1, last)},
            device_id_type=MESH,
        )

    def project_shard(j):
        shard = shard_at(j)
        rows = rows_of(shard)

        @pl.when(j > 0)
        def _():
            for copy in outs_project(shard_at(j - 1)):
                copy.wait()

            @pl.when(index < last)
            def _():
                near_copy(j - 1).wait_send()

        x = both[0, rows].astype(F32)
        average, inverse = moments(x)
        mean_ref[rows, :] = average
        inverse_ref[rows, :] = inverse
        standard = (x - average) * inverse
        n1s[...] = (standard * g1_ref[...] + b1_ref[...]).astype(BF16)
        n2s[...] = (standard * g2_ref[...] + b2_ref[...]).astype(BF16)
        cos_block, sin_block = cos_ref[rows, :], sin_ref[rows, :]
        lanes = cos_block.shape[1]
        scale = 1.0 / math.sqrt(head_dim)
        for part in range(3):
            low = part * width
            projected = dot(n1s[...], wq[:, low : low + width]) + qb_ref[:, low : low + width]
            if part == 2:
                kvs[:, width:] = projected.astype(BF16)
                continue
            for head in range(heads):
                at = head * head_dim
                turned = turn(projected[:, at : at + lanes], cos_block, sin_block)
                other = projected[:, at + lanes : at + head_dim]
                if part == 0:
                    qs[:, at : at + lanes] = (turned * scale).astype(BF16)
                    qs[:, at + lanes : at + head_dim] = (other * scale).astype(BF16)
                else:
                    kvs[:, at : at + lanes] = turned.astype(BF16)
                    kvs[:, at + lanes : at + head_dim] = other.astype(BF16)
        for copy in outs_project(shard):
            copy.start()

        @pl.when(index < last)
        def _():
            near_copy(j).start()

    def up_half(j, half):
        if half == 0:
            @pl.when(j > 0)
            def _():
                for copy in outs_up(shard_at(j - 1)):
                    copy.wait()

        size = hidden_width // 2
        step = min(512, size)
        for column in range(half * size, (half + 1) * size, step):
            part = slice(column, column + step)
            hidden = dot(n2s[...], w_up[:, part]) + ub_ref[:, part]
            phi = (1.0 + lax.erf(hidden * F32(math.sqrt(0.5)))) * 0.5
            acts[:, part] = (hidden * phi).astype(BF16)
            density = jnp.exp(hidden * hidden * -0.5) * F32(1.0 / math.sqrt(2.0 * math.pi))
            slopes[:, part] = phi + hidden * density
        if half == 1:
            for copy in outs_up(shard_at(j)):
                copy.start()

    def forward_shard(j):
        @pl.when(j > 0)
        def _():
            out_forward(shard_at(j - 1)).wait()

        step = min(512, depth)
        for column in range(0, depth, step):
            part = slice(column, column + step)
            forwards[:, part] = dot(acts[...], w_down[:, part])
        out_forward(shard_at(j)).start()

    def pass_kv(j):
        @pl.when(index > 0)
        def _():
            near_copy(j).wait_recv()

            @pl.when(index < last)
            def _():
                far_copy(j).start()

    def agrad_shard(j):
        @pl.when(j > 0)
        def _():
            for copy in outs_agrad(shard_at(j - 1)):
                copy.wait()

        shard = shard_at(j)
        agrads[...] = dot_cols(both[1, rows_of(shard)], w_out[...]).astype(BF16)
        for copy in outs_agrad(shard):
            copy.start()

    def on(condition, act):
        @pl.when(condition)
        def _():
            act()

    def slot(t, carry):
        on(t < 2 * span, lambda: relay(t))

        @pl.when(t == 2)
        def _():
            for b in range(depth // wrows):
                wq_copy(b).wait()
                for part in range(3):
                    wq[b * wrows : (b + 1) * wrows, part * width : (part + 1) * width] = wstage[
                        b % 2, :, part
                    ].reshape(wrows, width)
                if b + 2 < depth // wrows:
                    wq_copy(b + 2).start()
            flat_copy.start()

        j, sub = t // PIECES - 1, lax.rem(t, PIECES)
        working = (j >= 0) & (j < tensor)
        on(working & (sub == 0), lambda: project_shard(j))

        @pl.when(t == PIECES + 1)
        def _():
            weight_copies[0].wait()

        on(working & (sub == 1), lambda: up_half(j, 0))
        on(working & (sub == 2), lambda: up_half(j, 1))

        @pl.when(t == PIECES + 3)
        def _():
            weight_copies[1].wait()

        on(working & (sub == 3), lambda: forward_shard(j))
        before = j - 1
        on((before >= 0) & (before < tensor) & (sub == 1), lambda: pass_kv(before))

        @pl.when(t == span + PIECES)
        def _():
            weight_copies[2].wait()

        late = j - tensor
        on((late >= 0) & (late < tensor) & (sub == 0), lambda: agrad_shard(late))
        return carry

    lax.fori_loop(0, 2 * span + 1, slot, 0)
    final = shard_at(tensor - 1)
    for copy in outs_project(final) + outs_up(final) + [out_forward(final)] + outs_agrad(final):
        copy.wait()
    flat_copy.wait()

    @pl.when(index < last)
    def _():
        near_copy(tensor - 1).wait_send()

    def kv_drain(j, carry):
        @pl.when((index > 0) & (index < last))
        def _():
            far_copy(j).wait_send()

        @pl.when(index > 1)
        def _():
            far_copy(j).wait_recv()

        return carry

    lax.fori_loop(0, tensor, kv_drain, 0)
    lax.fori_loop(0, 2 * span, drain, 0)


def front(tokens, grads, w4, fc1_weight, fc2_weight, flat_out, small, tables, sizes):
    tensor, last, heads, head_dim = sizes
    own, depth = tokens.shape
    rows, width, hidden_width = own * tensor, heads * head_dim, fc1_weight.shape[1]
    span, wrows = tensor * PIECES, 256
    hbm = pl.BlockSpec(memory_space=pl.ANY)
    vmem = pl.BlockSpec(memory_space=pltpu.VMEM)
    shape = jax.ShapeDtypeStruct
    return pl.pallas_call(
        lambda *refs: front_kernel(sizes, *refs),
        name="front",
        in_specs=[hbm] * 6 + [vmem] * 8,
        out_specs=[hbm] * 13 + [vmem] * 2,
        out_shape=[
            shape((rows, depth), BF16),
            shape((rows, depth), BF16),
            shape((depth, 3 * width), BF16),
            shape((rows, depth), BF16),
            shape((rows, depth), BF16),
            shape((rows, width), BF16),
            *[shape((rows, 2 * width), BF16)] * 3,
            shape((rows, hidden_width), BF16),
            shape((rows, hidden_width), F32),
            shape((rows, depth), F32),
            shape((rows, width), BF16),
            shape((rows, 1), F32),
            shape((rows, 1), F32),
        ],
        scratch_shapes=[
            pltpu.VMEM((2, rows, depth), BF16),
            pltpu.VMEM((depth, 3 * width), BF16),
            pltpu.VMEM((depth, hidden_width), BF16),
            pltpu.VMEM((hidden_width, depth), BF16),
            pltpu.VMEM((width, depth), BF16),
            pltpu.VMEM((2, wrows, 3, heads, head_dim), BF16),
            pltpu.VMEM((own, depth), BF16),
            pltpu.VMEM((own, depth), BF16),
            pltpu.VMEM((own, width), BF16),
            pltpu.VMEM((own, 2 * width), BF16),
            pltpu.VMEM((own, hidden_width), BF16),
            pltpu.VMEM((own, hidden_width), F32),
            pltpu.VMEM((own, depth), F32),
            pltpu.VMEM((own, width), BF16),
            pltpu.SemaphoreType.DMA((2,)),
            pltpu.SemaphoreType.DMA((4,)),
            pltpu.SemaphoreType.DMA((2,)),
            pltpu.SemaphoreType.DMA((2, 2 * span)),
            pltpu.SemaphoreType.DMA((2, 2 * span)),
            pltpu.SemaphoreType.DMA((4, tensor)),
            pltpu.SemaphoreType.DMA((10,)),
        ],
        compiler_params=pltpu.CompilerParams(
            collective_id=1, has_side_effects=True, vmem_limit_bytes=62 << 20
        ),
        cost_estimate=cost(
            2 * rows * depth * (3 * width + 2 * hidden_width + width),
            2 * rows * (6 * depth + 4 * hidden_width),
        ),
    )(tokens, grads, w4, fc1_weight, fc2_weight, flat_out, *small, *tables)


def attention_kernel(heads, head_dim, parts, bk, first_ref, q_ref, do_ref, start_ref, *refs):
    kv_parts, refs = refs[:parts], refs[parts:]
    att_ref, dq_ref, refs = refs[0], refs[1], refs[2:]
    grad_parts, (kv_ref, dkv_ref, s_ref, dp_ref, o_ref, sems) = refs[:parts], refs[parts:]
    block = pl.program_id(0)
    bq = q_ref.shape[0]
    width = heads * head_dim
    rows_each = kv_ref.shape[0] // parts
    ahead = rows_each * (parts - 1)
    low = first_ref[block]
    high = (ahead + (block + 1) * bq + bk - 1) // bk
    row = ahead + block * bq + lax.broadcasted_iota(jnp.int32, (bq, 1), 0)
    start = start_ref[...]
    lane = lax.broadcasted_iota(jnp.int32, (bq, bk), 1)
    chunks = bk // 128

    @pl.when(block == 0)
    def _():
        copies = [
            pltpu.make_async_copy(
                part, kv_ref.at[pl.ds(k * rows_each, rows_each)], sems.at[k]
            )
            for k, part in enumerate(kv_parts)
        ]
        for copy in copies:
            copy.start()

        def clear(j, carry):
            dkv_ref[pl.ds(pl.multiple_of(j * 128, 128), 128), :] = jnp.zeros((128, 2 * width), F32)
            return carry

        lax.fori_loop(0, dkv_ref.shape[0] // 128, clear, 0)
        for copy in copies:
            copy.wait()

    def rows_of(j):
        return pl.ds(pl.multiple_of(j * bk, bk), bk)

    at = [head * head_dim for head in range(heads)]
    head_of = lambda ref, head: ref[:, at[head] : at[head] + head_dim]
    folded = lambda x, fold: functools.reduce(
        fold, [x[:, c * 128 : (c + 1) * 128] for c in range(chunks)]
    )

    def scores(j, best):
        rows = rows_of(j)
        column = j * bk + lane
        allowed = (column >= start) & (column <= row)
        out = []
        for head in range(heads):
            key = kv_ref[rows, at[head] : at[head] + head_dim]
            s = jnp.where(allowed, dot_cols(head_of(q_ref, head), key), -1e30)
            s_ref[head, j] = s
            out.append(jnp.maximum(best[head], folded(s, jnp.maximum)))
        for head in range(heads):
            value = kv_ref[rows, width + at[head] : width + at[head] + head_dim]
            dp_ref[head, j] = dot_cols(head_of(do_ref, head), value)
        return tuple(out)

    low_best = jnp.full((bq, 128), -1e30, F32)
    best = lax.fori_loop(low, high, scores, (low_best,) * heads)
    best = [jnp.max(b, 1, keepdims=True) for b in best]

    def weigh(j, carry):
        out = []
        for head in range(heads):
            total, mixed = carry[head]
            e = jnp.exp(s_ref[head, j] - best[head])
            s_ref[head, j] = e
            out.append(
                (total + folded(e, jnp.add), mixed + folded(e * dp_ref[head, j], jnp.add))
            )
        return tuple(out)

    zero = jnp.zeros((bq, 128), F32)
    sums = lax.fori_loop(low, high, weigh, ((zero, zero),) * heads)
    scale = [1.0 / jnp.sum(total, 1, keepdims=True) for total, _ in sums]
    delta = [jnp.sum(mixed, 1, keepdims=True) * k for (_, mixed), k in zip(sums, scale)]
    o_ref[...] = jnp.zeros_like(o_ref)

    def spread_back(j, carry):
        rows = rows_of(j)
        for head in range(heads):
            p = s_ref[head, j] * scale[head]
            p_low = p.astype(BF16)
            ds = (p * (dp_ref[head, j] - delta[head])).astype(BF16)
            keys = slice(at[head], at[head] + head_dim)
            values = slice(width + at[head], width + at[head] + head_dim)
            o_ref[head, :, :head_dim] += dot(p_low, kv_ref[rows, values])
            o_ref[head, :, head_dim:] += dot(ds, kv_ref[rows, keys])
            dkv_ref[rows, keys] += dot_rows(ds, head_of(q_ref, head))
            dkv_ref[rows, values] += dot_rows(p_low, head_of(do_ref, head))
        return carry

    lax.fori_loop(low, high, spread_back, 0)
    for head in range(heads):
        keys = slice(at[head], at[head] + head_dim)
        att_ref[:, keys] = o_ref[head, :, :head_dim].astype(BF16)
        dq_ref[:, keys] = o_ref[head, :, head_dim:] * (1.0 / math.sqrt(head_dim))

    @pl.when(block == pl.num_programs(0) - 1)
    def _():
        for k, part in enumerate(grad_parts):
            part[...] = dkv_ref[k * rows_each : (k + 1) * rows_each, :].astype(part.dtype)


def attention(q, kv_parts, do, positions, heads, head_dim):
    rows, width = q.shape
    parts = len(kv_parts)
    total = rows * parts
    bq = min(256, rows)
    bk = 256
    start = jnp.arange(rows, dtype=jnp.int32) - positions + (total - rows)
    first = start[::bq] // bk
    by_row = lambda i, f: (i, 0)
    whole = lambda i, f: (0, 0)
    part_types = [BF16] + [F32] * (parts - 1)
    return pl.pallas_call(
        lambda *refs: attention_kernel(heads, head_dim, parts, bk, *refs),
        name="attention",
        grid_spec=pltpu.PrefetchScalarGridSpec(
            num_scalar_prefetch=1,
            grid=(rows // bq,),
            in_specs=[
                pl.BlockSpec((bq, width), by_row),
                pl.BlockSpec((bq, width), by_row),
                pl.BlockSpec((bq, 1), by_row),
                *[pl.BlockSpec(memory_space=pl.ANY)] * parts,
            ],
            out_specs=[
                pl.BlockSpec((bq, width), by_row),
                pl.BlockSpec((bq, width), by_row),
                *[pl.BlockSpec((rows, 2 * width), whole, pipeline_mode=pl.Buffered(1))] * parts,
            ],
            scratch_shapes=[
                pltpu.VMEM((total, 2 * width), BF16),
                pltpu.VMEM((total, 2 * width), F32),
                pltpu.VMEM((heads, total // bk, bq, bk), F32),
                pltpu.VMEM((heads, total // bk, bq, bk), F32),
                pltpu.VMEM((heads, bq, 2 * head_dim), F32),
                pltpu.SemaphoreType.DMA((parts,)),
            ],
        ),
        out_shape=[
            jax.ShapeDtypeStruct((rows, width), BF16),
            jax.ShapeDtypeStruct((rows, width), F32),
            *[jax.ShapeDtypeStruct((rows, 2 * width), kind) for kind in part_types],
        ],
        compiler_params=params("arbitrary"),
        cost_estimate=cost(12 * rows * MOST * width, 8 * total * width),
    )(first, q, do, start[:, None], *kv_parts)


def finish_kernel(heads, head_dim, natural, *refs):
    fc2_ref, out_ref, fc1_ref, qkv_ref, x_ref, g_ref, d_ref, dgot_ref, b_ref, bgot_ref = refs[:10]
    bias_ref, fc2_to, out_to, fc1_to, qkv_to, block_to, tokens_to = refs[10:]
    x, grad, branch = x_ref[...].astype(F32), d_ref[...], b_ref[...]
    for k in range(dgot_ref.shape[0]):
        grad = grad + dgot_ref[k].astype(F32)
        branch = branch + bgot_ref[k].astype(F32)
    block_to[...] = (x + branch + bias_ref[0:1, :] + bias_ref[1:2, :]).astype(BF16)
    average, inverse = moments(x)
    standard = (x - average) * inverse
    tokens_to[...] = (
        g_ref[...].astype(F32)
        + inverse
        * (
            grad
            - jnp.mean(grad, -1, keepdims=True)
            - standard * jnp.mean(grad * standard, -1, keepdims=True)
        )
    ).astype(BF16)
    fc2_to[...] = fc2_ref[...].astype(F32)
    out_to[...] = out_ref[...].astype(F32)
    fc1_to[...] = (fc1_ref[...] if natural else fc1_ref[...].T).astype(F32)
    for part in range(3):
        for head in range(heads):
            at = (part * heads + head) * head_dim
            qkv_to[:, part, head, :] = qkv_ref[at : at + head_dim, :].T.astype(F32)


def finish(fc2, out, fc1, qkv, x, g, d, d_got, b, b_got, biases, heads, head_dim, natural):
    depth = fc2.shape[1]
    steps = 8
    by_row = lambda i: (i, 0)
    by_column = lambda i: (0, i)
    rows_of = lambda x: pl.BlockSpec((x.shape[0] // steps, x.shape[1]), by_row)
    columns_of = lambda x: pl.BlockSpec((x.shape[0], depth // steps), by_column)
    parts_of = lambda x: pl.BlockSpec((x.shape[0], x.shape[1] // steps, depth), lambda i: (0, i, 0))
    shape = lambda *dims: jax.ShapeDtypeStruct(dims, F32)
    fc1_shape = fc1.shape if natural else fc1.shape[::-1]
    return pl.pallas_call(
        lambda *refs: finish_kernel(heads, head_dim, natural, *refs),
        name="finish",
        grid=(steps,),
        in_specs=[
            rows_of(fc2), rows_of(out), rows_of(fc1) if natural else columns_of(fc1), columns_of(qkv),
            rows_of(x), rows_of(g), rows_of(d), parts_of(d_got), rows_of(b), parts_of(b_got),
            pl.BlockSpec(biases.shape, lambda i: (0, 0)),
        ],
        out_specs=[
            rows_of(fc2),
            rows_of(out),
            pl.BlockSpec((fc1_shape[0] // steps, fc1_shape[1]), by_row),
            pl.BlockSpec((depth // steps, 3, heads, head_dim), lambda i: (i, 0, 0, 0)),
            rows_of(x),
            rows_of(g),
        ],
        out_shape=[
            shape(*fc2.shape), shape(*out.shape), shape(*fc1_shape), shape(depth, 3, heads, head_dim),
            jax.ShapeDtypeStruct(x.shape, BF16), jax.ShapeDtypeStruct(g.shape, BF16),
        ],
        compiler_params=params("arbitrary"),
        cost_estimate=cost(0, 6 * (fc2.size + out.size + fc1.size + qkv.size)),
    )(fc2, out, fc1, qkv, x, g, d, d_got, b, b_got, biases)


def reduce_kernel(plan, dims, *refs):
    chunks, bits, tensor, heads, head_dim, blocks, wide_b = dims
    refs = list(refs)
    take = lambda count: [refs.pop(0) for _ in range(count)]
    g_ref, n1_ref, slope_ref, up_ref, down_ref, w1_ref, x_ref, wout_ref, forward_ref = take(9)
    far_ref, near_ref, own_ref, dq_ref = take(4)
    extra_refs = take(wide_b)
    lefts = take(sum(1 for item in plan if item[3]))
    att_ref, vec_ref, gain1_ref, gain2_ref, mean_ref, inverse_ref, cos_ref, sin_ref = take(8)
    out_refs = take(len(plan))
    down_own, dgot, branch_own, bgot, total_ref = take(5)
    abuf, full, r0, ag, gbuf, hg, dqkv = take(7)
    kept, sent, got = take(bits - 1), take(bits - 1), take(bits - 1)
    w1buf, w2buf, xbuf, sbuf, wobuf, fbuf, zsend, zown, mine_ref = take(9)
    near_buf, own_buf, dq_buf, hop_send, far_got, near_got = take(6)
    vgot, vsend, vnow = take(3)
    a_sem, o_sem, send_sem, recv_sem, d_send, d_recv, v_send, v_recv = take(8)
    w_sem, b_sem, h_sem, hop_sems, z_sem = take(5)
    index, me = lax.axis_index("dp"), lax.axis_index("tensor")
    last = (1 << bits) - 1
    deep, wide = full.shape[1], full.shape[2]
    rows_all = gbuf.shape[0]
    slots, ring, lag = r0.shape[0], ag.shape[0], 2

    def bit_of(bit):
        return (index // (1 << bit)) % 2

    def partner(bit):
        return index + (1 << bit) * (1 - 2 * bit_of(bit))

    barrier = pltpu.get_barrier_semaphore()

    def greet(axis, to):
        pl.semaphore_signal(barrier, inc=1, device_id={axis: to}, device_id_type=MESH)

    for bit in range(bits):
        greet("dp", partner(bit))
    for k in range(1, tensor):
        greet("tensor", lax.rem(me + k, tensor))

    @pl.when(index > 0)
    def _():
        greet("dp", index - 1)

    @pl.when(index < last)
    def _():
        greet("dp", index + 1)

    inner = jnp.where(index > 0, 1, 0) + jnp.where(index < last, 1, 0)
    pl.semaphore_wait(barrier, bits + tensor - 1 + inner)

    hidden_units = hg.shape[1] // deep

    def columns_of(u):
        return pl.ds(pl.multiple_of(u * deep, deep), deep)

    def hidden_copies(u):
        slot = lax.rem(u, 2)
        return [
            pltpu.make_async_copy(down_ref.at[columns_of(u)], w2buf.at[slot], w_sem.at[1, slot]),
            pltpu.make_async_copy(slope_ref.at[:, columns_of(u)], sbuf.at[slot], w_sem.at[3, slot]),
        ]

    row_step = min(256, rows_all)

    def hidden_unit(u):
        slot, columns = lax.rem(u, 2), columns_of(u)

        @pl.when(u + 1 < hidden_units)
        def _():
            for copy in hidden_copies(u + 1):
                copy.start()

        for copy in hidden_copies(u):
            copy.wait()

        def row_block(i, total):
            rows = pl.ds(pl.multiple_of(i * row_step, row_step), row_step)
            grad = dot_cols(gbuf[rows, :], w2buf[slot])
            low = (grad * sbuf[slot, rows, :]).astype(BF16)
            hg[rows, columns] = low
            return total + jnp.sum(low.astype(F32), 0, keepdims=True)

        total = lax.fori_loop(0, rows_all // row_step, row_block, jnp.zeros((1, deep), F32))
        mine_ref[5:6, columns] = total

    block = rows_all // blocks
    width = heads * head_dim

    def block_of(p):
        return pl.ds(pl.multiple_of(p * block, block), block)

    def far_copy(p):
        return pltpu.make_async_remote_copy(
            src_ref=far_ref.at[block_of(p)],
            dst_ref=far_got.at[block_of(p)],
            send_sem=hop_sems.at[0, p],
            recv_sem=hop_sems.at[1, p],
            device_id={"dp": jnp.maximum(index - 1, 0)},
            device_id_type=MESH,
        )

    def near_copy(p):
        return pltpu.make_async_remote_copy(
            src_ref=hop_send.at[lax.rem(p, 4)],
            dst_ref=near_got.at[block_of(p)],
            send_sem=hop_sems.at[2, p],
            recv_sem=hop_sems.at[3, p],
            device_id={"dp": jnp.maximum(index - 1, 0)},
            device_id_type=MESH,
        )

    def near_load(p):
        slot = lax.rem(p, 2)
        return pltpu.make_async_copy(near_ref.at[block_of(p)], near_buf.at[slot], h_sem.at[0, slot])

    def own_loads(p):
        slot = lax.rem(p, 2)
        return [
            pltpu.make_async_copy(own_ref.at[block_of(p)], own_buf.at[slot], h_sem.at[1, slot]),
            pltpu.make_async_copy(dq_ref.at[block_of(p)], dq_buf.at[slot], h_sem.at[2, slot]),
        ]

    def far_start(p):
        @pl.when(index > 0)
        def _():
            far_copy(p).start()

    def relay(p):
        slot = lax.rem(p, 2)

        @pl.when(index > 0)
        def _():
            far_copy(p).wait_send()

        near_load(p).wait()

        @pl.when(index < last)
        def _():
            far_copy(p).wait_recv()
            near_buf[slot] += far_got[block_of(p)].astype(F32)

        @pl.when(index > 0)
        def _():
            hop_send[lax.rem(p, 4)] = near_buf[slot].astype(BF16)
            near_copy(p).start()

    def turn_block(p):
        slot, rows = lax.rem(p, 2), block_of(p)

        @pl.when(index > 0)
        def _():
            near_copy(p).wait_send()

        for copy in own_loads(p):
            copy.wait()

        @pl.when(index < last)
        def _():
            near_copy(p).wait_recv()
            own_buf[slot] += near_got[rows].astype(F32)

        cos_block, sin_block = cos_ref[rows, :], -sin_ref[rows, :]
        lanes = cos_block.shape[1]
        for part in range(3):
            for head in range(heads):
                at = head * head_dim
                to = part * width + at
                if part == 0:
                    grad = dq_buf[slot, :, at : at + head_dim]
                else:
                    low = (part - 1) * width + at
                    grad = own_buf[slot, :, low : low + head_dim]
                if part < 2:
                    first = turn(grad[:, :lanes], cos_block, sin_block)
                    grad = jnp.concatenate([first, grad[:, lanes:]], 1)
                low_grad = grad.astype(BF16)
                dqkv[rows, to : to + head_dim] = low_grad
                mine_ref[6:7, to : to + head_dim] += jnp.sum(
                    low_grad.astype(F32), 0, keepdims=True
                )

    own_rows = down_own.shape[0]
    units = wide // deep
    zslots = zsend.shape[0]
    begin = max(chunks // 2 + 3, blocks + 4)

    def z_copy(k, v, target):
        other = lax.rem(me + k, tensor)
        rows = pl.ds(pl.multiple_of(other * own_rows, own_rows), own_rows)
        return pltpu.make_async_remote_copy(
            src_ref=zsend.at[lax.rem(v, zslots), rows],
            dst_ref=target.at[k - 1, :, columns_of(lax.rem(v, units))],
            send_sem=d_send.at[k - 1, v],
            recv_sem=d_recv.at[k - 1, v],
            device_id={"tensor": other},
            device_id_type=MESH,
        )

    def own_copy(v, target):
        slot = lax.rem(v, 2)
        return pltpu.make_async_copy(
            zown.at[slot], target.at[:, columns_of(lax.rem(v, units))], z_sem.at[slot]
        )

    def z_clear(v):
        @pl.when(v >= zslots)
        def _():
            for k in range(1, tensor):
                z_copy(k, v - zslots, dgot).wait_send()

        @pl.when(v >= 2)
        def _():
            own_copy(v - 2, down_own).wait()

    def z_put(v, i, rows, value):
        zsend[lax.rem(v, zslots), rows] = value.astype(BF16)

        @pl.when(i == me)
        def _():
            zown[lax.rem(v, 2)] = value

    def z_start(v, target, own_target):
        for k in range(1, tensor):
            z_copy(k, v, target).start()
        own_copy(v, own_target).start()

    def branch_copies(u):
        slot = lax.rem(u, 2)
        return [
            pltpu.make_async_copy(wout_ref.at[:, columns_of(u)], wobuf.at[slot], w_sem.at[4, slot]),
            pltpu.make_async_copy(forward_ref.at[:, columns_of(u)], fbuf.at[slot], w_sem.at[5, slot]),
        ]

    def branch_unit(u):
        slot = lax.rem(u, 2)

        @pl.when(u + 1 < units)
        def _():
            for copy in branch_copies(u + 1):
                copy.start()

        for copy in branch_copies(u):
            copy.wait()

        z_clear(u)

        def row_block(i, carry):
            rows = pl.ds(pl.multiple_of(i * own_rows, own_rows), own_rows)
            z_put(u, i, rows, dot(att_ref[rows, :], wobuf[slot]) + fbuf[slot, rows, :])
            return carry

        lax.fori_loop(0, tensor, row_block, 0)
        z_start(u, bgot, branch_own)

    def unit_copies(u):
        slot = lax.rem(u, 2)
        return [
            pltpu.make_async_copy(w1_ref.at[columns_of(u)], w1buf.at[slot], w_sem.at[0, slot]),
            pltpu.make_async_copy(
                up_ref.at[columns_of(u)], w2buf.at[slot, :, pl.ds(0, hg.shape[1])], w_sem.at[1, slot]
            ),
            pltpu.make_async_copy(x_ref.at[:, columns_of(u)], xbuf.at[slot], w_sem.at[2, slot]),
        ]

    def unit(u):
        slot, v = lax.rem(u, 2), units + u
        columns = columns_of(u)

        @pl.when(u + 1 < units)
        def _():
            for copy in unit_copies(u + 1):
                copy.start()

        for copy in unit_copies(u):
            copy.wait()

        z_clear(v)
        gain1, gain2 = gain1_ref[:, columns], gain2_ref[:, columns]
        mine_ref[0:4, columns] = jnp.zeros((4, deep), F32)

        def row_block(i, carry):
            rows = pl.ds(pl.multiple_of(i * own_rows, own_rows), own_rows)
            one = dot_cols(dqkv[rows, :], w1buf[slot])
            two = dot_cols(hg[rows, :], w2buf[slot, :, : hg.shape[1]])
            both = one * gain1 + two * gain2
            z_put(v, i, rows, both)
            standard = (xbuf[slot, rows].astype(F32) - mean_ref[rows, :]) * inverse_ref[rows, :]
            add = lambda v: jnp.sum(v, 0, keepdims=True)
            mine_ref[0:4, columns] += jnp.concatenate(
                [add(one * standard), add(one), add(two * standard), add(two)], 0
            )
            return carry

        lax.fori_loop(0, tensor, row_block, 0)
        z_start(v, dgot, down_own)

    def v_copy(k, to, slot):
        return pltpu.make_async_remote_copy(
            src_ref=mine_ref,
            dst_ref=vgot.at[slot],
            send_sem=v_send.at[k - 1],
            recv_sem=v_recv.at[slot],
            device_id={"tensor": to},
            device_id_type=MESH,
        )

    def v_step(bit):
        return pltpu.make_async_remote_copy(
            src_ref=vsend.at[bit],
            dst_ref=vnow.at[bit],
            send_sem=v_send.at[tensor + bit],
            recv_sem=v_recv.at[tensor + bit],
            device_id={"dp": partner(bit)},
            device_id_type=MESH,
        )

    left_at = {}
    for item, entry in enumerate(plan):
        if entry[3]:
            left_at[item] = lefts[len(left_at)]

    def fetch_copy(item, c):
        column = pl.multiple_of((c - plan[item][0]) * deep, deep)
        slot = lax.rem(c, 2)
        return pltpu.make_async_copy(
            left_at[item].at[:, pl.ds(column, deep)], abuf.at[slot], a_sem.at[slot]
        )

    def fetch(c):
        def start(item):
            if item in left_at:
                fetch_copy(item, c).start()

        on_items(c, start)

    def g_copy():
        return pltpu.make_async_copy(g_ref, gbuf, b_sem.at[0])

    def n1_copy():
        return pltpu.make_async_copy(n1_ref, gbuf, b_sem.at[1])

    def on_items(c, act):
        for item, (first, count, _, _, _) in enumerate(plan):
            @pl.when((c >= first) & (c < first + count))
            def _():
                act(item)

    even, odd = list(range(bits)), [0, *range(2, bits), 1]

    def mixed(level, parity, of):
        first, second = of(even[level]), of(odd[level])
        return first + parity * (second - first)

    def base(level, parity):
        row = 0
        for k in range(level):
            row = row + mixed(k, parity, bit_of) * (deep >> (k + 1))
        return row

    def down_copy(level, c):
        parity, slot = lax.rem(c, 2), lax.rem(c, slots)
        half = deep >> (level + 1)
        if level == 0:
            row = pl.multiple_of((1 - bit_of(0)) * half, half)
            source, target = full.at[lax.rem(c, 3), pl.ds(row, half)], r0.at[slot]
        else:
            source, target = sent[level - 1].at[slot], got[level - 1].at[slot]
        return pltpu.make_async_remote_copy(
            src_ref=source,
            dst_ref=target,
            send_sem=send_sem.at[level, lax.rem(c, ring)],
            recv_sem=recv_sem.at[level, lax.rem(c, ring)],
            device_id={"dp": mixed(level, parity, partner)},
            device_id_type=MESH,
        )

    def up_copy(level, c):
        parity, slot = lax.rem(c, 2), lax.rem(c, ring)
        size = deep >> (level + 1)
        row = base(level + 1, parity)
        rows = pl.ds(pl.multiple_of(row, size), size)
        return pltpu.make_async_remote_copy(
            src_ref=ag.at[slot, rows],
            dst_ref=ag.at[slot, rows],
            send_sem=send_sem.at[bits + level, slot],
            recv_sem=recv_sem.at[bits + level, slot],
            device_id={"dp": mixed(level, parity, partner)},
            device_id_type=MESH,
        )

    def out_copy(item, c):
        slot = lax.rem(c, ring)
        row = pl.multiple_of((c - plan[item][0]) * deep, deep)
        return pltpu.make_async_copy(
            ag.at[slot], out_refs[item].at[pl.ds(row, deep)], o_sem.at[slot]
        )

    def multiply(c):
        slot = lax.rem(c, 3)

        def with_item(item):
            _, _, right, _, local = plan[item]
            right = gbuf if right is None else hg if right == "hidden" else extra_refs[right]
            if item in left_at:
                fetch_copy(item, c).wait()
                left = abuf[lax.rem(c, 2)].T
            else:
                column = pl.multiple_of((c - plan[item][0]) * deep, deep)
                held = {"hidden": hg, "projected": dqkv, "attended": att_ref}[local]
                left = held[:, pl.ds(column, deep)].T
            step = min(512, wide)
            for column in range(0, wide, step):
                full[slot, :, column : column + step] = dot(left, right[:, column : column + step])

        on_items(c, with_item)
        down_copy(0, c).start()

    def halve(level, c):
        parity, slot = lax.rem(c, 2), lax.rem(c, slots)
        down_copy(level - 1, c).wait()
        size = deep >> level
        half = size // 2
        if level < bits:
            bit = mixed(level, parity, bit_of)
            keep = pl.multiple_of(bit * half, half)
            give = pl.multiple_of((1 - bit) * half, half)
            pieces = ((keep, True), (give, False))
        else:
            pieces = ((0, True),)
            half = size
        for row, stays in pieces:
            if level == 1:
                mine = full[
                    lax.rem(c, 3), pl.ds(pl.multiple_of(bit_of(0) * size + row, half), half)
                ]
                value = mine + r0[slot, pl.ds(row, half)]
            else:
                mine = kept[level - 2][slot, pl.ds(row, half)]
                value = mine + got[level - 2][slot, pl.ds(row, half)].astype(F32)
            if level == bits:
                at = pl.multiple_of(base(bits, parity), size)
                ag[lax.rem(c, ring), pl.ds(at, size)] = value.astype(BF16)
            elif stays:
                kept[level - 1][slot] = value
            else:
                sent[level - 1][slot] = value.astype(BF16)
        if level < bits:
            down_copy(level, c).start()
        else:
            up_copy(bits - 1, c).start()

    def widen(level, c):
        up_copy(level, c).wait()
        up_copy(level - 1, c).start()

    def finish(c):
        up_copy(0, c).wait()
        on_items(c, lambda item: out_copy(item, c).start())

    fetch(0)
    g_copy().start()
    for copy in hidden_copies(0) + branch_copies(0):
        copy.start()
    mine_ref[...] = vec_ref[...]
    g_copy().wait()

    def stage(t, delay, act):
        c = t - delay

        @pl.when((c >= 0) & (c < chunks))
        def _():
            act(c)

    def stage_of(t, first, count, act):
        @pl.when((t >= first) & (t < first + count))
        def _():
            act(t - first)

    def iteration(t, carry):
        @pl.when(t + 1 < chunks)
        def _():
            fetch(t + 1)

        @pl.when(t == plan[2][0])
        def _():
            n1_copy().start()

        @pl.when(t == plan[3][0])
        def _():
            n1_copy().wait()

        @pl.when(t == begin - 1)
        def _():
            for copy in unit_copies(0):
                copy.start()

        stage_of(t, 0, blocks, far_start)
        stage(
            t, 2 * bits * lag + 1,
            lambda c: on_items(c, lambda item: out_copy(item, c).wait()),
        )
        stage(t, 2 * bits * lag, finish)
        for level in range(1, bits):
            stage(t, (2 * bits - level) * lag, lambda c, level=level: widen(level, c))
        for level in range(bits, 0, -1):
            stage(t, level * lag, lambda c, level=level: halve(level, c))
        stage(t, 0, multiply)

        stage_of(t, 1, blocks, lambda p: near_load(p).start())
        stage_of(t, 2, blocks, relay)
        stage_of(t, 3, blocks, lambda p: [copy.start() for copy in own_loads(p)])
        stage_of(t, 4, blocks, turn_block)
        stage_of(t, 0, hidden_units, hidden_unit)
        stage_of(t, 0, units, branch_unit)
        stage_of(t, begin, units, unit)

        @pl.when(t == begin + units)
        def _():
            for k in range(1, tensor):
                v_copy(k, lax.rem(me + k, tensor), me).start()
            vgot[me] = mine_ref[...]

        @pl.when(t == begin + units + 2)
        def _():
            for k in range(1, tensor):
                other = lax.rem(me + k, tensor)
                v_copy(k, other, me).wait_send()
                v_copy(k, other, other).wait_recv()
            line = lax.broadcasted_iota(jnp.int32, mine_ref.shape, 0)
            both = vgot[0]
            for k in range(1, tensor):
                both = both + vgot[k]
            vsend[0] = jnp.where(line < 5, both, mine_ref[...])
            v_step(0).start()

        for bit in range(bits):
            @pl.when(t == begin + units + 4 + 2 * bit)
            def _():
                v_step(bit).wait()
                both = vsend[bit] + vnow[bit]
                if bit + 1 < bits:
                    vsend[bit + 1] = both
                    v_step(bit + 1).start()
                else:
                    total_ref[...] = both

        return carry

    lax.fori_loop(0, max(chunks + 2 * bits * lag + 1, begin + units + 3 + 2 * bits), iteration, 0)

    def gather(u, carry):
        for k in range(1, tensor):
            z_copy(k, u, bgot).wait_recv()
            z_copy(k, units + u, dgot).wait_recv()
        return carry

    lax.fori_loop(0, units, gather, 0)
    for v in range(2 * units - zslots, 2 * units):
        for k in range(1, tensor):
            z_copy(k, v, dgot).wait_send()
    for v in range(2 * units - 2, 2 * units):
        own_copy(v, down_own).wait()


def reduce_grads(pairs, kv_grads, dq, vectors, tables, moments_of, gains, weights, x, sizes):
    act, att, n2, grads, n1, slope, forward = pairs
    bits, tensor, heads, head_dim = sizes
    fc1_weight, fc2_weight, w1, flat_out = weights
    deep = 256
    rows, wide = grads.shape
    hidden_width, width = act.shape[1], heads * head_dim
    natural = hidden_width == wide
    shapes = [
        (hidden_width, None, True, None),
        (width, None, False, "attended"),
        (wide, "hidden", True, None) if natural else (hidden_width, 0, False, "hidden"),
        (3 * width, None, False, "projected"),
    ]
    plan, first = [], 0
    for size, right, fetched, local in shapes:
        plan.append((first, size // deep, right, fetched, local))
        first += size // deep
    chunks, ring, slots, zslots = first, 2 * bits + 4, 4, 5
    blocks = 8 if chunks >= 20 else 4
    block = rows // blocks
    own_rows, units = rows // tensor, wide // deep
    halves_of = [deep >> (level + 1) for level in range(1, bits)]
    hbm = pl.BlockSpec(memory_space=pl.ANY)
    vmem = pl.BlockSpec(memory_space=pltpu.VMEM)
    lefts = [act, n2] if natural else [act]
    extra = [] if natural else [n2]
    dims = (chunks, bits, tensor, heads, head_dim, blocks, len(extra))
    return pl.pallas_call(
        lambda *refs: reduce_kernel(plan, dims, *refs),
        name="reduce_grads",
        in_specs=[hbm] * 13 + [vmem] * len(extra) + [hbm] * len(lefts) + [vmem] * 8,
        out_specs=[hbm] * 8 + [vmem],
        out_shape=[
            *[jax.ShapeDtypeStruct((item[0], wide), BF16) for item in shapes],
            *[
                jax.ShapeDtypeStruct((own_rows, wide), F32),
                jax.ShapeDtypeStruct((tensor - 1, own_rows, wide), BF16),
            ]
            * 2,
            jax.ShapeDtypeStruct(vectors.shape, F32),
        ],
        scratch_shapes=[
            pltpu.VMEM((2, rows, deep), BF16),
            pltpu.VMEM((3, deep, wide), F32),
            pltpu.VMEM((slots, deep // 2, wide), F32),
            pltpu.VMEM((ring, deep, wide), BF16),
            pltpu.VMEM((rows, wide), BF16),
            pltpu.VMEM((rows, hidden_width), BF16),
            pltpu.VMEM((rows, 3 * width), BF16),
            *[pltpu.VMEM((slots, half, wide), F32) for half in halves_of],
            *[pltpu.VMEM((slots, half, wide), BF16) for half in halves_of],
            *[pltpu.VMEM((slots, half, wide), BF16) for half in halves_of],
            pltpu.VMEM((2, deep, 3 * width), BF16),
            pltpu.VMEM((2, deep, wide), BF16),
            pltpu.VMEM((2, rows, deep), BF16),
            pltpu.VMEM((2, rows, deep), F32),
            pltpu.VMEM((2, width, deep), BF16),
            pltpu.VMEM((2, rows, deep), F32),
            pltpu.VMEM((zslots, rows, deep), BF16),
            pltpu.VMEM((2, own_rows, deep), F32),
            pltpu.VMEM(vectors.shape, F32),
            pltpu.VMEM((2, block, 2 * width), F32),
            pltpu.VMEM((2, block, 2 * width), F32),
            pltpu.VMEM((2, block, width), F32),
            pltpu.VMEM((4, block, 2 * width), BF16),
            pltpu.VMEM((rows, 2 * width), BF16),
            pltpu.VMEM((rows, 2 * width), BF16),
            pltpu.VMEM((tensor, *vectors.shape), F32),
            pltpu.VMEM((bits, *vectors.shape), F32),
            pltpu.VMEM((bits, *vectors.shape), F32),
            pltpu.SemaphoreType.DMA((2,)),
            pltpu.SemaphoreType.DMA((ring,)),
            pltpu.SemaphoreType.DMA((2 * bits, ring)),
            pltpu.SemaphoreType.DMA((2 * bits, ring)),
            pltpu.SemaphoreType.DMA((tensor - 1, 2 * units)),
            pltpu.SemaphoreType.DMA((tensor - 1, 2 * units)),
            pltpu.SemaphoreType.DMA((tensor + bits,)),
            pltpu.SemaphoreType.DMA((tensor + bits,)),
            pltpu.SemaphoreType.DMA((6, 2)),
            pltpu.SemaphoreType.DMA((2,)),
            pltpu.SemaphoreType.DMA((3, 2)),
            pltpu.SemaphoreType.DMA((4, blocks)),
            pltpu.SemaphoreType.DMA((2,)),
        ],
        compiler_params=pltpu.CompilerParams(
            collective_id=0, has_side_effects=True, vmem_limit_bytes=63 << 20
        ),
        cost_estimate=cost(
            2 * rows * wide * (chunks * deep + 2 * hidden_width + 3 * width), 8 * chunks * deep * wide
        ),
    )(
        grads, n1, slope, fc1_weight, fc2_weight, w1, x, flat_out, forward, *kv_grads, dq,
        *extra, *lefts, att, vectors, *gains, *moments_of, *tables,
    )


def body(
    tokens, out_grad, segment_ids, positions, norm1_gain, norm1_bias, norm2_gain, norm2_bias,
    qkv_weight, qkv_bias, out_weight, out_bias, fc1_weight, fc1_bias, fc2_weight, fc2_bias,
):
    model_width, heads, _, head_dim = qkv_weight.shape
    width = heads * head_dim
    hidden_width = fc1_weight.shape[1]
    row = lambda v: v.reshape(1, -1).astype(F32)
    w4 = jnp.transpose(qkv_weight, (0, 2, 1, 3))
    flat_bias = jnp.transpose(qkv_bias, (1, 0, 2)).reshape(1, 3 * width).astype(F32)
    flat_out = out_weight.reshape(width, model_width)
    tables = rope_tables(positions, 128)
    small = [
        row(norm1_gain), row(norm1_bias), row(norm2_gain), row(norm2_bias), flat_bias, row(fc1_bias)
    ]
    tensor, last = lax.axis_size("tensor"), lax.axis_size("dp") - 1
    (
        rows_all, grads_all, flat_qkv, normed_one, normed_two, queries, kv_own, kv_near, kv_far,
        activated, slope, forward, attended_grad, mean, inverse,
    ) = front(
        tokens, out_grad, w4, fc1_weight, fc2_weight, flat_out, small, tables,
        (tensor, last, heads, head_dim),
    )
    assert MOST - 2 < 2 * rows_all.shape[0]
    attended, query_grad, *kv_grads = attention(
        queries, [kv_far, kv_near, kv_own], attended_grad, positions, heads, head_dim
    )
    own_grad = out_grad.astype(F32)
    vectors = jnp.pad(jnp.sum(own_grad, 0, keepdims=True), ((4, 3), (0, 0)))
    bits = last.bit_length()
    *stacked, d_sum, d_got, branch, b_got, vectors = reduce_grads(
        (activated, attended, normed_two, grads_all, normed_one, slope, forward), kv_grads, query_grad,
        vectors, tables, (mean, inverse), (row(norm1_gain), row(norm2_gain)),
        (fc1_weight, fc2_weight, flat_qkv, flat_out), rows_all,
        (bits, tensor, heads, head_dim),
    )
    natural = hidden_width == model_width
    biases = jnp.stack([out_bias.astype(F32), fc2_bias.astype(F32)], 0)
    fc2_grad, out_weight_grad, fc1_grad, qkv_weight_grad, block_out, tokens_grad = finish(
        *stacked, tokens, out_grad, d_sum, d_got, branch, b_got, biases, heads, head_dim, natural
    )
    out_weight_grad = out_weight_grad.reshape(heads, head_dim, model_width)
    qkv_weight_grad = jnp.transpose(qkv_weight_grad, (0, 2, 1, 3))
    fc1_bias_grad = vectors[5, :hidden_width]
    qkv_bias_grad = vectors[6, : 3 * width].reshape(3, heads, head_dim)
    qkv_bias_grad = jnp.transpose(qkv_bias_grad, (1, 0, 2))
    return (
        block_out, tokens_grad,
        vectors[0], vectors[1], vectors[2], vectors[3],
        qkv_weight_grad, qkv_bias_grad, out_weight_grad, vectors[4],
        fc1_grad, fc1_bias_grad, fc2_grad, vectors[4],
    )


def solution(mesh):
    rows = P(("dp", "tensor"), None)
    return jax.shard_map(
        body,
        mesh=mesh,
        in_specs=(
            rows, rows, P("dp"), P("dp"), P(), P(), P(), P(),
            P(None, "tensor", None, None), P("tensor", None, None), P("tensor", None, None), P(),
            P(None, "tensor"), P("tensor"), P("tensor", None), P(),
        ),
        out_specs=(
            rows, rows, P(), P(), P(), P(),
            P(None, "tensor", None, None), P("tensor", None, None), P("tensor", None, None), P(),
            P(None, "tensor"), P("tensor"), P("tensor", None), P(),
        ),
        check_vma=False,
    )
```
